128 devices in a mesh: rep: 4 (over z_hi, core), row: 4 (over x), col: 8 (over z_lo, y).
Axes of the slice: x: 4, y: 4, z: 4 (z_hi: 2, z_lo: 2; z = z_hi * 2 + z_lo), core: 2. Of those that a mesh axis runs over, the one named last changes fastest.
Arguments:
- grad_parts: bfloat16 [4, 16384, 6144], P('rep', ('row', 'col')), may hold values from -0.03125 to 0.03125, as said below
- statistic: float32 [6144, 6144], P('row', 'col'), may hold values from -150 to 150, as said below
Outputs:
- gram_matrix: float32 [6144, 6144], P('row', 'col')
- statistic_next: float32 [6144, 6144], P('row', 'col')
The draws below stay inside these ranges and needn't reach their ends.
Inputs may be any that keep to these rules, and one draw needn't show every extreme that they name: Every entry of grad_parts has a magnitude between 2^-10 and 2^-5. statistic is symmetric and positive definite.
All inputs are finite; a program needn't handle non-finite values.
Results may differ from the reference program's by a relative error of at most 0.008.
Values may be sent and summed in bfloat16 or wider, within the bound.
A program may use at most 128 MiB of HBM per device.

```python
import math
import jax
import jax.numpy as jnp
from jax import lax

D = 6144
HID = 16384
N_REP = 4


def draw_grad_parts(key, part):
    key_sign = jax.random.fold_in(key, 41)
    key_level = jax.random.fold_in(key, 53)
    signs = jnp.where(jax.random.bernoulli(key_sign, 0.5, (N_REP, HID, D)), 1.0, -1.0).astype(jnp.float32)
    level = jax.random.uniform(key_level, (N_REP, HID, D), jnp.float32, -10.0, -5.0)
    return (signs * jnp.exp2(level)).astype(jnp.bfloat16)


def draw_statistic(key, part):
    key_factor = jax.random.fold_in(key, 11)
    key_ridge = jax.random.fold_in(key, 23)
    factor = jax.random.truncated_normal(key_factor, -3.0, 3.0, (D, D), jnp.float32) * (2.0 / math.sqrt(D))
    crossed = jnp.dot(factor.T, factor, precision=lax.Precision.HIGHEST)
    crossed = 0.5 * (crossed + crossed.T)
    ridge = jax.random.uniform(key_ridge, (D,), jnp.float32, 0.25, 1.0)
    return crossed + jnp.diag(ridge)


def setup_inputs(seed: int = 0) -> dict:
    seeds = jax.random.split(jax.random.key(seed), 3)
    grad_parts = draw_grad_parts(jax.random.fold_in(seeds[2], 71), 0)
    statistic = draw_statistic(jax.random.fold_in(seeds[2], 71), 0)
    return {"grad_parts": grad_parts, "statistic": statistic}


def reference(grad_parts, statistic):
    summed = jnp.sum(grad_parts.astype(jnp.float32), axis=0).astype(jnp.bfloat16)
    summed = lax.optimization_barrier(summed)
    summed_f32 = summed.astype(jnp.float32)
    product = jnp.dot(summed_f32.T, summed_f32, precision=lax.Precision.HIGHEST)
    gram_full = 0.5 * (product + product.T)
    statistic_next = 0.95 * statistic + 0.05 * gram_full
    return gram_full, statistic_next
```

```python
import functools

import jax
import jax.numpy as jnp
from jax import lax
from jax.experimental import pallas as pl
from jax.experimental.pallas import tpu as pltpu
from jax.sharding import PartitionSpec as P

MESH = pl.DeviceIdType.MESH
BF16 = jnp.bfloat16
F32 = jnp.float32
CHUNKS = 16


def mod(a, n):
    return lax.rem(a, n)


def rcopy(src, dst, send, recv, device):
    return pltpu.make_async_remote_copy(
        src_ref=src, dst_ref=dst, send_sem=send, recv_sem=recv, device_id=device, device_id_type=MESH
    )


class Ring:
    def __init__(self, i, up, down, src, add, bufs, sends, recvs):
        self.i, self.src, self.add = i, src, add
        (ra, rb, fa, fb, ga, gb, sa, sb) = bufs
        at = lambda j: mod(i + j, 4)
        mk = lambda n, s, d, dev: rcopy(s, d, sends.at[n], recvs.at[n], dev)
        self.sa, self.sb, self.at = sa, sb, at
        self.ra = mk(0, src(0, at(2)), ra, up)
        self.rb = mk(1, src(1, at(2)), rb, down)
        self.fb = mk(2, src(1, at(1)), fb, up)
        self.fa = mk(3, src(0, at(3)), fa, down)
        self.ga = mk(4, sa, ga, up)
        self.gb = mk(5, sb, gb, down)
        self.bufs = bufs

    def far(self):
        self.ra.start()
        self.rb.start()

    def near_up(self):
        self.fb.start()

    def near_down(self):
        self.fa.start()

    def pass_on(self):
        ra, rb = self.bufs[0], self.bufs[1]
        self.ra.wait_recv()
        self.sa[...] = (ra[...].astype(F32) + self.add(0, self.at(1))).astype(BF16)
        self.ga.start()
        self.rb.wait_recv()
        self.sb[...] = (rb[...].astype(F32) + self.add(1, self.at(3))).astype(BF16)
        self.gb.start()

    def result(self):
        _, _, fa, fb, ga, gb, _, _ = self.bufs
        self.fa.wait_recv()
        self.ga.wait_recv()
        a = self.add(0, self.i) + (fa[...].astype(F32) + ga[...].astype(F32))
        self.fb.wait_recv()
        self.gb.wait_recv()
        b = self.add(1, self.i) + (fb[...].astype(F32) + gb[...].astype(F32))
        return a, b

    def drain(self):
        for c in (self.ra, self.rb, self.fb, self.fa, self.ga, self.gb):
            c.wait_send()


def kernel(
    g, out, gown, gsib, psend, zrel, zrec, sline, t, u,
    al, be, t8a, t8b, a2, b2, c2a, c2b, xf, xb, x8f, x8b, zf, zb, oa, o8,
    lsem, csend, crecv, rsend, rrecv, fsend, frecv, dsend, drecv,
):
    rep, x, col = lax.axis_index("rep"), lax.axis_index("row"), lax.axis_index("col")
    zh, k = lax.div(rep, 2), mod(rep, 2)
    zl, y = lax.div(col, 4), mod(col, 4)
    z = 2 * zh + zl
    q, d = psend.shape
    half = q // 2
    w = d // CHUNKS
    b = d // 8
    h = b // 2
    hq = h // 4
    h8 = hq // 2

    def dev(x, y, z, k):
        return {"rep": lax.div(z, 2) * 2 + k, "row": x, "col": mod(z, 2) * 4 + y}

    sib = dev(x, y, z, 1 - k)
    zp, zm = dev(x, y, mod(z + 1, 4), k), dev(x, y, mod(z + 3, 4), k)
    yp, ym = dev(x, mod(y + 1, 4), z, k), dev(x, mod(y + 3, 4), z, k)
    xp, xm = dev(mod(x + 1, 4), y, z, k), dev(mod(x + 3, 4), y, z, k)

    def cols(c):
        return pl.ds(pl.multiple_of(c * w, w), w)

    def rows(i):
        return pl.ds(pl.multiple_of(i * q, q), q)

    def load(c):
        return pltpu.make_async_copy(g.at[:, k, :, cols(c)], gown.at[:, :, cols(c)], lsem.at[c])

    def swap(c):
        return rcopy(g.at[:, 1 - k, :, cols(c)], gsib.at[:, :, cols(c)], csend.at[0], crecv.at[0, c], sib)

    def z1(c):
        return (
            rcopy(psend.at[0:half, cols(c)], zrel.at[0, :, cols(c)], csend.at[1], crecv.at[1, c], zp),
            rcopy(psend.at[half:q, cols(c)], zrel.at[1, :, cols(c)], csend.at[2], crecv.at[2, c], zm),
        )

    def z2(c):
        return (
            rcopy(zrel.at[0, :, cols(c)], zrec.at[0, :, cols(c)], csend.at[3], crecv.at[3, c], zp),
            rcopy(zrel.at[1, :, cols(c)], zrec.at[1, :, cols(c)], csend.at[4], crecv.at[4, c], zm),
        )

    def block(j, c, part=None):
        base = (2 * mod(y + j, 4) + k) * q
        if part is None:
            return sline.at[pl.ds(pl.multiple_of(base, q), q), cols(c)]
        return sline.at[pl.ds(pl.multiple_of(base + part * half, half), half), cols(c)]

    def sblock(j, c):
        return sline.at[pl.ds(pl.multiple_of((2 * mod(y + j, 4) + 1 - k) * q, q), q), cols(c)]

    def y1(c):
        own = block(0, c)
        return (
            rcopy(own, own, csend.at[5], crecv.at[5, c], yp),
            rcopy(own, own, csend.at[6], crecv.at[6, c], ym),
        )

    def y1_landed(c):
        down, upper = block(3, c), block(1, c)
        return (
            rcopy(down, down, csend.at[5], crecv.at[5, c], yp),
            rcopy(upper, upper, csend.at[6], crecv.at[6, c], ym),
        )

    def y2(c):
        down, upper = block(3, c, 0), block(1, c, 1)
        return (
            rcopy(down, down, csend.at[7], crecv.at[7, c], yp),
            rcopy(upper, upper, csend.at[8], crecv.at[8, c], ym),
        )

    def y2_landed(c):
        lo, hi = block(2, c, 0), block(2, c, 1)
        return (
            rcopy(lo, lo, csend.at[7], crecv.at[7, c], yp),
            rcopy(hi, hi, csend.at[8], crecv.at[8, c], ym),
        )

    def share(j, c):
        blk = block(j, c)
        return rcopy(blk, blk, csend.at[9 + j], crecv.at[9 + j, c], sib)

    def share_landed(j, c):
        blk = sblock(j, c)
        return rcopy(blk, blk, csend.at[9 + j], crecv.at[9 + j, c], sib)

    @pl.loop(0, CHUNKS)
    def _(c):
        load(c).start()
        swap(c).start()

    @pl.loop(0, CHUNKS + 4)
    def _(step):
        @pl.when(step < CHUNKS)
        def _():
            c = step
            load(c).wait()
            swap(c).wait_recv()
            o = 1 - zh
            psend[:, cols(c)] = (gown[o, :, cols(c)].astype(F32) + gsib[o, :, cols(c)].astype(F32)).astype(BF16)
            for cp in z1(c):
                cp.start()

        @pl.when((step >= 1) & (step < CHUNKS + 1))
        def _():
            c = step - 1
            for cp, fwd in zip(z1(c), z2(c)):
                cp.wait_recv()
                fwd.start()

        @pl.when((step >= 2) & (step < CHUNKS + 2))
        def _():
            c = step - 2
            for cp in z2(c):
                cp.wait_recv()
            own = gown[zh, :, cols(c)].astype(F32) + gsib[zh, :, cols(c)].astype(F32)
            far = jnp.concatenate([zrec[0, :, cols(c)], zrec[1, :, cols(c)]], axis=0).astype(F32)
            sline[rows(2 * y + k), cols(c)] = (own + far).astype(BF16)
            for cp in y1(c):
                cp.start()
            share(0, c).start()

        @pl.when((step >= 3) & (step < CHUNKS + 3))
        def _():
            c = step - 3
            for cp, fwd, j in zip(y1_landed(c), y2(c), (3, 1)):
                cp.wait_recv()
                fwd.start()
                share(j, c).start()

        @pl.when(step >= 4)
        def _():
            c = step - 4
            for cp in y2_landed(c):
                cp.wait_recv()
            share(2, c).start()

    @pl.loop(0, CHUNKS)
    def _(c):
        for j in range(4):
            share_landed(j, c).wait_recv()

    def sent(n, ref):
        rcopy(ref, ref, csend.at[n], crecv.at[0, 0], sib).wait_send()

    sent(0, gsib)
    for n in (1, 2, 3, 4):
        sent(n, zrel.at[0])
    for n in (5, 6, 9, 10, 11, 12):
        sent(n, psend)
    for n in (7, 8):
        sent(n, zrel.at[0])

    def cof(r):
        return y + 4 * lax.div(mod(r - y + 8, 8), 4)

    def tile(slot, r, c):
        lhs = sline[:, pl.ds(pl.multiple_of(r * b + k * h, h), h)]
        rhs = sline[:, pl.ds(pl.multiple_of(c * b, b), b)]
        acc = lax.dot_general(lhs, rhs, (((0,), (0,)), ((), ())), preferred_element_type=F32)
        t[slot] = acc.astype(BF16)

    def pair(j):
        @pl.loop(0, 2)
        def _(s):
            r = 2 * mod(x + j, 4) + s
            tile(r, r, cof(r))

    def hrows(i, n):
        return pl.ds(pl.multiple_of(i * n, n), n)

    f = lambda v: v.astype(F32)
    left, right = slice(0, h), slice(h, b)
    xring = lambda n, src, add, bufs: Ring(x, xp, xm, src, add, bufs, rsend.at[n], rrecv.at[n])
    zring = lambda n, src, add, bufs: Ring(z, zp, zm, src, add, bufs, rsend.at[n], rrecv.at[n])

    alpha = xring(
        0,
        lambda s, p: t.at[2 * p + s, :, left],
        lambda s, p: f(t[2 * p + s, :, left]),
        [al.at[n] for n in range(8)],
    )
    eight = xring(
        1,
        lambda s, p: t.at[8, hrows(p, hq), (left, right)[s]],
        lambda s, p: f(t[8, hrows(p, hq), (left, right)[s]]),
        [t8a.at[n] for n in range(8)],
    )

    def beta_of(j):
        p = mod(x + j, 4)
        return zring(
            2 + j,
            lambda s, v: t.at[2 * p + s, hrows(v, hq), right],
            lambda s, v: f(t[2 * p + s, hrows(v, hq), right]),
            [be.at[j, n] for n in range(8)],
        )

    beta = [beta_of(j) for j in range(4)]

    def start_all(ring):
        ring.far()
        ring.near_up()
        ring.near_down()

    pair(2)
    alpha.far()
    start_all(beta[2])
    pair(1)
    alpha.near_up()
    start_all(beta[1])
    pair(3)
    alpha.near_down()
    start_all(beta[3])
    tile(8, y, y + 4)
    start_all(eight)
    pair(0)
    start_all(beta[0])
    alpha.pass_on()
    beta[2].pass_on()
    eight.pass_on()
    for j in (1, 3, 0):
        beta[j].pass_on()

    beta2 = xring(
        6, lambda s, p: zb.at[2 * p + s], lambda s, p: zf[2 * p + s], [b2.at[n] for n in range(8)]
    )
    alpha2 = zring(
        7,
        lambda s, v: xb.at[s, hrows(v, hq), :],
        lambda s, v: xf[s, hrows(v, hq), :],
        [a2.at[n] for n in range(8)],
    )
    ha = 2 * h // 3
    eight_cols = (slice(0, ha), slice(ha, h))

    def piece8(v):
        return hrows(lax.div(v, 2), h8), mod(v, 2)

    def src8(s, v):
        r, c = piece8(v)
        return x8b.at[c, r, eight_cols[s]]

    def add8(s, v):
        r, c = piece8(v)
        return x8f[c, r, eight_cols[s]]

    bufs8 = [(c2a, c2b)[n % 2].at[n // 2] for n in range(8)]
    eight2 = zring(8, src8, add8, bufs8)

    for j, go in ((2, beta2.far), (1, beta2.near_up), (3, beta2.near_down), (0, None)):
        for s, v in enumerate(beta[j].result()):
            zf[2 * mod(x + j, 4) + s] = v
            zb[2 * mod(x + j, 4) + s] = v.astype(BF16)
        if go is not None:
            go()
    for s, v in enumerate(alpha.result()):
        xf[s] = v
        xb[s] = v.astype(BF16)
    start_all(alpha2)
    for s, v in enumerate(eight.result()):
        x8f[s] = v
        x8b[s] = v.astype(BF16)
    start_all(eight2)
    beta2.pass_on()
    alpha2.pass_on()
    eight2.pass_on()
    for s, v in enumerate(beta2.result()):
        oa[s, :, right] = v.astype(BF16)
    for s, v in enumerate(alpha2.result()):
        oa[s, :, left] = v.astype(BF16)
    for s, v in enumerate(eight2.result()):
        o8[:, eight_cols[s]] = v.astype(BF16)

    place = pl.ds(pl.multiple_of(k * h + z * hq, hq), hq)
    place8 = pl.ds(pl.multiple_of(k * h + x * hq + lax.div(z, 2) * h8, h8), h8)
    cols8 = pl.ds(pl.multiple_of(mod(z, 2) * h, h), h)

    def to_direct(s, up, act):
        r = 2 * x + s
        c = cof(r)
        to = 2 * up + lax.div(c, 4)
        src, dst = oa.at[s], u.at[s, place, :]

        @pl.when(to != z)
        def _():
            act(rcopy(src, dst, fsend.at[s, up], frecv.at[s], dev(x, y, to, k)))

        return to == z, src, dst

    def to_mirror(s, up, act):
        r = 2 * x + s
        c = cof(r)

        @pl.when(r != c)
        def _():
            slot = mod(c, 2)
            to = dev(lax.div(c, 2), mod(r, 4), 2 * up + lax.div(r, 4), k)
            act(rcopy(oa.at[s], u.at[slot, place, :], fsend.at[s, 2 + up], frecv.at[slot], to))

    def to_eight(side, up, act):
        slot = mod(y, 2)
        tx, tz = lax.div(y + 4 * side, 2), 2 * up + 1 - side
        src, dst = o8, u.at[slot, place8, cols8]

        @pl.when((tx != x) | (tz != z))
        def _():
            act(rcopy(src, dst, fsend.at[2, 2 * side + up], frecv.at[slot], dev(tx, y, tz, k)))

        return (tx == x) & (tz == z), src, dst

    begin = lambda cp: cp.start()
    ended = lambda cp: cp.wait_send()
    for up in (0, 1):
        for s in (0, 1):
            mine, src, dst = to_direct(s, up, begin)

            @pl.when(mine)
            def _():
                pltpu.make_async_copy(src, dst, frecv.at[s]).start()

            to_mirror(s, up, begin)
        for side in (0, 1):
            mine, src, dst = to_eight(side, up, begin)

            @pl.when(mine)
            def _():
                pltpu.make_async_copy(src, dst, frecv.at[mod(y, 2)]).start()

    for ring in (alpha, eight, *beta, beta2, alpha2, eight2):
        ring.drain()

    for s in (0, 1):
        part = u.at[s, hrows(k, h), :]
        rcopy(part, part, fsend.at[s, 0], frecv.at[s], sib).wait_recv()
        rcopy(part, part, dsend.at[s], drecv.at[s], sib).start()
    for up in (0, 1):
        for s in (0, 1):
            to_direct(s, up, ended)
            to_mirror(s, up, ended)
        for side in (0, 1):
            to_eight(side, up, ended)
    for s in (0, 1):
        part, other = u.at[s, hrows(k, h), :], u.at[s, hrows(1 - k, h), :]
        rcopy(other, other, dsend.at[s], drecv.at[s], sib).wait_recv()
        rcopy(part, part, dsend.at[s], drecv.at[s], sib).wait_send()
        pltpu.make_async_copy(u.at[s], out.at[s], lsem.at[s]).start()
    for s in (0, 1):
        pltpu.make_async_copy(u.at[s], out.at[s], lsem.at[s]).wait()


def gather_tiles(grad):
    _, n, d = grad.shape
    q, b = n // 4, d // 8
    h = b // 2
    hq = h // 4
    h8 = hq // 2
    ha = 2 * h // 3
    vm = pltpu.VMEM
    dma = pltpu.SemaphoreType.DMA
    return pl.pallas_call(
        kernel,
        out_shape=jax.ShapeDtypeStruct((2, b, b), BF16),
        in_specs=[pl.BlockSpec(memory_space=pl.ANY)],
        out_specs=pl.BlockSpec(memory_space=pl.ANY),
        scratch_shapes=[
            vm((2, q, d), BF16), vm((2, q, d), BF16), vm((q, d), BF16),
            vm((2, q // 2, d), BF16), vm((2, q // 2, d), BF16),
            vm((8 * q, d), BF16), vm((9, h, b), BF16), vm((2, b, b), BF16),
            vm((8, h, h), BF16), vm((4, 8, hq, h), BF16), vm((8, hq, h), BF16), vm((8, hq, h), BF16),
            vm((8, hq, h), BF16), vm((8, hq, h), BF16), vm((4, h8, ha), BF16), vm((4, h8, h - ha), BF16),
            vm((2, h, h), F32), vm((2, h, h), BF16), vm((2, hq, h), F32), vm((2, hq, h), BF16),
            vm((8, hq, h), F32), vm((8, hq, h), BF16), vm((2, hq, b), BF16), vm((h8, h), BF16),
            dma((CHUNKS,)), dma((13,)), dma((13, CHUNKS)), dma((9, 6)), dma((9, 6)),
            dma((3, 4)), dma((2,)), dma((2,)), dma((2,)),
        ],
        compiler_params=pltpu.CompilerParams(has_side_effects=True, vmem_limit_bytes=64 * 1024 * 1024 - 66 * 1024),
    )(grad.reshape(2, 2, q, d))


def shards(grad, statistic):
    tiles = gather_tiles(grad)
    x, col = lax.axis_index("row"), lax.axis_index("col")
    parts = []
    for s in (0, 1):
        r = 2 * x + s
        apart = (r - col) % 8
        mirrored = (apart > 4) | ((apart == 4) & (r >= 4))
        parts.append(jnp.where(mirrored, tiles[s].T, tiles[s]).astype(F32))
    gram = jnp.concatenate(parts, axis=0)
    return gram, 0.95 * statistic + 0.05 * gram


def solution(mesh):
    return jax.shard_map(
        shards,
        mesh=mesh,
        in_specs=(P("rep", ("row", "col"), None), P("row", "col")),
        out_specs=(P("row", "col"), P("row", "col")),
        check_vma=False,
    )
```

```python
import functools

import jax
import jax.numpy as jnp
from jax import lax
from jax.experimental import pallas as pl
from jax.experimental.pallas import tpu as pltpu
from jax.sharding import PartitionSpec as P

MESH = pl.DeviceIdType.MESH
BF16 = jnp.bfloat16
F32 = jnp.float32
STAGES = 6
PER = 2
CHUNKS = STAGES * PER


def mod(a, n):
    return lax.rem(a, n)


def rcopy(src, dst, send, recv, device):
    return pltpu.make_async_remote_copy(
        src_ref=src, dst_ref=dst, send_sem=send, recv_sem=recv, device_id=device, device_id_type=MESH
    )


class Ring:
    def __init__(self, i, up, down, n, src, add, bufs, sends, recvs):
        self.i, self.n, self.add = i, n, add
        (ra, rb, fa, fb, ga, gb, sa, sb) = bufs
        at = lambda j: mod(i + j, 4)
        mk = lambda n, s, d, dev: rcopy(s, d, sends.at[n], recvs.at[n], dev)
        self.at = at
        self.ra = mk(0, src(0, at(2)), ra, up)
        self.rb = mk(1, src(1, at(2)), rb, down)
        self.fb = mk(2, src(1, at(1)), fb, up)
        self.fa = mk(3, src(0, at(3)), fa, down)
        self.ga = mk(4, sa, ga, up)
        self.gb = mk(5, sb, gb, down)
        self.bufs = bufs

    def start(self):
        self.ra.start()
        self.rb.start()
        self.fb.start()
        self.fa.start()

    def pass_on(self):
        ra, rb, _, _, _, _, sa, sb = self.bufs
        for far, got, sum_, s, to, on in ((self.ra, ra, sa, 0, 1, self.ga), (self.rb, rb, sb, 1, 3, self.gb)):
            far.wait_recv()

            @pl.loop(0, self.n)
            def _(m):
                sum_[m] = (got[m].astype(F32) + self.add(s, self.at(to), m)).astype(BF16)

            on.start()

    def result(self, put):
        _, _, fa, fb, ga, gb, _, _ = self.bufs
        for s, near, far, a, b in ((0, self.fa, self.ga, fa, ga), (1, self.fb, self.gb, fb, gb)):
            near.wait_recv()
            far.wait_recv()

            @pl.loop(0, self.n)
            def _(m):
                put(s, m, self.add(s, self.i, m) + (a[m].astype(F32) + b[m].astype(F32)))

    def drain(self):
        for c in (self.ra, self.rb, self.fb, self.fa, self.ga, self.gb):
            c.wait_send()


def kernel(
    g, out, gown, gsib, psend, zrel, zrec, sline, t, l1, l2, xf, xb, o, u,
    lsem, csend, crecv, rsend, rrecv, fsend, frecv, dsem,
):
    rep, x, col = lax.axis_index("rep"), lax.axis_index("row"), lax.axis_index("col")
    zh, k = lax.div(rep, 2), mod(rep, 2)
    zl, y = lax.div(col, 4), mod(col, 4)
    z = 2 * zh + zl
    q, d = psend.shape
    half = q // 2
    w = d // CHUNKS
    n8 = d // STAGES // 8
    n4 = n8 // 4

    def dev(x, y, z, k):
        return {"rep": lax.div(z, 2) * 2 + k, "row": x, "col": mod(z, 2) * 4 + y}

    sib = dev(x, y, z, 1 - k)
    zp, zm = dev(x, y, mod(z + 1, 4), k), dev(x, y, mod(z + 3, 4), k)
    yp, ym = dev(x, mod(y + 1, 4), z, k), dev(x, mod(y + 3, 4), z, k)
    xp, xm = dev(mod(x + 1, 4), y, z, k), dev(mod(x + 3, 4), y, z, k)

    def cols(c):
        return pl.ds(pl.multiple_of(c * w, w), w)

    def rows(i):
        return pl.ds(pl.multiple_of(i * q, q), q)

    def load(c):
        return pltpu.make_async_copy(g.at[:, k, :, cols(c)], gown.at[:, :, cols(c)], lsem.at[c])

    def swap(c):
        return rcopy(g.at[:, 1 - k, :, cols(c)], gsib.at[:, :, cols(c)], csend.at[0], crecv.at[0, c], sib)

    def z1(c):
        return (
            rcopy(psend.at[0:half, cols(c)], zrel.at[0, :, cols(c)], csend.at[1], crecv.at[1, c], zp),
            rcopy(psend.at[half:q, cols(c)], zrel.at[1, :, cols(c)], csend.at[2], crecv.at[2, c], zm),
        )

    def z2(c):
        return (
            rcopy(zrel.at[0, :, cols(c)], zrec.at[0, :, cols(c)], csend.at[3], crecv.at[3, c], zp),
            rcopy(zrel.at[1, :, cols(c)], zrec.at[1, :, cols(c)], csend.at[4], crecv.at[4, c], zm),
        )

    def block(j, c, part=None):
        base = (2 * mod(y + j, 4) + k) * q
        if part is None:
            return sline.at[pl.ds(pl.multiple_of(base, q), q), cols(c)]
        return sline.at[pl.ds(pl.multiple_of(base + part * half, half), half), cols(c)]

    def sblock(j, c):
        return sline.at[pl.ds(pl.multiple_of((2 * mod(y + j, 4) + 1 - k) * q, q), q), cols(c)]

    def y1(c):
        own = block(0, c)
        return (
            rcopy(own, own, csend.at[5], crecv.at[5, c], yp),
            rcopy(own, own, csend.at[6], crecv.at[6, c], ym),
        )

    def y1_landed(c):
        down, upper = block(3, c), block(1, c)
        return (
            rcopy(down, down, csend.at[5], crecv.at[5, c], yp),
            rcopy(upper, upper, csend.at[6], crecv.at[6, c], ym),
        )

    def y2(c):
        down, upper = block(3, c, 0), block(1, c, 1)
        return (
            rcopy(down, down, csend.at[7], crecv.at[7, c], yp),
            rcopy(upper, upper, csend.at[8], crecv.at[8, c], ym),
        )

    def y2_landed(c):
        lo, hi = block(2, c, 0), block(2, c, 1)
        return (
            rcopy(lo, lo, csend.at[7], crecv.at[7, c], yp),
            rcopy(hi, hi, csend.at[8], crecv.at[8, c], ym),
        )

    def share(j, c):
        blk = block(j, c)
        return rcopy(blk, blk, csend.at[9 + j], crecv.at[9 + j, c], sib)

    def share_landed(j, c):
        blk = sblock(j, c)
        return rcopy(blk, blk, csend.at[9 + j], crecv.at[9 + j, c], sib)

    @pl.loop(0, CHUNKS)
    def _(c):
        load(c).start()
        swap(c).start()

    def gather_step(step):
        c = step
        if c < CHUNKS:
            load(c).wait()
            swap(c).wait_recv()
            away = 1 - zh
            psend[:, cols(c)] = (gown[away, :, cols(c)].astype(F32) + gsib[away, :, cols(c)].astype(F32)).astype(BF16)
            for cp in z1(c):
                cp.start()
        c = step - 1
        if 0 <= c < CHUNKS:
            for cp, fwd in zip(z1(c), z2(c)):
                cp.wait_recv()
                fwd.start()
        c = step - 2
        if 0 <= c < CHUNKS:
            for cp in z2(c):
                cp.wait_recv()
            own = gown[zh, :, cols(c)].astype(F32) + gsib[zh, :, cols(c)].astype(F32)
            far = jnp.concatenate([zrec[0, :, cols(c)], zrec[1, :, cols(c)]], axis=0).astype(F32)
            sline[rows(2 * y + k), cols(c)] = (own + far).astype(BF16)
            for cp in y1(c):
                cp.start()
            share(0, c).start()
        c = step - 3
        if 0 <= c < CHUNKS:
            for cp, fwd, j in zip(y1_landed(c), y2(c), (3, 1)):
                cp.wait_recv()
                fwd.start()
                share(j, c).start()
        c = step - 4
        if 0 <= c < CHUNKS:
            for cp in y2_landed(c):
                cp.wait_recv()
            share(2, c).start()

    def first(n):
        return n * (n + 1) // 2

    strip = 2 * y + k

    def tiles(n):
        for c in range(n * PER, (n + 1) * PER):
            for j in range(4):
                share_landed(j, c).wait_recv()

        @pl.loop(0, n + 1)
        def _(m):
            lhs = sline[:, pl.ds(pl.multiple_of((8 * n + strip) * n8, n8), n8)]
            rhs = sline[:, pl.ds(pl.multiple_of(m * 8 * n8, 8 * n8), 8 * n8)]
            acc = lax.dot_general(lhs, rhs, (((0,), (0,)), ((), ())), preferred_element_type=F32)
            for j in range(8):
                t[first(n) + m, j] = acc[:, j * n8 : (j + 1) * n8].astype(BF16)

    def quarter(v):
        return pl.ds(pl.multiple_of(v * n4, n4), n4)

    def ring1(n):
        f = first(n)
        return Ring(
            x, xp, xm, n + 1,
            lambda s, p: t.at[f : f + n + 1, 2 * p + s],
            lambda s, p, m: t[f + m, 2 * p + s].astype(F32),
            [l1.at[i, f : f + n + 1] for i in range(8)],
            rsend.at[0, n], rrecv.at[0, n],
        )

    def ring2(n):
        f = first(n)
        return Ring(
            z, zp, zm, n + 1,
            lambda s, v: xb.at[s, f : f + n + 1, quarter(v), :],
            lambda s, v, m: xf[s, f + m, quarter(v), :],
            [l2.at[i, f : f + n + 1] for i in range(8)],
            rsend.at[1, n], rrecv.at[1, n],
        )

    rings1 = [ring1(n) for n in range(STAGES)]
    rings2 = [ring2(n) for n in range(STAGES)]

    def exchange(n, begin):
        f = first(n)
        rblk = 8 * n + strip

        def one(m, up, side):
            cblk = 8 * m + 2 * x
            src = o.at[f + m]
            if side == 0:
                tx, tc = lax.div(rblk, 12), lax.div(cblk, 6)
                dst = u.at[mod(rblk, 12), pl.ds(mod(cblk, 6), 2), quarter(z), :]
            else:
                tx, tc = lax.div(cblk, 12), lax.div(rblk, 6)
                dst = u.at[pl.ds(mod(cblk, 12), 2), mod(rblk, 6), quarter(z), :]
            ty, tz = mod(tc, 4), 2 * up + lax.div(tc, 4)
            mine = (tx == x) & (ty == y) & (tz == z)

            @pl.when(jnp.logical_not(mine))
            def _():
                cp = rcopy(src, dst, fsend.at[f + m, 2 * side + up], frecv.at[0], dev(tx, ty, tz, k))
                if begin:
                    cp.start()
                else:
                    cp.wait_send()

            if begin:

                @pl.when(mine)
                def _():
                    pltpu.make_async_copy(src, dst, frecv.at[0]).start()

        for up in (0, 1):

            @pl.loop(0, n + 1)
            def _(m):
                one(m, up, 0)

            if n:

                @pl.loop(0, n)
                def _(m):
                    one(m, up, 1)

    def reduce1(n):
        f = first(n)

        def put(s, m, v):
            xf[s, f + m] = v
            xb[s, f + m] = v.astype(BF16)

        rings1[n].result(put)
        rings2[n].start()

    def reduce2(n):
        f = first(n)

        def put(s, m, v):
            o[f + m, s] = v.astype(BF16)

        rings2[n].result(put)
        exchange(n, True)

    def begin(n):
        tiles(n)
        rings1[n].start()

    plan = {}

    def at(step, what, n):
        plan.setdefault(step, []).append((what, n))

    passes1 = lambda n: rings1[n].pass_on()
    passes2 = lambda n: rings2[n].pass_on()
    for n in range(STAGES):
        s0 = PER * (n + 1) + 4
        at(s0 + 1 + (n in (3, 4)), passes1, n)
        at(s0 + 4, reduce1, n)
        at(s0 + 5, passes2, n)
        at(s0 + 6, reduce2, n)
        at(s0, begin, n)
    for step in range(max(plan) + 1):
        gather_step(step)
        for what, n in plan.get(step, ()):
            what(n)

    def sent(n, ref):
        rcopy(ref, ref, csend.at[n], crecv.at[0, 0], sib).wait_send()

    sent(0, gsib)
    for n in (1, 2, 3, 4):
        sent(n, zrel.at[0])
    for n in (5, 6, 9, 10, 11, 12):
        sent(n, psend)
    for n in (7, 8):
        sent(n, zrel.at[0])

    for n in range(STAGES):
        rings1[n].drain()
        rings2[n].drain()

    whole = u.at[0:6]
    rcopy(whole, whole, dsem.at[0], frecv.at[0], sib).wait_recv()

    @pl.loop(0, 12)
    def _(i):
        for j in range(6):
            direct = lax.div(12 * x + i, 8) >= lax.div(6 * col + j, 8)
            from_me = jnp.where(direct, mod(i, 2), j % 2) == k

            @pl.when(from_me)
            def _():
                rcopy(u.at[i, j], u.at[i, j], dsem.at[0], dsem.at[1], sib).start()

    for n in range(STAGES):
        exchange(n, False)
    rcopy(whole, whole, dsem.at[0], dsem.at[1], sib).wait_recv()
    rcopy(whole, whole, dsem.at[0], dsem.at[1], sib).wait_send()
    whole_out = pltpu.make_async_copy(u, out, lsem.at[0])
    whole_out.start()
    whole_out.wait()


def gather_blocks(grad):
    _, n, d = grad.shape
    q = n // 4
    n8 = d // STAGES // 8
    n4 = n8 // 4
    count = STAGES * (STAGES + 1) // 2
    vm = pltpu.VMEM
    dma = pltpu.SemaphoreType.DMA
    return pl.pallas_call(
        kernel,
        out_shape=jax.ShapeDtypeStruct((12, 6, n8, n8), BF16),
        in_specs=[pl.BlockSpec(memory_space=pl.ANY)],
        out_specs=pl.BlockSpec(memory_space=pl.ANY),
        scratch_shapes=[
            vm((2, q, d), BF16), vm((2, q, d), BF16), vm((q, d), BF16),
            vm((2, q // 2, d), BF16), vm((2, q // 2, d), BF16),
            vm((8 * q, d), BF16), vm((count, 8, n8, n8), BF16),
            vm((8, count, n8, n8), BF16), vm((8, count, n4, n8), BF16),
            vm((2, count, n8, n8), F32), vm((2, count, n8, n8), BF16),
            vm((count, 2, n4, n8), BF16), vm((12, 6, n8, n8), BF16),
            dma((CHUNKS,)), dma((13,)), dma((13, CHUNKS)), dma((2, STAGES, 6)), dma((2, STAGES, 6)),
            dma((count, 4)), dma((1,)), dma((2,)),
        ],
        compiler_params=pltpu.CompilerParams(has_side_effects=True, vmem_limit_bytes=56 * 1024 * 1024),
    )(grad.reshape(2, 2, q, d))


GROUP = 2


def finish(blocks, statistic, gram, following):
    i0 = pl.program_id(0) * GROUP
    row0, col0 = 12 * lax.axis_index("row"), 6 * lax.axis_index("col")
    n = blocks.shape[-1]
    for i in range(GROUP):
        for j in range(6):
            direct = lax.div(row0 + i0 + i, 8) >= lax.div(col0 + j, 8)
            at = (slice(i * n, (i + 1) * n), slice(j * n, (j + 1) * n))

            @pl.when(direct)
            def _():
                gram[at] = blocks[i, j].astype(F32)

            @pl.when(jnp.logical_not(direct))
            def _():
                gram[at] = blocks[i, j].astype(F32).T

    following[...] = 0.95 * statistic[...] + 0.05 * gram[...]


def shards(grad, statistic):
    blocks = gather_blocks(grad)
    n = blocks.shape[-1]
    tile = pl.BlockSpec((GROUP * n, 6 * n), lambda i: (i, 0))
    shape = jax.ShapeDtypeStruct(statistic.shape, F32)
    return pl.pallas_call(
        finish,
        grid=(12 // GROUP,),
        out_shape=(shape, shape),
        in_specs=[pl.BlockSpec((GROUP, 6, n, n), lambda i: (i, 0, 0, 0)), tile],
        out_specs=(tile, tile),
    )(blocks, statistic)


def solution(mesh):
    return jax.shard_map(
        shards,
        mesh=mesh,
        in_specs=(P("rep", ("row", "col"), None), P("row", "col")),
        out_specs=(P("row", "col"), P("row", "col")),
        check_vma=False,
    )
```

```python
import functools

import jax
import jax.numpy as jnp
from jax import lax
from jax.experimental import pallas as pl
from jax.experimental.pallas import tpu as pltpu
from jax.sharding import PartitionSpec as P

MESH = pl.DeviceIdType.MESH
BF16 = jnp.bfloat16
F32 = jnp.float32
BLOCK = 128
STAGES = 12
WIDTHS = (1, 1, 2) + (4,) * 11
STARTS = tuple(sum(WIDTHS[:i]) for i in range(len(WIDTHS)))
CHUNKS = len(WIDTHS)
BETA_FROM = 8


def count(n):
    return n // 2 + 1


def first(n):
    return sum(count(i) for i in range(n))


TOTAL = first(STAGES)


def mod(a, n):
    return lax.rem(a, n)


def rcopy(src, dst, send, recv, device):
    return pltpu.make_async_remote_copy(
        src_ref=src, dst_ref=dst, send_sem=send, recv_sem=recv, device_id=device, device_id_type=MESH
    )


class Ring:
    def __init__(self, i, up, down, span, src, add, bufs, sends, recvs):
        lo, hi = span
        mid = lo + (hi - lo + 1) // 2
        far, near, got, total = bufs
        at = lambda j: mod(i + j, 4)
        self.i, self.add, self.bufs, self.halves = i, add, bufs, []
        for s, (a, b, long, short, j) in enumerate(((lo, mid, up, down, 3), (mid, hi, down, up, 1))):
            if a == b:
                continue
            cut = lambda ref: ref.at[a:b]
            self.halves.append((
                a, b, at(4 - j),
                rcopy(src(at(2), a, b), cut(far), sends.at[3 * s], recvs.at[3 * s], long),
                rcopy(src(at(j), a, b), cut(near), sends.at[3 * s + 1], recvs.at[3 * s + 1], short),
                rcopy(cut(total), cut(got), sends.at[3 * s + 2], recvs.at[3 * s + 2], long),
            ))

    def start(self):
        for h in self.halves:
            h[3].start()
        for h in self.halves:
            h[4].start()

    def pass_on(self):
        far, _, _, total = self.bufs
        for a, b, to, one, _, on in self.halves:
            one.wait_recv()

            @pl.loop(a, b)
            def _(m):
                total[m] = (far[m].astype(F32) + self.add(to, m)).astype(BF16)

            on.start()

    def result(self, put):
        _, near, got, _ = self.bufs
        for a, b, _, _, two, on in self.halves:
            two.wait_recv()
            on.wait_recv()

            @pl.loop(a, b)
            def _(m):
                put(m, self.add(self.i, m) + (near[m].astype(F32) + got[m].astype(F32)))

    def drain(self):
        for h in self.halves:
            for c in h[3:]:
                c.wait_send()


def kernel(
    g, out, gown, gsib, psend, zrel, zrec, sline, own, t, l1, l2, xf, xb, o, u,
    lsem, csend, crecv, rsend, rrecv, fsend, frecv, dsem,
):
    rep, x, col = lax.axis_index("rep"), lax.axis_index("row"), lax.axis_index("col")
    zh, k = lax.div(rep, 2), mod(rep, 2)
    zl, y = lax.div(col, 4), mod(col, 4)
    z = 2 * zh + zl
    q, d = psend.shape
    half = q // 2
    bs = BLOCK
    b4 = bs // 4

    def dev(x, y, z, k):
        return {"rep": lax.div(z, 2) * 2 + k, "row": x, "col": mod(z, 2) * 4 + y}

    sib = dev(x, y, z, 1 - k)
    zp, zm = dev(x, y, mod(z + 1, 4), k), dev(x, y, mod(z + 3, 4), k)
    yp, ym = dev(x, mod(y + 1, 4), z, k), dev(x, mod(y + 3, 4), z, k)
    xp, xm = dev(mod(x + 1, 4), y, z, k), dev(mod(x + 3, 4), y, z, k)

    def cols(c):
        return slice(STARTS[c] * bs, (STARTS[c] + WIDTHS[c]) * bs)

    def rows(i):
        return pl.ds(pl.multiple_of(i * q, q), q)

    def load(c):
        return pltpu.make_async_copy(g.at[:, k, :, cols(c)], gown.at[:, :, cols(c)], lsem.at[c])

    def swap(c):
        return rcopy(g.at[:, 1 - k, :, cols(c)], gsib.at[:, :, cols(c)], csend.at[0], crecv.at[0, c], sib)

    def z1(c):
        return (
            rcopy(psend.at[0:half, cols(c)], zrel.at[0, :, cols(c)], csend.at[1], crecv.at[1, c], zp),
            rcopy(psend.at[half:q, cols(c)], zrel.at[1, :, cols(c)], csend.at[2], crecv.at[2, c], zm),
        )

    def z2(c):
        return (
            rcopy(zrel.at[0, :, cols(c)], zrec.at[0, :, cols(c)], csend.at[3], crecv.at[3, c], zp),
            rcopy(zrel.at[1, :, cols(c)], zrec.at[1, :, cols(c)], csend.at[4], crecv.at[4, c], zm),
        )

    def block(j, c, part=None):
        base = (2 * mod(y + j, 4) + k) * q
        if part is None:
            return sline.at[pl.ds(pl.multiple_of(base, q), q), cols(c)]
        return sline.at[pl.ds(pl.multiple_of(base + part * half, half), half), cols(c)]

    def sblock(j, c):
        return sline.at[pl.ds(pl.multiple_of((2 * mod(y + j, 4) + 1 - k) * q, q), q), cols(c)]

    def y1(c):
        own = block(0, c)
        return (
            rcopy(own, own, csend.at[5], crecv.at[5, c], yp),
            rcopy(own, own, csend.at[6], crecv.at[6, c], ym),
        )

    def y1_landed(c):
        down, upper = block(3, c), block(1, c)
        return (
            rcopy(down, down, csend.at[5], crecv.at[5, c], yp),
            rcopy(upper, upper, csend.at[6], crecv.at[6, c], ym),
        )

    def y2(c):
        down, upper = block(3, c, 0), block(1, c, 1)
        return (
            rcopy(down, down, csend.at[7], crecv.at[7, c], yp),
            rcopy(upper, upper, csend.at[8], crecv.at[8, c], ym),
        )

    def y2_landed(c):
        lo, hi = block(2, c, 0), block(2, c, 1)
        return (
            rcopy(lo, lo, csend.at[7], crecv.at[7, c], yp),
            rcopy(hi, hi, csend.at[8], crecv.at[8, c], ym),
        )

    def share(j, c):
        blk = block(j, c)
        return rcopy(blk, blk, csend.at[9 + j], crecv.at[9 + j, c], sib)

    def share_landed(j, c):
        blk = sblock(j, c)
        return rcopy(blk, blk, csend.at[9 + j], crecv.at[9 + j, c], sib)

    for c in range(CHUNKS):
        load(c).start()
        swap(c).start()
    own[...] = jnp.zeros_like(own)

    def gather_step(step):
        c = step
        if c < CHUNKS:
            load(c).wait()
            swap(c).wait_recv()
            away = 1 - zh
            psend[:, cols(c)] = (gown[away, :, cols(c)].astype(F32) + gsib[away, :, cols(c)].astype(F32)).astype(BF16)
            for cp in z1(c):
                cp.start()
        c = step - 1
        if 0 <= c < CHUNKS:
            for cp, fwd in zip(z1(c), z2(c)):
                cp.wait_recv()
                fwd.start()
        c = step - 2
        if 0 <= c < CHUNKS:
            for cp in z2(c):
                cp.wait_recv()
            own = gown[zh, :, cols(c)].astype(F32) + gsib[zh, :, cols(c)].astype(F32)
            far = jnp.concatenate([zrec[0, :, cols(c)], zrec[1, :, cols(c)]], axis=0).astype(F32)
            sline[rows(2 * y + k), cols(c)] = (own + far).astype(BF16)
            for cp in y1(c):
                cp.start()
            share(0, c).start()
        c = step - 3
        if 0 <= c < CHUNKS:
            for cp, fwd, j in zip(y1_landed(c), y2(c), (3, 1)):
                cp.wait_recv()
                fwd.start()
                share(j, c).start()
        c = step - 4
        if 0 <= c < CHUNKS:
            for cp in y2_landed(c):
                cp.wait_recv()
            share(2, c).start()

    strip = 2 * y + k

    def tiles(n):
        for c in range(CHUNKS):
            if STARTS[c] // 4 == n:
                for j in range(4):
                    share_landed(j, c).wait_recv()
        last = n // 2

        @pl.when((strip >= 4) if n % 2 else (strip < 4))
        def _():
            mine = pl.ds(pl.multiple_of((8 * last + strip) * bs, bs), bs)
            own[:, last * bs : (last + 1) * bs] = sline[:, mine]

        lhs = sline[:, 4 * n * bs : 4 * (n + 1) * bs]
        acc = lax.dot_general(
            lhs, own[:, : count(n) * bs], (((0,), (0,)), ((), ())), preferred_element_type=F32
        )
        for m in range(count(n)):
            for p in range(4):
                t[first(n) + m, p] = acc[p * bs : (p + 1) * bs, m * bs : (m + 1) * bs].astype(BF16)

    def quarter(v):
        return pl.ds(pl.multiple_of(v * b4, b4), b4)

    parts = []
    for n in range(STAGES):
        a, b = first(n), first(n + 1)
        h = b if n < BETA_FROM else a + (b - a + 1) // 2
        parts.append([(a, h, True)] + ([(h, b, False)] if h < b else []))
    rings1, rings2, used = [], [], 0
    for n in range(STAGES):
        ones, twos = [], []
        for a, b, x_first in parts[n]:
            along = ((x, xp, xm), (z, zp, zm))
            one, two = along if x_first else along[::-1]
            ones.append(Ring(
                *one, (a, b),
                lambda p, a, b: t.at[a:b, p],
                lambda p, m: t[m, p].astype(F32),
                [l1.at[i] for i in range(4)],
                rsend.at[0, used], rrecv.at[0, used],
            ))
            twos.append(Ring(
                *two, (a, b),
                lambda v, a, b: xb.at[a:b, quarter(v), :],
                lambda v, m: xf[m, quarter(v), :],
                [l2.at[i] for i in range(4)],
                rsend.at[1, used], rrecv.at[1, used],
            ))
            used += 1
        rings1.append(ones)
        rings2.append(twos)

    def exchange(n, begin):
        for a, b, x_first in parts[n]:
            p1, p2 = (x, z) if x_first else (z, x)
            rblk = 4 * n + p1

            def one(f, up, side):
                m = f - first(n)
                cblk = 8 * m + strip
                stage = lax.div(cblk, 4)
                wanted = (stage <= n) if side == 0 else (stage < n)
                rr, cc = (rblk, cblk) if side == 0 else (cblk, rblk)
                tx, tc = lax.div(rr, 12), lax.div(cc, 6)
                src = o.at[f]
                dst = u.at[mod(rr, 12), mod(cc, 6), quarter(p2), :]
                ty, tz = mod(tc, 4), 2 * up + lax.div(tc, 4)
                mine = (tx == x) & (ty == y) & (tz == z)

                @pl.when(wanted & jnp.logical_not(mine))
                def _():
                    cp = rcopy(src, dst, fsend.at[f, 2 * side + up], frecv.at[0], dev(tx, ty, tz, k))
                    if begin:
                        cp.start()
                    else:
                        cp.wait_send()

                if begin:

                    @pl.when(wanted & mine)
                    def _():
                        pltpu.make_async_copy(src, dst, frecv.at[0]).start()

            @pl.loop(a, b)
            def _(f):
                for side in (0, 1):
                    for up in (0, 1):
                        one(f, up, side)

    def begin(n):
        tiles(n)
        for r in rings1[n]:
            r.start()

    def pass1(n):
        for r in rings1[n]:
            r.pass_on()

    def reduce1(n):
        def put(m, v):
            xf[m] = v
            xb[m] = v.astype(BF16)

        for r, r2 in zip(rings1[n], rings2[n]):
            r.result(put)
            r2.start()

    def pass2(n):
        for r in rings2[n]:
            r.pass_on()

    def reduce2(n):
        def put(m, v):
            o[m] = v.astype(BF16)

        for r in rings2[n]:
            r.result(put)
        exchange(n, True)

    plan = {}
    for n in range(STAGES):
        step = n + 7
        for after, what in ((0, begin), (1 if n < 7 else 2, pass1), (2, reduce1), (1, pass2), (1, reduce2)):
            step += after
            plan.setdefault(step, []).append((what, n))
    for step in range(max(plan) + 1):
        gather_step(step)
        for what, n in plan.get(step, ()):
            what(n)

    def sent(n, ref):
        rcopy(ref, ref, csend.at[n], crecv.at[0, 0], sib).wait_send()

    sent(0, gsib)
    for n in (1, 2, 3, 4):
        sent(n, zrel.at[0])
    for n in (5, 6, 9, 10, 11, 12):
        sent(n, psend)
    for n in (7, 8):
        sent(n, zrel.at[0])

    for n in range(STAGES):
        for r in rings1[n] + rings2[n]:
            r.drain()

    whole = u.at[0:6]
    rcopy(whole, whole, dsem.at[0], frecv.at[0], sib).wait_recv()

    @pl.loop(0, 12)
    def _(i):
        for j in range(6):
            direct = lax.div(12 * x + i, 4) >= lax.div(6 * col + j, 4)
            from_me = jnp.where(direct, j % 2, mod(i, 2)) == k

            @pl.when(from_me)
            def _():
                rcopy(u.at[i, j], u.at[i, j], dsem.at[0], dsem.at[1], sib).start()

    for n in range(STAGES):
        exchange(n, False)
    rcopy(whole, whole, dsem.at[0], dsem.at[1], sib).wait_recv()
    rcopy(whole, whole, dsem.at[0], dsem.at[1], sib).wait_send()
    whole_out = pltpu.make_async_copy(u, out, lsem.at[0])
    whole_out.start()
    whole_out.wait()


def gather_blocks(grad):
    _, n, d = grad.shape
    q, bs = n // 4, BLOCK
    b4 = bs // 4
    subs = STAGES + STAGES - BETA_FROM
    vm = pltpu.VMEM
    dma = pltpu.SemaphoreType.DMA
    return pl.pallas_call(
        kernel,
        out_shape=jax.ShapeDtypeStruct((12, 6, bs, bs), BF16),
        in_specs=[pl.BlockSpec(memory_space=pl.ANY)],
        out_specs=pl.BlockSpec(memory_space=pl.ANY),
        scratch_shapes=[
            vm((2, q, d), BF16), vm((2, q, d), BF16), vm((q, d), BF16),
            vm((2, q // 2, d), BF16), vm((2, q // 2, d), BF16),
            vm((8 * q, d), BF16), vm((8 * q, d // 8), BF16), vm((TOTAL, 4, bs, bs), BF16),
            vm((4, TOTAL, bs, bs), BF16), vm((4, TOTAL, b4, bs), BF16),
            vm((TOTAL, bs, bs), F32), vm((TOTAL, bs, bs), BF16),
            vm((TOTAL, b4, bs), BF16), vm((12, 6, bs, bs), BF16),
            dma((CHUNKS,)), dma((13,)), dma((13, CHUNKS)), dma((2, subs, 6)), dma((2, subs, 6)),
            dma((TOTAL, 4)), dma((1,)), dma((2,)),
        ],
        compiler_params=pltpu.CompilerParams(has_side_effects=True, vmem_limit_bytes=56 * 1024 * 1024),
    )(grad.reshape(2, 2, q, d))


GROUP = 2


def finish(blocks, statistic, gram, following):
    i0 = pl.program_id(0) * GROUP
    row0, col0 = 12 * lax.axis_index("row"), 6 * lax.axis_index("col")
    n = blocks.shape[-1]
    for i in range(GROUP):
        for j in range(6):
            direct = lax.div(row0 + i0 + i, 4) >= lax.div(col0 + j, 4)
            at = (slice(i * n, (i + 1) * n), slice(j * n, (j + 1) * n))

            @pl.when(direct)
            def _():
                gram[at] = blocks[i, j].astype(F32)

            @pl.when(jnp.logical_not(direct))
            def _():
                gram[at] = blocks[i, j].astype(F32).T

    following[...] = 0.95 * statistic[...] + 0.05 * gram[...]


def shards(grad, statistic):
    blocks = gather_blocks(grad)
    n = blocks.shape[-1]
    tile = pl.BlockSpec((GROUP * n, 6 * n), lambda i: (i, 0))
    shape = jax.ShapeDtypeStruct(statistic.shape, F32)
    return pl.pallas_call(
        finish,
        grid=(12 // GROUP,),
        out_shape=(shape, shape),
        in_specs=[pl.BlockSpec((GROUP, 6, n, n), lambda i: (i, 0, 0, 0)), tile],
        out_specs=(tile, tile),
    )(blocks, statistic)


def solution(mesh):
    return jax.shard_map(
        shards,
        mesh=mesh,
        in_specs=(P("rep", ("row", "col"), None), P("row", "col")),
        out_specs=(P("row", "col"), P("row", "col")),
        check_vma=False,
    )
```

```python
import functools

import jax
import jax.numpy as jnp
from jax import lax
from jax.experimental import pallas as pl
from jax.experimental.pallas import tpu as pltpu
from jax.sharding import PartitionSpec as P

MESH = pl.DeviceIdType.MESH
BF16 = jnp.bfloat16
F32 = jnp.float32
BLOCK = 128
STAGES = 12
WIDTHS = (4,) * 12
STARTS = tuple(sum(WIDTHS[:i]) for i in range(len(WIDTHS)))
CHUNKS = len(WIDTHS)
BETA_FROM = 8


def count(n):
    return n // 2 + 1


def first(n):
    return sum(count(i) for i in range(n))


TOTAL = first(STAGES)


def mod(a, n):
    return lax.rem(a, n)


def rcopy(src, dst, send, recv, device):
    return pltpu.make_async_remote_copy(
        src_ref=src, dst_ref=dst, send_sem=send, recv_sem=recv, device_id=device, device_id_type=MESH
    )


class Ring:
    def __init__(self, i, up, down, span, src, add, bufs, sends, recvs):
        lo, hi = span
        mid = lo + (hi - lo + 1) // 2
        far, near, got, total = bufs
        at = lambda j: mod(i + j, 4)
        self.i, self.add, self.bufs, self.halves = i, add, bufs, []
        for s, (a, b, long, short, j) in enumerate(((lo, mid, up, down, 3), (mid, hi, down, up, 1))):
            if a == b:
                continue
            cut = lambda ref: ref.at[a:b]
            self.halves.append((
                a, b, at(4 - j),
                rcopy(src(at(2), a, b), cut(far), sends.at[3 * s], recvs.at[3 * s], long),
                rcopy(src(at(j), a, b), cut(near), sends.at[3 * s + 1], recvs.at[3 * s + 1], short),
                rcopy(cut(total), cut(got), sends.at[3 * s + 2], recvs.at[3 * s + 2], long),
            ))

    def start(self):
        for h in self.halves:
            h[3].start()
        for h in self.halves:
            h[4].start()

    def pass_on(self):
        far, _, _, total = self.bufs
        for a, b, to, one, _, on in self.halves:
            one.wait_recv()

            @pl.loop(a, b)
            def _(m):
                total[m] = (far[m].astype(F32) + self.add(to, m)).astype(BF16)

            on.start()

    def result(self, put):
        _, near, got, _ = self.bufs
        for a, b, _, _, two, on in self.halves:
            two.wait_recv()
            on.wait_recv()

            @pl.loop(a, b)
            def _(m):
                put(m, self.add(self.i, m) + (near[m].astype(F32) + got[m].astype(F32)))

    def drain(self):
        for h in self.halves:
            for c in h[3:]:
                c.wait_send()


def kernel(
    g, out, gown, gsib, psend, zrel, zrec, sline, own, t, l1, l2, xf, xb, o, u,
    lsem, csend, crecv, rsend, rrecv, fsend, frecv, dsem,
):
    rep, x, col = lax.axis_index("rep"), lax.axis_index("row"), lax.axis_index("col")
    zh, k = lax.div(rep, 2), mod(rep, 2)
    zl, y = lax.div(col, 4), mod(col, 4)
    z = 2 * zh + zl
    q, d = psend.shape
    half = q // 2
    bs = BLOCK
    b4 = bs // 4

    def dev(x, y, z, k):
        return {"rep": lax.div(z, 2) * 2 + k, "row": x, "col": mod(z, 2) * 4 + y}

    sib = dev(x, y, z, 1 - k)
    zp, zm = dev(x, y, mod(z + 1, 4), k), dev(x, y, mod(z + 3, 4), k)
    yp, ym = dev(x, mod(y + 1, 4), z, k), dev(x, mod(y + 3, 4), z, k)
    xp, xm = dev(mod(x + 1, 4), y, z, k), dev(mod(x + 3, 4), y, z, k)

    def cols(c):
        return slice(STARTS[c] * bs, (STARTS[c] + WIDTHS[c]) * bs)

    def rows(i):
        return pl.ds(pl.multiple_of(i * q, q), q)

    def strided(c):
        return [(pl.ds((c + STAGES * i) * bs, bs), pl.ds((4 * c + i) * bs, bs)) for i in range(4)]

    def load(c):
        for there, here in strided(c):
            pltpu.make_async_copy(g.at[:, k, :, there], gown.at[:, :, here], lsem.at[c]).start()

    def swap(c):
        for there, here in strided(c):
            rcopy(g.at[:, 1 - k, :, there], gsib.at[:, :, here], csend.at[0], crecv.at[0, c], sib).start()

    def loaded(c):
        whole = gown.at[:, :, cols(c)]
        pltpu.make_async_copy(whole, whole, lsem.at[c]).wait()
        whole = gsib.at[:, :, cols(c)]
        rcopy(whole, whole, csend.at[0], crecv.at[0, c], sib).wait_recv()

    def z1(c):
        return (
            rcopy(psend.at[0:half, cols(c)], zrel.at[0, :, cols(c)], csend.at[1], crecv.at[1, c], zp),
            rcopy(psend.at[half:q, cols(c)], zrel.at[1, :, cols(c)], csend.at[2], crecv.at[2, c], zm),
        )

    def z2(c):
        return (
            rcopy(zrel.at[0, :, cols(c)], zrec.at[0, :, cols(c)], csend.at[3], crecv.at[3, c], zp),
            rcopy(zrel.at[1, :, cols(c)], zrec.at[1, :, cols(c)], csend.at[4], crecv.at[4, c], zm),
        )

    def block(j, c, part=None):
        base = (2 * mod(y + j, 4) + k) * q
        if part is None:
            return sline.at[pl.ds(pl.multiple_of(base, q), q), cols(c)]
        return sline.at[pl.ds(pl.multiple_of(base + part * half, half), half), cols(c)]

    def sblock(j, c):
        return sline.at[pl.ds(pl.multiple_of((2 * mod(y + j, 4) + 1 - k) * q, q), q), cols(c)]

    def y1(c):
        own = block(0, c)
        return (
            rcopy(own, own, csend.at[5], crecv.at[5, c], yp),
            rcopy(own, own, csend.at[6], crecv.at[6, c], ym),
        )

    def y1_landed(c):
        down, upper = block(3, c), block(1, c)
        return (
            rcopy(down, down, csend.at[5], crecv.at[5, c], yp),
            rcopy(upper, upper, csend.at[6], crecv.at[6, c], ym),
        )

    def y2(c):
        down, upper = block(3, c, 0), block(1, c, 1)
        return (
            rcopy(down, down, csend.at[7], crecv.at[7, c], yp),
            rcopy(upper, upper, csend.at[8], crecv.at[8, c], ym),
        )

    def y2_landed(c):
        lo, hi = block(2, c, 0), block(2, c, 1)
        return (
            rcopy(lo, lo, csend.at[7], crecv.at[7, c], yp),
            rcopy(hi, hi, csend.at[8], crecv.at[8, c], ym),
        )

    def share(j, c):
        blk = block(j, c)
        return rcopy(blk, blk, csend.at[9 + j], crecv.at[9 + j, c], sib)

    def share_landed(j, c):
        blk = sblock(j, c)
        return rcopy(blk, blk, csend.at[9 + j], crecv.at[9 + j, c], sib)

    for c in range(CHUNKS):
        load(c)
        swap(c)
    own[...] = jnp.zeros_like(own)

    def gather_step(step):
        c = step
        if c < CHUNKS:
            loaded(c)
            away = 1 - zh
            psend[:, cols(c)] = (gown[away, :, cols(c)].astype(F32) + gsib[away, :, cols(c)].astype(F32)).astype(BF16)
            for cp in z1(c):
                cp.start()
        c = step - 1
        if 0 <= c < CHUNKS:
            for cp, fwd in zip(z1(c), z2(c)):
                cp.wait_recv()
                fwd.start()
        c = step - 2
        if 0 <= c < CHUNKS:
            for cp in z2(c):
                cp.wait_recv()
            own = gown[zh, :, cols(c)].astype(F32) + gsib[zh, :, cols(c)].astype(F32)
            far = jnp.concatenate([zrec[0, :, cols(c)], zrec[1, :, cols(c)]], axis=0).astype(F32)
            sline[rows(2 * y + k), cols(c)] = (own + far).astype(BF16)
            for cp in y1(c):
                cp.start()
            share(0, c).start()
        c = step - 3
        if 0 <= c < CHUNKS:
            for cp, fwd, j in zip(y1_landed(c), y2(c), (3, 1)):
                cp.wait_recv()
                fwd.start()
                share(j, c).start()
        c = step - 4
        if 0 <= c < CHUNKS:
            for cp in y2_landed(c):
                cp.wait_recv()
            share(2, c).start()

    turn = 2 * mod(y, 2) + lax.div(y, 2)
    strip = 4 * k + turn

    def tiles(n):
        for c in range(CHUNKS):
            if STARTS[c] // 4 == n:
                for j in range(4):
                    share_landed(j, c).wait_recv()
        last = n // 2

        @pl.when(k == n % 2)
        def _():
            mine = pl.ds(pl.multiple_of((8 * last + strip) * bs, bs), bs)
            own[:, last * bs : (last + 1) * bs] = sline[:, mine]

        lhs = sline[:, 4 * n * bs : 4 * (n + 1) * bs]
        acc = lax.dot_general(
            lhs, own[:, : count(n) * bs], (((0,), (0,)), ((), ())), preferred_element_type=F32
        )
        for m in range(count(n)):
            for p in range(4):
                t[first(n) + m, p] = acc[p * bs : (p + 1) * bs, m * bs : (m + 1) * bs].astype(BF16)

    def quarter(v):
        return pl.ds(pl.multiple_of(v * b4, b4), b4)

    parts = []
    for n in range(STAGES):
        a, b = first(n), first(n + 1)
        h = b if n < BETA_FROM else a + (b - a + 1) // 2
        parts.append([(a, h, True)] + ([(h, b, False)] if h < b else []))
    rings1, rings2, used = [], [], 0
    for n in range(STAGES):
        ones, twos = [], []
        for a, b, x_first in parts[n]:
            along = ((x, xp, xm), (z, zp, zm))
            one, two = along if x_first else along[::-1]
            ones.append(Ring(
                *one, (a, b),
                lambda p, a, b: t.at[a:b, p],
                lambda p, m: t[m, p].astype(F32),
                [l1.at[i] for i in range(4)],
                rsend.at[0, used], rrecv.at[0, used],
            ))
            twos.append(Ring(
                *two, (a, b),
                lambda v, a, b: xb.at[a:b, quarter(v), :],
                lambda v, m: xf[m, quarter(v), :],
                [l2.at[i] for i in range(4)],
                rsend.at[1, used], rrecv.at[1, used],
            ))
            used += 1
        rings1.append(ones)
        rings2.append(twos)

    def exchange(n, begin):
        for a, b, x_first in parts[n]:
            p1, p2 = (x, z) if x_first else (z, x)
            rblk = n + STAGES * p1

            def one(f, up, side):
                m = f - first(n)
                stage = 2 * m + k
                cblk = stage + STAGES * turn
                wanted = (stage <= n) if side == 0 else (stage < n)
                rr, cc = (rblk, cblk) if side == 0 else (cblk, rblk)
                tx, tc = lax.div(rr, 12), lax.div(cc, 6)
                src = o.at[f]
                dst = u.at[mod(rr, 12), mod(cc, 6), quarter(p2), :]
                ty, tz = mod(tc, 4), 2 * up + lax.div(tc, 4)
                mine = (tx == x) & (ty == y) & (tz == z)

                @pl.when(wanted & jnp.logical_not(mine))
                def _():
                    cp = rcopy(src, dst, fsend.at[f, 2 * side + up], frecv.at[0], dev(tx, ty, tz, k))
                    if begin:
                        cp.start()
                    else:
                        cp.wait_send()

                if begin:

                    @pl.when(wanted & mine)
                    def _():
                        pltpu.make_async_copy(src, dst, frecv.at[0]).start()

            @pl.loop(a, b)
            def _(f):
                for side in (0, 1):
                    for up in (0, 1):
                        one(f, up, side)

    def begin(n):
        tiles(n)
        for r in rings1[n]:
            r.start()

    def pass1(n):
        for r in rings1[n]:
            r.pass_on()

    def reduce1(n):
        def put(m, v):
            xf[m] = v
            xb[m] = v.astype(BF16)

        for r, r2 in zip(rings1[n], rings2[n]):
            r.result(put)
            r2.start()

    def pass2(n):
        for r in rings2[n]:
            r.pass_on()

    def reduce2(n):
        def put(m, v):
            o[m] = v.astype(BF16)

        for r in rings2[n]:
            r.result(put)
        exchange(n, True)

    plan = {}
    for n in range(STAGES):
        step = n + 5
        for after, what in ((0, begin), (1 if n < 7 else 2, pass1), (2, reduce1), (1, pass2), (1, reduce2)):
            step += after
            plan.setdefault(step, []).append((what, n))
    for step in range(max(plan) + 1):
        gather_step(step)
        for what, n in plan.get(step, ()):
            what(n)

    def sent(n, ref):
        rcopy(ref, ref, csend.at[n], crecv.at[0, 0], sib).wait_send()

    sent(0, gsib)
    for n in (1, 2, 3, 4):
        sent(n, zrel.at[0])
    for n in (5, 6, 9, 10, 11, 12):
        sent(n, psend)
    for n in (7, 8):
        sent(n, zrel.at[0])

    for n in range(STAGES):
        for r in rings1[n] + rings2[n]:
            r.drain()

    sized = (l1.at[0, 0:39], l1.at[0, 0:33])
    for core in (0, 1):

        @pl.when(k == core)
        def _():
            rcopy(sized[core], sized[core], dsem.at[0], frecv.at[0], sib).wait_recv()

    @pl.loop(0, 12)
    def _(i):
        for j in range(6):
            direct = i >= 6 * mod(col, 2) + j
            from_me = jnp.where(direct, j % 2, mod(i, 2)) == k

            @pl.when(from_me)
            def _():
                rcopy(u.at[i, j], u.at[i, j], dsem.at[0], dsem.at[1], sib).start()

    for n in range(STAGES):
        exchange(n, False)
    for core in (0, 1):

        @pl.when(k == core)
        def _():
            rcopy(sized[1 - core], sized[1 - core], dsem.at[0], dsem.at[1], sib).wait_recv()
            rcopy(sized[core], sized[core], dsem.at[0], dsem.at[1], sib).wait_send()

    whole_out = pltpu.make_async_copy(u, out, lsem.at[0])
    whole_out.start()
    whole_out.wait()


def gather_blocks(grad):
    _, n, d = grad.shape
    q, bs = n // 4, BLOCK
    b4 = bs // 4
    subs = STAGES + STAGES - BETA_FROM
    vm = pltpu.VMEM
    dma = pltpu.SemaphoreType.DMA
    return pl.pallas_call(
        kernel,
        out_shape=jax.ShapeDtypeStruct((12, 6, bs, bs), BF16),
        in_specs=[pl.BlockSpec(memory_space=pl.ANY)],
        out_specs=pl.BlockSpec(memory_space=pl.ANY),
        scratch_shapes=[
            vm((2, q, d), BF16), vm((2, q, d), BF16), vm((q, d), BF16),
            vm((2, q // 2, d), BF16), vm((2, q // 2, d), BF16),
            vm((8 * q, d), BF16), vm((8 * q, d // 8), BF16), vm((TOTAL, 4, bs, bs), BF16),
            vm((4, TOTAL, bs, bs), BF16), vm((4, TOTAL, b4, bs), BF16),
            vm((TOTAL, bs, bs), F32), vm((TOTAL, bs, bs), BF16),
            vm((TOTAL, b4, bs), BF16), vm((12, 6, bs, bs), BF16),
            dma((CHUNKS,)), dma((13,)), dma((13, CHUNKS)), dma((2, subs, 6)), dma((2, subs, 6)),
            dma((TOTAL, 4)), dma((1,)), dma((2,)),
        ],
        compiler_params=pltpu.CompilerParams(has_side_effects=True, vmem_limit_bytes=56 * 1024 * 1024),
    )(grad.reshape(2, 2, q, d))


GROUP = 2


def finish(blocks, statistic, gram, following):
    i0 = pl.program_id(0) * GROUP
    col0 = 6 * mod(lax.axis_index("col"), 2)
    n = blocks.shape[-1]
    for i in range(GROUP):
        for j in range(6):
            direct = i0 + i >= col0 + j
            at = (slice(i * n, (i + 1) * n), slice(j * n, (j + 1) * n))

            @pl.when(direct)
            def _():
                gram[at] = blocks[i, j].astype(F32)

            @pl.when(jnp.logical_not(direct))
            def _():
                gram[at] = blocks[i, j].astype(F32).T

    following[...] = 0.95 * statistic[...] + 0.05 * gram[...]


def shards(grad, statistic):
    blocks = gather_blocks(grad)
    n = blocks.shape[-1]
    tile = pl.BlockSpec((GROUP * n, 6 * n), lambda i: (i, 0))
    shape = jax.ShapeDtypeStruct(statistic.shape, F32)
    return pl.pallas_call(
        finish,
        grid=(12 // GROUP,),
        out_shape=(shape, shape),
        in_specs=[pl.BlockSpec((GROUP, 6, n, n), lambda i: (i, 0, 0, 0)), tile],
        out_specs=(tile, tile),
    )(blocks, statistic)


def solution(mesh):
    return jax.shard_map(
        shards,
        mesh=mesh,
        in_specs=(P("rep", ("row", "col"), None), P("row", "col")),
        out_specs=(P("row", "col"), P("row", "col")),
        check_vma=False,
    )
```

```python
import functools

import jax
import jax.numpy as jnp
from jax import lax
from jax.experimental import pallas as pl
from jax.experimental.pallas import tpu as pltpu
from jax.sharding import PartitionSpec as P

MESH = pl.DeviceIdType.MESH
BF16 = jnp.bfloat16
F32 = jnp.float32
BLOCK = 128
STAGES = 12
WIDTHS = (4,) * 12
STARTS = tuple(sum(WIDTHS[:i]) for i in range(len(WIDTHS)))
CHUNKS = len(WIDTHS)
BETA_FROM = 8


def count(n):
    return n // 2 + 1


def first(n):
    return sum(count(i) for i in range(n))


TOTAL = first(STAGES)


def mod(a, n):
    return lax.rem(a, n)


def rcopy(src, dst, send, recv, device):
    return pltpu.make_async_remote_copy(
        src_ref=src, dst_ref=dst, send_sem=send, recv_sem=recv, device_id=device, device_id_type=MESH
    )


class Ring:
    def __init__(self, i, up, down, span, src, add, bufs, pair, sends, recvs):
        lo, hi = span
        mid = lo + (hi - lo + 1) // 2
        far, near, got, total = bufs
        at = lambda j: mod(i + j, 4)
        self.i, self.add, self.bufs, self.halves = i, add, bufs, []
        self.span, self.last, self.pair, self.up = span, recvs.at[2], pair, up
        for s, (a, b, long, short, j) in enumerate(((lo, mid, up, down, 3), (mid, hi, down, up, 1))):
            if a == b:
                continue
            cut = lambda ref: ref.at[a:b]
            self.halves.append((
                a, b, at(4 - j),
                rcopy(src(at(2), a, b), cut(far), sends.at[s], recvs.at[s], long),
                rcopy(src(at(j), a, b), cut(near), sends.at[s], recvs.at[2], short),
                rcopy(cut(total), cut(got), sends.at[s], recvs.at[2], long),
            ))

    def start(self):
        for h in self.halves:
            h[3].start()
        for h in self.halves:
            h[4].start()

    def pass_on(self):
        far, _, _, total = self.bufs
        for a, b, to, one, _, on in self.halves:
            one.wait_recv()

            @pl.loop(a, b)
            def _(m):
                total[m] = (far[m].astype(F32) + self.add(to, m)).astype(BF16)

            on.start()

    def result(self, put):
        _, near, got, _ = self.bufs
        both = self.pair.at[:, self.span[0] : self.span[1]]
        rcopy(both, both, self.last, self.last, self.up).wait_recv()
        for a, b, *_ in self.halves:

            @pl.loop(a, b)
            def _(m):
                put(m, self.add(self.i, m) + (near[m].astype(F32) + got[m].astype(F32)))


def kernel(
    g, out, gown, gsib, psend, zrel, zrec, sline, own, t, l1, l2, xf, xb, o, u, spare,
    lsem, csend, crecv, rsend, rrecv, fsem, dsem,
):
    rep, x, col = lax.axis_index("rep"), lax.axis_index("row"), lax.axis_index("col")
    zh, k = lax.div(rep, 2), mod(rep, 2)
    zl, y = lax.div(col, 4), mod(col, 4)
    z = 2 * zh + zl
    q, d = psend.shape
    half = q // 2
    bs = BLOCK
    b4 = bs // 4

    def dev(x, y, z, k):
        return {"rep": lax.div(z, 2) * 2 + k, "row": x, "col": mod(z, 2) * 4 + y}

    sib = dev(x, y, z, 1 - k)
    zp, zm = dev(x, y, mod(z + 1, 4), k), dev(x, y, mod(z + 3, 4), k)
    yp, ym = dev(x, mod(y + 1, 4), z, k), dev(x, mod(y + 3, 4), z, k)
    xp, xm = dev(mod(x + 1, 4), y, z, k), dev(mod(x + 3, 4), y, z, k)

    def cols(c):
        return slice(STARTS[c] * bs, (STARTS[c] + WIDTHS[c]) * bs)

    def rows(i):
        return pl.ds(pl.multiple_of(i * q, q), q)

    def strided(c):
        return [(pl.ds((c + STAGES * i) * bs, bs), pl.ds((4 * c + i) * bs, bs)) for i in range(4)]

    def load(c):
        for there, here in strided(c):
            pltpu.make_async_copy(g.at[:, k, :, there], gown.at[:, :, here], lsem.at[c]).start()

    def swap(c):
        for there, here in strided(c):
            rcopy(g.at[:, 1 - k, :, there], gsib.at[:, :, here], csend.at[0], crecv.at[0, c], sib).start()

    def loaded(c):
        whole = gown.at[:, :, cols(c)]
        pltpu.make_async_copy(whole, whole, lsem.at[c]).wait()
        whole = gsib.at[:, :, cols(c)]
        rcopy(whole, whole, csend.at[0], crecv.at[0, c], sib).wait_recv()

    def z1(c):
        return (
            rcopy(psend.at[0:half, cols(c)], zrel.at[0, :, cols(c)], csend.at[1], crecv.at[1, c], zp),
            rcopy(psend.at[half:q, cols(c)], zrel.at[1, :, cols(c)], csend.at[2], crecv.at[2, c], zm),
        )

    def z2(c):
        return (
            rcopy(zrel.at[0, :, cols(c)], zrec.at[0, :, cols(c)], csend.at[3], crecv.at[3, c], zp),
            rcopy(zrel.at[1, :, cols(c)], zrec.at[1, :, cols(c)], csend.at[4], crecv.at[4, c], zm),
        )

    def block(j, c, part=None):
        base = (2 * mod(y + j, 4) + k) * q
        if part is None:
            return sline.at[pl.ds(pl.multiple_of(base, q), q), cols(c)]
        return sline.at[pl.ds(pl.multiple_of(base + part * half, half), half), cols(c)]

    def y1(c):
        own = block(0, c)
        return (
            rcopy(own, own, csend.at[5], crecv.at[5, c], yp),
            rcopy(own, own, csend.at[6], crecv.at[6, c], ym),
        )

    def y1_landed(c):
        down, upper = block(3, c), block(1, c)
        return (
            rcopy(down, down, csend.at[5], crecv.at[5, c], yp),
            rcopy(upper, upper, csend.at[6], crecv.at[6, c], ym),
        )

    def y2(c):
        down, upper = block(3, c, 0), block(1, c, 1)
        return (
            rcopy(down, down, csend.at[7], crecv.at[7, c], yp),
            rcopy(upper, upper, csend.at[8], crecv.at[8, c], ym),
        )

    def y2_landed(c):
        lo, hi = block(2, c, 0), block(2, c, 1)
        return (
            rcopy(lo, lo, csend.at[7], crecv.at[7, c], yp),
            rcopy(hi, hi, csend.at[8], crecv.at[8, c], ym),
        )

    def share(j, c):
        blk = block(j, c)
        return rcopy(blk, blk, csend.at[9], crecv.at[9, c], sib)

    def shares_landed(c):
        four = sline.at[0 : 4 * q, cols(c)]
        rcopy(four, four, csend.at[9], crecv.at[9, c], sib).wait_recv()

    for c in range(CHUNKS):
        load(c)
        swap(c)
    own[...] = jnp.zeros_like(own)

    def gather_step(step):
        c = step
        if c < CHUNKS:
            loaded(c)
            away = 1 - zh
            psend[:, cols(c)] = (gown[away, :, cols(c)].astype(F32) + gsib[away, :, cols(c)].astype(F32)).astype(BF16)
            for cp in z1(c):
                cp.start()
        c = step - 1
        if 0 <= c < CHUNKS:
            for cp, fwd in zip(z1(c), z2(c)):
                cp.wait_recv()
                fwd.start()
        c = step - 2
        if 0 <= c < CHUNKS:
            for cp in z2(c):
                cp.wait_recv()
            own = gown[zh, :, cols(c)].astype(F32) + gsib[zh, :, cols(c)].astype(F32)
            far = jnp.concatenate([zrec[0, :, cols(c)], zrec[1, :, cols(c)]], axis=0).astype(F32)
            sline[rows(2 * y + k), cols(c)] = (own + far).astype(BF16)
            for cp in y1(c):
                cp.start()
            share(0, c).start()
        c = step - 3
        if 0 <= c < CHUNKS:
            for cp, fwd, j in zip(y1_landed(c), y2(c), (3, 1)):
                cp.wait_recv()
                fwd.start()
                share(j, c).start()
        c = step - 4
        if 0 <= c < CHUNKS:
            for cp in y2_landed(c):
                cp.wait_recv()
            share(2, c).start()

    turn = 2 * mod(y, 2) + lax.div(y, 2)
    strip = 4 * k + turn

    def tiles(n):
        for c in range(CHUNKS):
            if STARTS[c] // 4 == n:
                shares_landed(c)
        last = n // 2

        @pl.when(k == n % 2)
        def _():
            mine = pl.ds(pl.multiple_of((8 * last + strip) * bs, bs), bs)
            own[:, last * bs : (last + 1) * bs] = sline[:, mine]

        lhs = sline[:, 4 * n * bs : 4 * (n + 1) * bs]
        acc = lax.dot_general(
            lhs, own[:, : count(n) * bs], (((0,), (0,)), ((), ())), preferred_element_type=F32
        )
        for m in range(count(n)):
            for p in range(4):
                t[first(n) + m, p] = acc[p * bs : (p + 1) * bs, m * bs : (m + 1) * bs].astype(BF16)

    def quarter(v):
        return pl.ds(pl.multiple_of(v * b4, b4), b4)

    parts = []
    for n in range(STAGES):
        a, b = first(n), first(n + 1)
        h = b if n < BETA_FROM else a + (b - a + 1) // 2
        parts.append([(a, h, True)] + ([(h, b, False)] if h < b else []))
    rings1, rings2, used = [], [], 0
    for n in range(STAGES):
        ones, twos = [], []
        for a, b, x_first in parts[n]:
            along = ((x, xp, xm), (z, zp, zm))
            one, two = along if x_first else along[::-1]
            ones.append(Ring(
                *one, (a, b),
                lambda p, a, b: t.at[a:b, p],
                lambda p, m: t[m, p].astype(F32),
                [l1.at[i] for i in range(4)],
                l1.at[0:2],
                rsend.at[0], rrecv.at[0, used],
            ))
            twos.append(Ring(
                *two, (a, b),
                lambda v, a, b: xb.at[a:b, quarter(v), :],
                lambda v, m: xf[m, quarter(v), :],
                [l2.at[i] for i in range(4)],
                l2.at[0:2],
                rsend.at[1], rrecv.at[1, used],
            ))
            used += 1
        rings1.append(ones)
        rings2.append(twos)

    def exchange(n):
        for a, b, x_first in parts[n]:
            p1, p2 = (x, z) if x_first else (z, x)
            rblk = n + STAGES * p1

            def one(f, up, side):
                m = f - first(n)
                stage = 2 * m + k
                cblk = stage + STAGES * turn
                wanted = (stage <= n) if side == 0 else (stage < n)
                rr, cc = (rblk, cblk) if side == 0 else (cblk, rblk)
                tx, tc = lax.div(rr, 12), lax.div(cc, 6)
                src = o.at[f]
                dst = u.at[mod(rr, 12), mod(cc, 6), quarter(p2), :]
                ty, tz = mod(tc, 4), 2 * up + lax.div(tc, 4)
                mine = (tx == x) & (ty == y) & (tz == z)

                @pl.when(wanted & jnp.logical_not(mine))
                def _():
                    rcopy(src, dst, fsem.at[0], fsem.at[1], dev(tx, ty, tz, k)).start()

                @pl.when(wanted & mine)
                def _():
                    pltpu.make_async_copy(src, dst, fsem.at[1]).start()
                    pltpu.make_async_copy(src, spare.at[f, 2 * side + up], fsem.at[0]).start()

            @pl.loop(a, b)
            def _(f):
                for side in (0, 1):
                    for up in (0, 1):
                        one(f, up, side)

    def begin(n):
        tiles(n)
        for r in rings1[n]:
            r.start()

    def pass1(n):
        for r in rings1[n]:
            r.pass_on()

    def reduce1(n):
        def put(m, v):
            xf[m] = v
            xb[m] = v.astype(BF16)

        for r, r2 in zip(rings1[n], rings2[n]):
            r.result(put)
            r2.start()

    def pass2(n):
        for r in rings2[n]:
            r.pass_on()

    def reduce2(n):
        def put(m, v):
            o[m] = v.astype(BF16)

        for r in rings2[n]:
            r.result(put)
        exchange(n)

    plan = []
    for n in range(STAGES):
        for after, what in ((0, begin), (1, pass1), (2.3, reduce1), (3.1, pass2), (3.9, reduce2)):
            plan.append((n + 5 + after, n, what))
    plan.sort(key=lambda item: item[:2])
    steps = CHUNKS + 4
    for step in range(steps):
        gather_step(step)
        while plan and plan[0][0] <= step:
            _, n, what = plan.pop(0)
            what(n)
    for _, n, what in plan:
        what(n)

    def sent(n, ref):
        rcopy(ref, ref, csend.at[n], crecv.at[0, 0], sib).wait_send()

    sent(0, gsib)
    for n in (1, 2, 3, 4):
        sent(n, zrel.at[0])
    for n in (5, 6):
        sent(n, psend)
    sent(9, sline.at[0 : 4 * q])
    for n in (7, 8):
        sent(n, zrel.at[0])

    ups = sum((hi - lo + 1) // 2 for ps in parts for lo, hi, _ in ps)
    for level, ref in ((0, l1), (1, l2)):
        for half_, blocks in ((0, ups), (1, TOTAL - ups)):
            done = ref.at[0:3, 0:blocks]
            rcopy(done, done, rsend.at[level, half_], rrecv.at[0, 0, 0], sib).wait_send()

    sized = (l1.at[0, 0:39], l1.at[0, 0:33])
    for core in (0, 1):

        @pl.when(k == core)
        def _():
            rcopy(sized[core], sized[core], fsem.at[0], fsem.at[1], sib).wait_recv()
            rcopy(sized[core], sized[core], fsem.at[0], fsem.at[1], sib).wait_send()

    @pl.loop(0, 12)
    def _(i):
        for j in range(6):
            direct = i >= 6 * mod(col, 2) + j
            from_me = jnp.where(direct, j % 2, mod(i, 2)) == k

            @pl.when(from_me)
            def _():
                rcopy(u.at[i, j], u.at[i, j], dsem.at[0], dsem.at[1], sib).start()

    for core in (0, 1):

        @pl.when(k == core)
        def _():
            rcopy(sized[1 - core], sized[1 - core], dsem.at[0], dsem.at[1], sib).wait_recv()
            rcopy(sized[core], sized[core], dsem.at[0], dsem.at[1], sib).wait_send()

    whole_out = pltpu.make_async_copy(u, out, lsem.at[0])
    whole_out.start()
    whole_out.wait()


def gather_blocks(grad):
    _, n, d = grad.shape
    q, bs = n // 4, BLOCK
    b4 = bs // 4
    subs = STAGES + STAGES - BETA_FROM
    vm = pltpu.VMEM
    dma = pltpu.SemaphoreType.DMA
    return pl.pallas_call(
        kernel,
        out_shape=jax.ShapeDtypeStruct((12, 6, bs, bs), BF16),
        in_specs=[pl.BlockSpec(memory_space=pl.ANY)],
        out_specs=pl.BlockSpec(memory_space=pl.ANY),
        scratch_shapes=[
            vm((2, q, d), BF16), vm((2, q, d), BF16), vm((q, d), BF16),
            vm((2, q // 2, d), BF16), vm((2, q // 2, d), BF16),
            vm((8 * q, d), BF16), vm((8 * q, d // 8), BF16), vm((TOTAL, 4, bs, bs), BF16),
            vm((4, TOTAL, bs, bs), BF16), vm((4, TOTAL, b4, bs), BF16),
            vm((TOTAL, bs, bs), F32), vm((TOTAL, bs, bs), BF16),
            vm((TOTAL, b4, bs), BF16), vm((12, 6, bs, bs), BF16), vm((TOTAL, 4, b4, bs), BF16),
            dma((CHUNKS,)), dma((10,)), dma((10, CHUNKS)), dma((2, 2)), dma((2, subs, 3)), dma((2,)), dma((2,)),
        ],
        compiler_params=pltpu.CompilerParams(has_side_effects=True, vmem_limit_bytes=56 * 1024 * 1024),
    )(grad.reshape(2, 2, q, d))


def finish(blocks, statistic, gram, following, ub, st, gr, fo, insem, outsem):
    n = ub.shape[-1]
    col0 = 6 * mod(lax.axis_index("col"), 2)

    def band(i):
        return pl.ds(pl.multiple_of(i * n, n), n)

    def reads(i):
        return (
            pltpu.make_async_copy(blocks.at[i], ub.at[i], insem.at[0, i]),
            pltpu.make_async_copy(statistic.at[band(i), :], st.at[band(i), :], insem.at[1, i]),
        )

    @pl.loop(0, 12)
    def _(i):
        for cp in reads(i):
            cp.start()

    @pl.loop(0, 12)
    def _(i):
        for cp in reads(i):
            cp.wait()
        for j in range(6):
            at = (band(i), slice(j * n, (j + 1) * n))

            @pl.when(i >= col0 + j)
            def _():
                gr[at] = ub[i, j].astype(F32)

            @pl.when(i < col0 + j)
            def _():
                gr[at] = ub[i, j].astype(F32).T

        rows = (band(i), slice(None))
        fo[rows] = 0.95 * st[rows] + 0.05 * gr[rows]
        pltpu.make_async_copy(gr.at[rows], gram.at[rows], outsem.at[0]).start()
        pltpu.make_async_copy(fo.at[rows], following.at[rows], outsem.at[1]).start()

    pltpu.make_async_copy(gr, gram, outsem.at[0]).wait()
    pltpu.make_async_copy(fo, following, outsem.at[1]).wait()


def shards(grad, statistic):
    blocks = gather_blocks(grad)
    shape = jax.ShapeDtypeStruct(statistic.shape, F32)
    whole = pltpu.VMEM(statistic.shape, F32)
    dma = pltpu.SemaphoreType.DMA
    return pl.pallas_call(
        finish,
        out_shape=(shape, shape),
        in_specs=[pl.BlockSpec(memory_space=pl.ANY)] * 2,
        out_specs=(pl.BlockSpec(memory_space=pl.ANY),) * 2,
        scratch_shapes=[pltpu.VMEM(blocks.shape, BF16), whole, whole, whole, dma((2, 12)), dma((2,))],
        compiler_params=pltpu.CompilerParams(vmem_limit_bytes=32 * 1024 * 1024),
    )(blocks, statistic)


def solution(mesh):
    return jax.shard_map(
        shards,
        mesh=mesh,
        in_specs=(P("rep", ("row", "col"), None), P("row", "col")),
        out_specs=(P("row", "col"), P("row", "col")),
        check_vma=False,
    )
```

```python
import functools

import jax
import jax.numpy as jnp
from jax import lax
from jax.experimental import pallas as pl
from jax.experimental.pallas import tpu as pltpu
from jax.sharding import PartitionSpec as P

MESH = pl.DeviceIdType.MESH
BF16 = jnp.bfloat16
F32 = jnp.float32
BLOCK = 128
STAGES = 12
WIDTHS = (4,) * 12
STARTS = tuple(sum(WIDTHS[:i]) for i in range(len(WIDTHS)))
CHUNKS = len(WIDTHS)
BETA_FROM = 8


def count(n):
    return n // 2 + 1


def first(n):
    return sum(count(i) for i in range(n))


TOTAL = first(STAGES)


def mod(a, n):
    return lax.rem(a, n)


def rcopy(src, dst, send, recv, device):
    return pltpu.make_async_remote_copy(
        src_ref=src, dst_ref=dst, send_sem=send, recv_sem=recv, device_id=device, device_id_type=MESH
    )


class Ring:
    def __init__(self, i, up, down, span, src, add, bufs, pair, sends, recvs):
        lo, hi = span
        mid = lo + (hi - lo + 1) // 2
        far, near, got, total = bufs
        at = lambda j: mod(i + j, 4)
        self.i, self.add, self.bufs, self.halves = i, add, bufs, []
        self.span, self.last, self.pair, self.up = span, recvs.at[2], pair, up
        for s, (a, b, long, short, j) in enumerate(((lo, mid, up, down, 3), (mid, hi, down, up, 1))):
            if a == b:
                continue
            cut = lambda ref: ref.at[a:b]
            self.halves.append((
                a, b, at(4 - j),
                rcopy(src(at(2), a, b), cut(far), sends.at[s], recvs.at[s], long),
                rcopy(src(at(j), a, b), cut(near), sends.at[s], recvs.at[2], short),
                rcopy(cut(total), cut(got), sends.at[s], recvs.at[2], long),
            ))

    def start(self):
        for h in self.halves:
            h[3].start()
        for h in self.halves:
            h[4].start()

    def pass_on(self):
        far, _, _, total = self.bufs
        for a, b, to, one, _, on in self.halves:
            one.wait_recv()

            @pl.loop(a, b)
            def _(m):
                total[m] = (far[m].astype(F32) + self.add(to, m)).astype(BF16)

            on.start()

    def result(self, put):
        _, near, got, _ = self.bufs
        both = self.pair.at[:, self.span[0] : self.span[1]]
        rcopy(both, both, self.last, self.last, self.up).wait_recv()
        for a, b, *_ in self.halves:

            @pl.loop(a, b)
            def _(m):
                put(m, self.add(self.i, m) + (near[m].astype(F32) + got[m].astype(F32)))


def kernel(
    g, out, gown, gsib, psend, zrel, zrec, sline, own, t, l1, l2, xf, xb, o, u, spare,
    lsem, csend, crecv, rsend, rrecv, fsem, dsem,
):
    rep, x, col = lax.axis_index("rep"), lax.axis_index("row"), lax.axis_index("col")
    zh, k = lax.div(rep, 2), mod(rep, 2)
    zl, y = lax.div(col, 4), mod(col, 4)
    z = 2 * zh + zl
    q, d = psend.shape
    half = q // 2
    bs = BLOCK
    b4 = bs // 4

    def dev(x, y, z, k):
        return {"rep": lax.div(z, 2) * 2 + k, "row": x, "col": mod(z, 2) * 4 + y}

    sib = dev(x, y, z, 1 - k)
    zp, zm = dev(x, y, mod(z + 1, 4), k), dev(x, y, mod(z + 3, 4), k)
    yp, ym = dev(x, mod(y + 1, 4), z, k), dev(x, mod(y + 3, 4), z, k)
    xp, xm = dev(mod(x + 1, 4), y, z, k), dev(mod(x + 3, 4), y, z, k)

    def cols(c):
        return slice(STARTS[c] * bs, (STARTS[c] + WIDTHS[c]) * bs)

    def rows(i):
        return pl.ds(pl.multiple_of(i * q, q), q)

    def strided(c):
        return [(pl.ds((c + STAGES * i) * bs, bs), pl.ds((4 * c + i) * bs, bs)) for i in range(4)]

    def load(c):
        for there, here in strided(c):
            pltpu.make_async_copy(g.at[:, k, :, there], gown.at[:, :, here], lsem.at[c]).start()

    def swap(c):
        for there, here in strided(c):
            rcopy(g.at[:, 1 - k, :, there], gsib.at[:, :, here], csend.at[0], crecv.at[0, c], sib).start()

    def loaded(c):
        whole = gown.at[:, :, cols(c)]
        pltpu.make_async_copy(whole, whole, lsem.at[c]).wait()
        whole = gsib.at[:, :, cols(c)]
        rcopy(whole, whole, csend.at[0], crecv.at[0, c], sib).wait_recv()

    def z1(c):
        return (
            rcopy(psend.at[0:half, cols(c)], zrel.at[0, :, cols(c)], csend.at[1], crecv.at[1, c], zp),
            rcopy(psend.at[half:q, cols(c)], zrel.at[1, :, cols(c)], csend.at[2], crecv.at[2, c], zm),
        )

    def z2(c):
        return (
            rcopy(zrel.at[0, :, cols(c)], zrec.at[0, :, cols(c)], csend.at[3], crecv.at[3, c], zp),
            rcopy(zrel.at[1, :, cols(c)], zrec.at[1, :, cols(c)], csend.at[4], crecv.at[4, c], zm),
        )

    def block(j, c, part=None):
        base = (2 * mod(y + j, 4) + k) * q
        if part is None:
            return sline.at[pl.ds(pl.multiple_of(base, q), q), cols(c)]
        return sline.at[pl.ds(pl.multiple_of(base + part * half, half), half), cols(c)]

    def y1(c):
        own = block(0, c)
        return (
            rcopy(own, own, csend.at[5], crecv.at[5, c], yp),
            rcopy(own, own, csend.at[6], crecv.at[6, c], ym),
        )

    def y1_landed(c):
        down, upper = block(3, c), block(1, c)
        return (
            rcopy(down, down, csend.at[5], crecv.at[5, c], yp),
            rcopy(upper, upper, csend.at[6], crecv.at[6, c], ym),
        )

    def y2(c):
        down, upper = block(3, c, 0), block(1, c, 1)
        return (
            rcopy(down, down, csend.at[7], crecv.at[7, c], yp),
            rcopy(upper, upper, csend.at[8], crecv.at[8, c], ym),
        )

    def y2_landed(c):
        lo, hi = block(2, c, 0), block(2, c, 1)
        return (
            rcopy(lo, lo, csend.at[7], crecv.at[7, c], yp),
            rcopy(hi, hi, csend.at[8], crecv.at[8, c], ym),
        )

    def share(j, c):
        blk = block(j, c)
        return rcopy(blk, blk, csend.at[9], crecv.at[9, c], sib)

    def shares_landed(c):
        four = sline.at[0 : 4 * q, cols(c)]
        rcopy(four, four, csend.at[9], crecv.at[9, c], sib).wait_recv()

    barrier = pltpu.get_barrier_semaphore()
    around = (sib, xp, xm, yp, ym, zp, zm)
    for other in around:
        pl.semaphore_signal(barrier, inc=1, device_id=other, device_id_type=MESH)
    for c in range(CHUNKS):
        load(c)
    own[...] = jnp.zeros_like(own)
    pl.semaphore_wait(barrier, len(around))
    for c in range(CHUNKS):
        swap(c)

    def gather_step(step):
        c = step
        if c < CHUNKS:
            loaded(c)
            away = 1 - zh
            psend[:, cols(c)] = (gown[away, :, cols(c)].astype(F32) + gsib[away, :, cols(c)].astype(F32)).astype(BF16)
            for cp in z1(c):
                cp.start()
        c = step - 1
        if 0 <= c < CHUNKS:
            for cp, fwd in zip(z1(c), z2(c)):
                cp.wait_recv()
                fwd.start()
        c = step - 2
        if 0 <= c < CHUNKS:
            for cp in z2(c):
                cp.wait_recv()
            own = gown[zh, :, cols(c)].astype(F32) + gsib[zh, :, cols(c)].astype(F32)
            far = jnp.concatenate([zrec[0, :, cols(c)], zrec[1, :, cols(c)]], axis=0).astype(F32)
            sline[rows(2 * y + k), cols(c)] = (own + far).astype(BF16)
            for cp in y1(c):
                cp.start()
            share(0, c).start()
        c = step - 3
        if 0 <= c < CHUNKS:
            for cp, fwd, j in zip(y1_landed(c), y2(c), (3, 1)):
                cp.wait_recv()
                fwd.start()
                share(j, c).start()
        c = step - 4
        if 0 <= c < CHUNKS:
            for cp in y2_landed(c):
                cp.wait_recv()
            share(2, c).start()

    turn = 2 * mod(y, 2) + lax.div(y, 2)
    strip = 4 * k + turn

    def tiles(n):
        for c in range(CHUNKS):
            if STARTS[c] // 4 == n:
                shares_landed(c)
        last = n // 2

        @pl.when(k == n % 2)
        def _():
            mine = pl.ds(pl.multiple_of((8 * last + strip) * bs, bs), bs)
            own[:, last * bs : (last + 1) * bs] = sline[:, mine]

        lhs = sline[:, 4 * n * bs : 4 * (n + 1) * bs]
        acc = lax.dot_general(
            lhs, own[:, : count(n) * bs], (((0,), (0,)), ((), ())), preferred_element_type=F32
        )
        for m in range(count(n)):
            for p in range(4):
                t[first(n) + m, p] = acc[p * bs : (p + 1) * bs, m * bs : (m + 1) * bs].astype(BF16)

    def quarter(v):
        return pl.ds(pl.multiple_of(v * b4, b4), b4)

    parts = []
    for n in range(STAGES):
        a, b = first(n), first(n + 1)
        h = b if n < BETA_FROM else a + (b - a + 1) // 2
        parts.append([(a, h, True)] + ([(h, b, False)] if h < b else []))
    rings1, rings2, used = [], [], 0
    for n in range(STAGES):
        ones, twos = [], []
        for a, b, x_first in parts[n]:
            along = ((x, xp, xm), (z, zp, zm))
            one, two = along if x_first else along[::-1]
            ones.append(Ring(
                *one, (a, b),
                lambda p, a, b: t.at[a:b, p],
                lambda p, m: t[m, p].astype(F32),
                [l1.at[i] for i in range(4)],
                l1.at[0:2],
                rsend.at[0], rrecv.at[0, used],
            ))
            twos.append(Ring(
                *two, (a, b),
                lambda v, a, b: xb.at[a:b, quarter(v), :],
                lambda v, m: xf[m, quarter(v), :],
                [l2.at[i] for i in range(4)],
                l2.at[0:2],
                rsend.at[1], rrecv.at[1, used],
            ))
            used += 1
        rings1.append(ones)
        rings2.append(twos)

    def exchange(n):
        for a, b, x_first in parts[n]:
            p1, p2 = (x, z) if x_first else (z, x)
            rblk = n + STAGES * p1

            def one(f, up, side):
                m = f - first(n)
                stage = 2 * m + k
                cblk = stage + STAGES * turn
                wanted = (stage <= n) if side == 0 else (stage < n)
                rr, cc = (rblk, cblk) if side == 0 else (cblk, rblk)
                tx, tc = lax.div(rr, 12), lax.div(cc, 6)
                src = o.at[f]
                dst = u.at[mod(rr, 12), mod(cc, 6), quarter(p2), :]
                ty, tz = mod(tc, 4), 2 * up + lax.div(tc, 4)
                mine = (tx == x) & (ty == y) & (tz == z)

                @pl.when(wanted & jnp.logical_not(mine))
                def _():
                    rcopy(src, dst, fsem.at[0], fsem.at[1], dev(tx, ty, tz, k)).start()

                @pl.when(wanted & mine)
                def _():
                    pltpu.make_async_copy(src, dst, fsem.at[1]).start()
                    pltpu.make_async_copy(src, spare.at[f, 2 * side + up], fsem.at[0]).start()

            @pl.loop(a, b)
            def _(f):
                for side in (0, 1):
                    for up in (0, 1):
                        one(f, up, side)

    def begin(n):
        tiles(n)
        for r in rings1[n]:
            r.start()

    def pass1(n):
        for r in rings1[n]:
            r.pass_on()

    def reduce1(n):
        def put(m, v):
            xf[m] = v
            xb[m] = v.astype(BF16)

        for r, r2 in zip(rings1[n], rings2[n]):
            r.result(put)
            r2.start()

    def pass2(n):
        for r in rings2[n]:
            r.pass_on()

    def reduce2(n):
        def put(m, v):
            o[m] = v.astype(BF16)

        for r in rings2[n]:
            r.result(put)
        exchange(n)

    rounds = {}
    for n in range(STAGES):
        lags = (1, 3, 4, 0, 5) if n < 7 else (1, 2, 3, 0, 4)
        for place, (lag, what) in enumerate(zip(lags, (pass1, reduce1, pass2, begin, reduce2))):
            rounds.setdefault(n + 5 + lag, []).append((place, n, what))
    for step in range(max(rounds) + 1):
        gather_step(step)
        for _, n, what in sorted(rounds.get(step, ()), key=lambda item: item[:2]):
            what(n)

    def sent(n, ref):
        rcopy(ref, ref, csend.at[n], crecv.at[0, 0], sib).wait_send()

    sent(0, gsib)
    for n in (1, 2, 3, 4):
        sent(n, zrel.at[0])
    for n in (5, 6):
        sent(n, psend)
    sent(9, sline.at[0 : 4 * q])
    for n in (7, 8):
        sent(n, zrel.at[0])

    ups = sum((hi - lo + 1) // 2 for ps in parts for lo, hi, _ in ps)
    for level, ref in ((0, l1), (1, l2)):
        for half_, blocks in ((0, ups), (1, TOTAL - ups)):
            done = ref.at[0:3, 0:blocks]
            rcopy(done, done, rsend.at[level, half_], rrecv.at[0, 0, 0], sib).wait_send()

    sized = (l1.at[0, 0:39], l1.at[0, 0:33])
    for core in (0, 1):

        @pl.when(k == core)
        def _():
            rcopy(sized[core], sized[core], fsem.at[0], fsem.at[1], sib).wait_recv()
            rcopy(sized[core], sized[core], fsem.at[0], fsem.at[1], sib).wait_send()

    @pl.loop(0, 12)
    def _(i):
        for j in range(6):
            direct = i >= 6 * mod(col, 2) + j
            from_me = jnp.where(direct, j % 2, mod(i, 2)) == k

            @pl.when(from_me)
            def _():
                rcopy(u.at[i, j], u.at[i, j], dsem.at[0], dsem.at[1], sib).start()

    for core in (0, 1):

        @pl.when(k == core)
        def _():
            rcopy(sized[1 - core], sized[1 - core], dsem.at[0], dsem.at[1], sib).wait_recv()
            rcopy(sized[core], sized[core], dsem.at[0], dsem.at[1], sib).wait_send()

    whole_out = pltpu.make_async_copy(u, out, lsem.at[0])
    whole_out.start()
    whole_out.wait()


def gather_blocks(grad):
    _, n, d = grad.shape
    q, bs = n // 4, BLOCK
    b4 = bs // 4
    subs = STAGES + STAGES - BETA_FROM
    vm = pltpu.VMEM
    dma = pltpu.SemaphoreType.DMA
    return pl.pallas_call(
        kernel,
        out_shape=jax.ShapeDtypeStruct((12, 6, bs, bs), BF16),
        in_specs=[pl.BlockSpec(memory_space=pl.ANY)],
        out_specs=pl.BlockSpec(memory_space=pl.ANY),
        scratch_shapes=[
            vm((2, q, d), BF16), vm((2, q, d), BF16), vm((q, d), BF16),
            vm((2, q // 2, d), BF16), vm((2, q // 2, d), BF16),
            vm((8 * q, d), BF16), vm((8 * q, d // 8), BF16), vm((TOTAL, 4, bs, bs), BF16),
            vm((4, TOTAL, bs, bs), BF16), vm((4, TOTAL, b4, bs), BF16),
            vm((TOTAL, bs, bs), F32), vm((TOTAL, bs, bs), BF16),
            vm((TOTAL, b4, bs), BF16), vm((12, 6, bs, bs), BF16), vm((TOTAL, 4, b4, bs), BF16),
            dma((CHUNKS,)), dma((10,)), dma((10, CHUNKS)), dma((2, 2)), dma((2, subs, 3)), dma((2,)), dma((2,)),
        ],
        compiler_params=pltpu.CompilerParams(collective_id=0, has_side_effects=True, vmem_limit_bytes=56 * 1024 * 1024),
    )(grad.reshape(2, 2, q, d))


def finish(blocks, statistic, gram, following, ub, st, gr, fo, insem, outsem):
    n = ub.shape[-1]
    col0 = 6 * mod(lax.axis_index("col"), 2)

    def band(i):
        return pl.ds(pl.multiple_of(i * n, n), n)

    def reads(i):
        return (
            pltpu.make_async_copy(blocks.at[i], ub.at[i], insem.at[0, i]),
            pltpu.make_async_copy(statistic.at[band(i), :], st.at[band(i), :], insem.at[1, i]),
        )

    @pl.loop(0, 12)
    def _(i):
        for cp in reads(i):
            cp.start()

    @pl.loop(0, 12)
    def _(i):
        for cp in reads(i):
            cp.wait()
        rows = (band(i), slice(None))
        for j in range(6):
            at = (band(i), slice(j * n, (j + 1) * n))
            block = ub[i, j].astype(F32)
            value = jnp.where(i >= col0 + j, block, block.T)
            gr[at] = value
            fo[at] = 0.95 * st[at] + 0.05 * value
        pltpu.make_async_copy(gr.at[rows], gram.at[rows], outsem.at[0]).start()
        pltpu.make_async_copy(fo.at[rows], following.at[rows], outsem.at[1]).start()

    pltpu.make_async_copy(gr, gram, outsem.at[0]).wait()
    pltpu.make_async_copy(fo, following, outsem.at[1]).wait()


def shards(grad, statistic):
    blocks = gather_blocks(grad)
    shape = jax.ShapeDtypeStruct(statistic.shape, F32)
    whole = pltpu.VMEM(statistic.shape, F32)
    dma = pltpu.SemaphoreType.DMA
    return pl.pallas_call(
        finish,
        out_shape=(shape, shape),
        in_specs=[pl.BlockSpec(memory_space=pl.ANY)] * 2,
        out_specs=(pl.BlockSpec(memory_space=pl.ANY),) * 2,
        scratch_shapes=[pltpu.VMEM(blocks.shape, BF16), whole, whole, whole, dma((2, 12)), dma((2,))],
        compiler_params=pltpu.CompilerParams(vmem_limit_bytes=60 * 1024 * 1024),
    )(blocks, statistic)


def solution(mesh):
    return jax.shard_map(
        shards,
        mesh=mesh,
        in_specs=(P("rep", ("row", "col"), None), P("row", "col")),
        out_specs=(P("row", "col"), P("row", "col")),
        check_vma=False,
    )
```

```python
import functools

import jax
import jax.numpy as jnp
from jax import lax
from jax.experimental import pallas as pl
from jax.experimental.pallas import tpu as pltpu
from jax.sharding import PartitionSpec as P

MESH = pl.DeviceIdType.MESH
BF16 = jnp.bfloat16
F32 = jnp.float32
BLOCK = 128
STAGES = 12
WIDTHS = (4,) * 12
STARTS = tuple(sum(WIDTHS[:i]) for i in range(len(WIDTHS)))
CHUNKS = len(WIDTHS)
BETA_FROM = 8


def count(n):
    return n // 2 + 1


def first(n):
    return sum(count(i) for i in range(n))


TOTAL = first(STAGES)


def block_of(i, stage):
    return STAGES * i + mod(stage + 6 * lax.div(i, 2), STAGES)


def mod(a, n):
    return lax.rem(a, n)


def rcopy(src, dst, send, recv, device):
    return pltpu.make_async_remote_copy(
        src_ref=src, dst_ref=dst, send_sem=send, recv_sem=recv, device_id=device, device_id_type=MESH
    )


class Ring:
    def __init__(self, i, up, down, span, src, add, bufs, pair, sends, recvs):
        lo, hi = span
        mid = lo + (hi - lo + 1) // 2
        far, near, got, total = bufs
        at = lambda j: mod(i + j, 4)
        self.i, self.add, self.bufs, self.halves = i, add, bufs, []
        self.span, self.last, self.pair, self.up = span, recvs.at[2], pair, up
        for s, (a, b, long, short, j) in enumerate(((lo, mid, up, down, 3), (mid, hi, down, up, 1))):
            if a == b:
                continue
            cut = lambda ref: ref.at[a:b]
            self.halves.append((
                a, b, at(4 - j),
                rcopy(src(at(2), a, b), cut(far), sends.at[s], recvs.at[s], long),
                rcopy(src(at(j), a, b), cut(near), sends.at[s], recvs.at[2], short),
                rcopy(cut(total), cut(got), sends.at[s], recvs.at[2], long),
            ))

    def start(self):
        for h in self.halves:
            h[3].start()
        for h in self.halves:
            h[4].start()

    def pass_on(self):
        far, _, _, total = self.bufs
        for a, b, to, one, _, on in self.halves:
            one.wait_recv()

            @pl.loop(a, b)
            def _(m):
                total[m] = (far[m].astype(F32) + self.add(to, m)).astype(BF16)

            on.start()

    def result(self, put):
        _, near, got, _ = self.bufs
        both = self.pair.at[:, self.span[0] : self.span[1]]
        rcopy(both, both, self.last, self.last, self.up).wait_recv()
        for a, b, *_ in self.halves:

            @pl.loop(a, b)
            def _(m):
                put(m, self.add(self.i, m) + (near[m].astype(F32) + got[m].astype(F32)))


class Spread:
    def __init__(self, i, others, span, src, add, buf, send, recv):
        a, b = span
        self.i, self.add, self.buf, self.span = i, add, buf, span
        self.copies = [
            rcopy(src(mod(i + j, 4), a, b), buf.at[j - 1, a:b], send, recv, other) for j, other in zip((2, 1, 3), others)
        ]
        landed = buf.at[:, a:b]
        self.landed = rcopy(landed, landed, send, recv, others[0])

    def start(self):
        for c in self.copies:
            c.start()

    def result(self, put):
        self.landed.wait_recv()

        @pl.loop(*self.span)
        def _(m):
            theirs = (self.buf[0, m].astype(F32) + self.buf[1, m].astype(F32)) + self.buf[2, m].astype(F32)
            put(m, self.add(self.i, m) + theirs)


def kernel(
    g, out, gown, gsib, psend, zrel, zrec, sline, own, t, l1, l2, xf, xb, o, u, spare,
    lsem, csend, crecv, rsend, rrecv, fsem, dsem,
):
    rep, x, col = lax.axis_index("rep"), lax.axis_index("row"), lax.axis_index("col")
    zh, k = lax.div(rep, 2), mod(rep, 2)
    zl, y = lax.div(col, 4), mod(col, 4)
    z = 2 * zh + zl
    q, d = psend.shape
    half = q // 2
    bs = BLOCK
    b4 = bs // 4

    def dev(x, y, z, k):
        return {"rep": lax.div(z, 2) * 2 + k, "row": x, "col": mod(z, 2) * 4 + y}

    sib = dev(x, y, z, 1 - k)
    zp, zm = dev(x, y, mod(z + 1, 4), k), dev(x, y, mod(z + 3, 4), k)
    yp, ym = dev(x, mod(y + 1, 4), z, k), dev(x, mod(y + 3, 4), z, k)
    xp, xm = dev(mod(x + 1, 4), y, z, k), dev(mod(x + 3, 4), y, z, k)

    xpp, zpp = dev(mod(x + 2, 4), y, z, k), dev(x, y, mod(z + 2, 4), k)

    def cols(c):
        return slice(STARTS[c] * bs, (STARTS[c] + WIDTHS[c]) * bs)

    def rows(i):
        return pl.ds(pl.multiple_of(i * q, q), q)

    def strided(c):
        return [(pl.ds((STAGES * i + (c + 6 * (i // 2)) % STAGES) * bs, bs), pl.ds((4 * c + i) * bs, bs)) for i in range(4)]

    def load(c):
        for there, here in strided(c):
            pltpu.make_async_copy(g.at[:, k, :, there], gown.at[:, :, here], lsem.at[c]).start()

    def swap(c):
        for there, here in strided(c):
            rcopy(g.at[:, 1 - k, :, there], gsib.at[:, :, here], csend.at[0], crecv.at[0, c], sib).start()

    def loaded(c):
        whole = gown.at[:, :, cols(c)]
        pltpu.make_async_copy(whole, whole, lsem.at[c]).wait()
        whole = gsib.at[:, :, cols(c)]
        rcopy(whole, whole, csend.at[0], crecv.at[0, c], sib).wait_recv()

    def z1(c):
        return (
            rcopy(psend.at[0:half, cols(c)], zrel.at[0, :, cols(c)], csend.at[1], crecv.at[1, c], zp),
            rcopy(psend.at[half:q, cols(c)], zrel.at[1, :, cols(c)], csend.at[2], crecv.at[2, c], zm),
        )

    def z2(c):
        return (
            rcopy(zrel.at[0, :, cols(c)], zrec.at[0, :, cols(c)], csend.at[3], crecv.at[3, c], zp),
            rcopy(zrel.at[1, :, cols(c)], zrec.at[1, :, cols(c)], csend.at[4], crecv.at[4, c], zm),
        )

    def block(j, c, part=None):
        base = (2 * mod(y + j, 4) + k) * q
        if part is None:
            return sline.at[pl.ds(pl.multiple_of(base, q), q), cols(c)]
        return sline.at[pl.ds(pl.multiple_of(base + part * half, half), half), cols(c)]

    def y1(c):
        own = block(0, c)
        return (
            rcopy(own, own, csend.at[5], crecv.at[5, c], yp),
            rcopy(own, own, csend.at[6], crecv.at[6, c], ym),
        )

    def y1_landed(c):
        down, upper = block(3, c), block(1, c)
        return (
            rcopy(down, down, csend.at[5], crecv.at[5, c], yp),
            rcopy(upper, upper, csend.at[6], crecv.at[6, c], ym),
        )

    def y2(c):
        down, upper = block(3, c, 0), block(1, c, 1)
        return (
            rcopy(down, down, csend.at[7], crecv.at[7, c], yp),
            rcopy(upper, upper, csend.at[8], crecv.at[8, c], ym),
        )

    def y2_landed(c):
        lo, hi = block(2, c, 0), block(2, c, 1)
        return (
            rcopy(lo, lo, csend.at[7], crecv.at[7, c], yp),
            rcopy(hi, hi, csend.at[8], crecv.at[8, c], ym),
        )

    def share(j, c):
        blk = block(j, c)
        return rcopy(blk, blk, csend.at[9], crecv.at[9, c], sib)

    def shares_landed(c):
        four = sline.at[0 : 4 * q, cols(c)]
        rcopy(four, four, csend.at[9], crecv.at[9, c], sib).wait_recv()

    barrier = pltpu.get_barrier_semaphore()
    around = (sib, xp, xm, yp, ym, zp, zm)
    for other in around:
        pl.semaphore_signal(barrier, inc=1, device_id=other, device_id_type=MESH)
    for c in range(CHUNKS):
        load(c)
    own[...] = jnp.zeros_like(own)
    pl.semaphore_wait(barrier, len(around))
    for c in range(CHUNKS):
        swap(c)

    def gather_step(step):
        c = step
        if c < CHUNKS:
            loaded(c)
            away = 1 - zh
            psend[:, cols(c)] = (gown[away, :, cols(c)].astype(F32) + gsib[away, :, cols(c)].astype(F32)).astype(BF16)
            for cp in z1(c):
                cp.start()
        c = step - 1
        if 0 <= c < CHUNKS:
            for cp, fwd in zip(z1(c), z2(c)):
                cp.wait_recv()
                fwd.start()
        c = step - 2
        if 0 <= c < CHUNKS:
            for cp in z2(c):
                cp.wait_recv()
            own = gown[zh, :, cols(c)].astype(F32) + gsib[zh, :, cols(c)].astype(F32)
            far = jnp.concatenate([zrec[0, :, cols(c)], zrec[1, :, cols(c)]], axis=0).astype(F32)
            sline[rows(2 * y + k), cols(c)] = (own + far).astype(BF16)
            for cp in y1(c):
                cp.start()
            share(0, c).start()
        c = step - 3
        if 0 <= c < CHUNKS:
            for cp, fwd, j in zip(y1_landed(c), y2(c), (3, 1)):
                cp.wait_recv()
                fwd.start()
                share(j, c).start()
        c = step - 4
        if 0 <= c < CHUNKS:
            for cp in y2_landed(c):
                cp.wait_recv()
            share(2, c).start()

    turn = 2 * mod(y, 2) + lax.div(y, 2)
    strip = 4 * k + turn

    def tiles(n):
        for c in range(CHUNKS):
            if STARTS[c] // 4 == n:
                shares_landed(c)
        last = n // 2

        @pl.when(k == n % 2)
        def _():
            mine = pl.ds(pl.multiple_of((8 * last + strip) * bs, bs), bs)
            own[:, last * bs : (last + 1) * bs] = sline[:, mine]

        lhs = sline[:, 4 * n * bs : 4 * (n + 1) * bs]
        acc = lax.dot_general(
            lhs, own[:, : count(n) * bs], (((0,), (0,)), ((), ())), preferred_element_type=F32
        )
        for m in range(count(n)):
            for p in range(4):
                t[first(n) + m, p] = acc[p * bs : (p + 1) * bs, m * bs : (m + 1) * bs].astype(BF16)

    def quarter(v):
        return pl.ds(pl.multiple_of(v * b4, b4), b4)

    parts = []
    for n in range(STAGES):
        a, b = first(n), first(n + 1)
        h = b if n < BETA_FROM else a + (b - a + 1) // 2
        parts.append([(a, h, True)] + ([(h, b, False)] if h < b else []))
    rings1, rings2, used = [], [], 0
    for n in range(STAGES):
        ones, twos = [], []
        for a, b, x_first in parts[n]:
            along = ((x, xp, xm), (z, zp, zm))
            one, two = along if x_first else along[::-1]
            ones.append(Ring(
                *one, (a, b),
                lambda p, a, b: t.at[a:b, p],
                lambda p, m: t[m, p].astype(F32),
                [l1.at[i] for i in range(4)],
                l1.at[0:2],
                rsend.at[0], rrecv.at[0, used],
            ))
            across = (zpp if x_first else xpp, two[1], two[2])
            twos.append(Spread(
                two[0], across, (a, b),
                lambda v, a, b: xb.at[a:b, quarter(v), :],
                lambda v, m: xf[m, quarter(v), :],
                l2, rsend.at[1, 0], rrecv.at[1, used, 0],
            ))
            used += 1
        rings1.append(ones)
        rings2.append(twos)

    def exchange(n):
        for a, b, x_first in parts[n]:
            p1, p2 = (x, z) if x_first else (z, x)
            rblk = block_of(p1, n)

            def one(f, up, side):
                m = f - first(n)
                stage = 2 * m + k
                cblk = block_of(turn, stage)
                wanted = (stage <= n) if side == 0 else (stage < n)
                rr, cc = (rblk, cblk) if side == 0 else (cblk, rblk)
                tx, tc = lax.div(rr, 12), lax.div(cc, 6)
                src = o.at[f]
                dst = u.at[mod(rr, 12), mod(cc, 6), quarter(p2), :]
                ty, tz = mod(tc, 4), 2 * up + lax.div(tc, 4)
                mine = (tx == x) & (ty == y) & (tz == z)

                @pl.when(wanted & jnp.logical_not(mine))
                def _():
                    rcopy(src, dst, fsem.at[0], fsem.at[1], dev(tx, ty, tz, k)).start()

                @pl.when(wanted & mine)
                def _():
                    pltpu.make_async_copy(src, dst, fsem.at[1]).start()
                    pltpu.make_async_copy(src, spare.at[f, 2 * side + up], fsem.at[0]).start()

            @pl.loop(a, b)
            def _(f):
                for side in (0, 1):
                    for up in (0, 1):
                        one(f, up, side)

    def begin(n):
        tiles(n)
        for r in rings1[n]:
            r.start()

    def pass1(n):
        for r in rings1[n]:
            r.pass_on()

    def reduce1(n):
        def put(m, v):
            xf[m] = v
            xb[m] = v.astype(BF16)

        for r, r2 in zip(rings1[n], rings2[n]):
            r.result(put)
            r2.start()

    def reduce2(n):
        def put(m, v):
            o[m] = v.astype(BF16)

        for r in rings2[n]:
            r.result(put)
        exchange(n)

    rounds = {}
    for n in range(STAGES):
        lags = (0, 1, 3, 4) if n < 7 else (0, 1, 2, 3)
        for place, (lag, what) in enumerate(zip(lags, (begin, pass1, reduce1, reduce2))):
            rounds.setdefault(n + 5 + lag, []).append((place, n, what))
    for step in range(max(rounds) + 1):
        gather_step(step)
        for _, n, what in sorted(rounds.get(step, ()), key=lambda item: item[:2]):
            what(n)

    def sent(n, ref):
        rcopy(ref, ref, csend.at[n], crecv.at[0, 0], sib).wait_send()

    sent(0, gsib)
    for n in (1, 2, 3, 4):
        sent(n, zrel.at[0])
    for n in (5, 6):
        sent(n, psend)
    sent(9, sline.at[0 : 4 * q])
    for n in (7, 8):
        sent(n, zrel.at[0])

    ups = sum((hi - lo + 1) // 2 for ps in parts for lo, hi, _ in ps)
    for half_, blocks in ((0, ups), (1, TOTAL - ups)):
        done = l1.at[0:3, 0:blocks]
        rcopy(done, done, rsend.at[0, half_], rrecv.at[0, 0, 0], sib).wait_send()
    rcopy(l2, l2, rsend.at[1, 0], rrecv.at[0, 0, 0], sib).wait_send()

    sized = (l1.at[0, 0:39], l1.at[0, 0:33])
    for core in (0, 1):

        @pl.when(k == core)
        def _():
            rcopy(sized[core], sized[core], fsem.at[0], fsem.at[1], sib).wait_recv()
            rcopy(sized[core], sized[core], fsem.at[0], fsem.at[1], sib).wait_send()

    @pl.loop(0, 12)
    def _(i):
        for j in range(6):
            direct = mod(i + 6 * lax.div(x, 2), 12) >= 6 * mod(col + zl, 2) + j
            from_me = jnp.where(direct, j % 2, mod(i, 2)) == k

            @pl.when(from_me)
            def _():
                rcopy(u.at[i, j], u.at[i, j], dsem.at[0], dsem.at[1], sib).start()

    for core in (0, 1):

        @pl.when(k == core)
        def _():
            rcopy(sized[1 - core], sized[1 - core], dsem.at[0], dsem.at[1], sib).wait_recv()
            rcopy(sized[core], sized[core], dsem.at[0], dsem.at[1], sib).wait_send()

    whole_out = pltpu.make_async_copy(u, out, lsem.at[0])
    whole_out.start()
    whole_out.wait()


def gather_blocks(grad):
    _, n, d = grad.shape
    q, bs = n // 4, BLOCK
    b4 = bs // 4
    subs = STAGES + STAGES - BETA_FROM
    vm = pltpu.VMEM
    dma = pltpu.SemaphoreType.DMA
    return pl.pallas_call(
        kernel,
        out_shape=jax.ShapeDtypeStruct((12, 6, bs, bs), BF16),
        in_specs=[pl.BlockSpec(memory_space=pl.ANY)],
        out_specs=pl.BlockSpec(memory_space=pl.ANY),
        scratch_shapes=[
            vm((2, q, d), BF16), vm((2, q, d), BF16), vm((q, d), BF16),
            vm((2, q // 2, d), BF16), vm((2, q // 2, d), BF16),
            vm((8 * q, d), BF16), vm((8 * q, d // 8), BF16), vm((TOTAL, 4, bs, bs), BF16),
            vm((4, TOTAL, bs, bs), BF16), vm((3, TOTAL, b4, bs), BF16),
            vm((TOTAL, bs, bs), F32), vm((TOTAL, bs, bs), BF16),
            vm((TOTAL, b4, bs), BF16), vm((12, 6, bs, bs), BF16), vm((TOTAL, 4, b4, bs), BF16),
            dma((CHUNKS,)), dma((10,)), dma((10, CHUNKS)), dma((2, 2)), dma((2, subs, 3)), dma((2,)), dma((2,)),
        ],
        compiler_params=pltpu.CompilerParams(collective_id=0, has_side_effects=True, vmem_limit_bytes=56 * 1024 * 1024),
    )(grad.reshape(2, 2, q, d))


def finish(blocks, statistic, gram, following, ub, st, gr, fo, insem, outsem):
    n = ub.shape[-1]
    col = lax.axis_index("col")
    col0 = 6 * mod(col + lax.div(col, 4), 2)
    row0 = 6 * lax.div(lax.axis_index("row"), 2)

    def band(i):
        return pl.ds(pl.multiple_of(i * n, n), n)

    def reads(i):
        return (
            pltpu.make_async_copy(blocks.at[i], ub.at[i], insem.at[0, i]),
            pltpu.make_async_copy(statistic.at[band(i), :], st.at[band(i), :], insem.at[1, i]),
        )

    @pl.loop(0, 12)
    def _(i):
        for cp in reads(i):
            cp.start()

    @pl.loop(0, 12)
    def _(i):
        for cp in reads(i):
            cp.wait()
        rows = (band(i), slice(None))
        for j in range(6):
            at = (band(i), slice(j * n, (j + 1) * n))
            block = ub[i, j].astype(F32)
            value = jnp.where(mod(i + row0, 12) >= col0 + j, block, block.T)
            gr[at] = value
            fo[at] = 0.95 * st[at] + 0.05 * value
        pltpu.make_async_copy(gr.at[rows], gram.at[rows], outsem.at[0]).start()
        pltpu.make_async_copy(fo.at[rows], following.at[rows], outsem.at[1]).start()

    pltpu.make_async_copy(gr, gram, outsem.at[0]).wait()
    pltpu.make_async_copy(fo, following, outsem.at[1]).wait()


def shards(grad, statistic):
    blocks = gather_blocks(grad)
    shape = jax.ShapeDtypeStruct(statistic.shape, F32)
    whole = pltpu.VMEM(statistic.shape, F32)
    dma = pltpu.SemaphoreType.DMA
    return pl.pallas_call(
        finish,
        out_shape=(shape, shape),
        in_specs=[pl.BlockSpec(memory_space=pl.ANY)] * 2,
        out_specs=(pl.BlockSpec(memory_space=pl.ANY),) * 2,
        scratch_shapes=[pltpu.VMEM(blocks.shape, BF16), whole, whole, whole, dma((2, 12)), dma((2,))],
        compiler_params=pltpu.CompilerParams(vmem_limit_bytes=60 * 1024 * 1024),
    )(blocks, statistic)


def solution(mesh):
    return jax.shard_map(
        shards,
        mesh=mesh,
        in_specs=(P("rep", ("row", "col"), None), P("row", "col")),
        out_specs=(P("row", "col"), P("row", "col")),
        check_vma=False,
    )
```

```python
import functools

import jax
import jax.numpy as jnp
from jax import lax
from jax.experimental import pallas as pl
from jax.experimental.pallas import tpu as pltpu
from jax.sharding import PartitionSpec as P

MESH = pl.DeviceIdType.MESH
BF16 = jnp.bfloat16
F32 = jnp.float32
BLOCK = 128
STAGES = 12
WIDTHS = (4,) * 12
STARTS = tuple(sum(WIDTHS[:i]) for i in range(len(WIDTHS)))
CHUNKS = len(WIDTHS)
BETA_FROM = 8


def count(n):
    return n // 2 + 1


def first(n):
    return sum(count(i) for i in range(n))


TOTAL = first(STAGES)


def block_of(i, stage):
    return STAGES * i + mod(stage + 6 * lax.div(i, 2), STAGES)


def mod(a, n):
    return lax.rem(a, n)


def rcopy(src, dst, send, recv, device):
    return pltpu.make_async_remote_copy(
        src_ref=src, dst_ref=dst, send_sem=send, recv_sem=recv, device_id=device, device_id_type=MESH
    )


class Ring:
    def __init__(self, i, up, down, span, src, add, bufs, pair, sends, recvs):
        lo, hi = span
        mid = lo + (hi - lo + 1) // 2
        far, near, got, total = bufs
        at = lambda j: mod(i + j, 4)
        self.i, self.add, self.bufs, self.halves = i, add, bufs, []
        self.span, self.last, self.pair, self.up = span, recvs.at[2], pair, up
        for s, (a, b, long, short, j) in enumerate(((lo, mid, up, down, 3), (mid, hi, down, up, 1))):
            if a == b:
                continue
            cut = lambda ref: ref.at[a:b]
            self.halves.append((
                a, b, at(4 - j),
                rcopy(src(at(2), a, b), cut(far), sends.at[s], recvs.at[s], long),
                rcopy(src(at(j), a, b), cut(near), sends.at[s], recvs.at[2], short),
                rcopy(cut(total), cut(got), sends.at[s], recvs.at[2], long),
            ))

    def start(self):
        for h in self.halves:
            h[3].start()
        for h in self.halves:
            h[4].start()

    def pass_on(self):
        far, _, _, total = self.bufs
        for a, b, to, one, _, on in self.halves:
            one.wait_recv()

            @pl.loop(a, b)
            def _(m):
                total[m] = (far[m].astype(F32) + self.add(to, m)).astype(BF16)

            on.start()

    def result(self, put):
        _, near, got, _ = self.bufs
        both = self.pair.at[:, self.span[0] : self.span[1]]
        rcopy(both, both, self.last, self.last, self.up).wait_recv()
        for a, b, *_ in self.halves:

            @pl.loop(a, b)
            def _(m):
                put(m, self.add(self.i, m) + (near[m].astype(F32) + got[m].astype(F32)))


class Spread:
    def __init__(self, i, others, span, src, add, buf, send, recv):
        a, b = span
        self.i, self.add, self.buf, self.span = i, add, buf, span
        self.copies = [
            rcopy(src(mod(i + j, 4), a, b), buf.at[j - 1, a:b], send, recv, other) for j, other in zip((2, 1, 3), others)
        ]
        landed = buf.at[:, a:b]
        self.landed = rcopy(landed, landed, send, recv, others[0])

    def start(self):
        for c in self.copies:
            c.start()

    def result(self, put):
        self.landed.wait_recv()

        @pl.loop(*self.span)
        def _(m):
            theirs = (self.buf[0, m].astype(F32) + self.buf[1, m].astype(F32)) + self.buf[2, m].astype(F32)
            put(m, self.add(self.i, m) + theirs)


def kernel(
    g, out, gown, gsib, psend, zrel, zrec, sline, own, t, l1, l2, xf, xb, o, u, spare,
    lsem, csend, crecv, rsend, rrecv, fsem, dsem,
):
    rep, x, col = lax.axis_index("rep"), lax.axis_index("row"), lax.axis_index("col")
    zh, k = lax.div(rep, 2), mod(rep, 2)
    zl, y = lax.div(col, 4), mod(col, 4)
    z = 2 * zh + zl
    q, d = psend.shape
    half = q // 2
    bs = BLOCK
    b4 = bs // 4

    def dev(x, y, z, k):
        return {"rep": lax.div(z, 2) * 2 + k, "row": x, "col": mod(z, 2) * 4 + y}

    sib = dev(x, y, z, 1 - k)
    zp, zm = dev(x, y, mod(z + 1, 4), k), dev(x, y, mod(z + 3, 4), k)
    yp, ym = dev(x, mod(y + 1, 4), z, k), dev(x, mod(y + 3, 4), z, k)
    xp, xm = dev(mod(x + 1, 4), y, z, k), dev(mod(x + 3, 4), y, z, k)

    xpp, zpp = dev(mod(x + 2, 4), y, z, k), dev(x, y, mod(z + 2, 4), k)

    def cols(c):
        return slice(STARTS[c] * bs, (STARTS[c] + WIDTHS[c]) * bs)

    def rows(i):
        return pl.ds(pl.multiple_of(i * q, q), q)

    def strided(c):
        return [(pl.ds((STAGES * i + (c + 6 * (i // 2)) % STAGES) * bs, bs), pl.ds((4 * c + i) * bs, bs)) for i in range(4)]

    def load(c):
        for there, here in strided(c):
            pltpu.make_async_copy(g.at[:, k, :, there], gown.at[:, :, here], lsem.at[c]).start()

    def swap(c):
        for there, here in strided(c):
            rcopy(g.at[:, 1 - k, :, there], gsib.at[:, :, here], csend.at[0], crecv.at[0, c], sib).start()

    def loaded(c):
        whole = gown.at[:, :, cols(c)]
        pltpu.make_async_copy(whole, whole, lsem.at[c]).wait()
        whole = gsib.at[:, :, cols(c)]
        rcopy(whole, whole, csend.at[0], crecv.at[0, c], sib).wait_recv()

    def z1(c):
        return (
            rcopy(psend.at[0:half, cols(c)], zrel.at[0, :, cols(c)], csend.at[1], crecv.at[1, c], zp),
            rcopy(psend.at[half:q, cols(c)], zrel.at[1, :, cols(c)], csend.at[2], crecv.at[2, c], zm),
        )

    def z2(c):
        return (
            rcopy(zrel.at[0, :, cols(c)], zrec.at[0, :, cols(c)], csend.at[3], crecv.at[3, c], zp),
            rcopy(zrel.at[1, :, cols(c)], zrec.at[1, :, cols(c)], csend.at[4], crecv.at[4, c], zm),
        )

    def block(j, c, part=None):
        base = (2 * mod(y + j, 4) + k) * q
        if part is None:
            return sline.at[pl.ds(pl.multiple_of(base, q), q), cols(c)]
        return sline.at[pl.ds(pl.multiple_of(base + part * half, half), half), cols(c)]

    def y1(c):
        own = block(0, c)
        return (
            rcopy(own, own, csend.at[5], crecv.at[5, c], yp),
            rcopy(own, own, csend.at[6], crecv.at[6, c], ym),
        )

    def y1_landed(c):
        down, upper = block(3, c), block(1, c)
        return (
            rcopy(down, down, csend.at[5], crecv.at[5, c], yp),
            rcopy(upper, upper, csend.at[6], crecv.at[6, c], ym),
        )

    def y2(c):
        down, upper = block(3, c, 0), block(1, c, 1)
        return (
            rcopy(down, down, csend.at[7], crecv.at[7, c], yp),
            rcopy(upper, upper, csend.at[8], crecv.at[8, c], ym),
        )

    def y2_landed(c):
        lo, hi = block(2, c, 0), block(2, c, 1)
        return (
            rcopy(lo, lo, csend.at[7], crecv.at[7, c], yp),
            rcopy(hi, hi, csend.at[8], crecv.at[8, c], ym),
        )

    def share(j, c):
        blk = block(j, c)
        return rcopy(blk, blk, csend.at[9], crecv.at[9, c], sib)

    def shares_landed(c):
        four = sline.at[0 : 4 * q, cols(c)]
        rcopy(four, four, csend.at[9], crecv.at[9, c], sib).wait_recv()

    barrier = pltpu.get_barrier_semaphore()
    around = (sib, xp, xm, yp, ym, zp, zm)
    for other in around:
        pl.semaphore_signal(barrier, inc=1, device_id=other, device_id_type=MESH)
    for c in range(CHUNKS):
        load(c)
    own[...] = jnp.zeros_like(own)
    pl.semaphore_wait(barrier, len(around))
    for c in range(CHUNKS):
        swap(c)

    def gather_step(step):
        c = step
        if c < CHUNKS:
            loaded(c)
            away = 1 - zh
            psend[:, cols(c)] = (gown[away, :, cols(c)].astype(F32) + gsib[away, :, cols(c)].astype(F32)).astype(BF16)
            for cp in z1(c):
                cp.start()
        c = step - 1
        if 0 <= c < CHUNKS:
            for cp, fwd in zip(z1(c), z2(c)):
                cp.wait_recv()
                fwd.start()
        c = step - 2
        if 0 <= c < CHUNKS:
            for cp in z2(c):
                cp.wait_recv()
            own = gown[zh, :, cols(c)].astype(F32) + gsib[zh, :, cols(c)].astype(F32)
            far = jnp.concatenate([zrec[0, :, cols(c)], zrec[1, :, cols(c)]], axis=0).astype(F32)
            sline[rows(2 * y + k), cols(c)] = (own + far).astype(BF16)
            for cp in y1(c):
                cp.start()
            share(0, c).start()
        c = step - 3
        if 0 <= c < CHUNKS:
            for cp, fwd, j in zip(y1_landed(c), y2(c), (3, 1)):
                cp.wait_recv()
                fwd.start()
                share(j, c).start()
        c = step - 4
        if 0 <= c < CHUNKS:
            for cp in y2_landed(c):
                cp.wait_recv()
            share(2, c).start()

    turn = 2 * mod(y, 2) + lax.div(y, 2)
    strip = 4 * k + turn

    def tiles(n):
        for c in range(CHUNKS):
            if STARTS[c] // 4 == n:
                shares_landed(c)
        last = n // 2

        @pl.when(k == n % 2)
        def _():
            mine = pl.ds(pl.multiple_of((8 * last + strip) * bs, bs), bs)
            own[:, last * bs : (last + 1) * bs] = sline[:, mine]

        lhs = sline[:, 4 * n * bs : 4 * (n + 1) * bs]
        acc = lax.dot_general(
            lhs, own[:, : count(n) * bs], (((0,), (0,)), ((), ())), preferred_element_type=F32
        )
        for m in range(count(n)):
            for p in range(4):
                t[first(n) + m, p] = acc[p * bs : (p + 1) * bs, m * bs : (m + 1) * bs].astype(BF16)

    def quarter(v):
        return pl.ds(pl.multiple_of(v * b4, b4), b4)

    parts = []
    for n in range(STAGES):
        a, b = first(n), first(n + 1)
        h = b if n < BETA_FROM else a + (b - a + 1) // 2
        parts.append([(a, h, True)] + ([(h, b, False)] if h < b else []))
    rings1, rings2, used = [], [], 0
    for n in range(STAGES):
        ones, twos = [], []
        for a, b, x_first in parts[n]:
            along = ((x, xp, xm), (z, zp, zm))
            one, two = along if x_first else along[::-1]
            ones.append(Ring(
                *one, (a, b),
                lambda p, a, b: t.at[a:b, p],
                lambda p, m: t[m, p].astype(F32),
                [l1.at[i] for i in range(4)],
                l1.at[0:2],
                rsend.at[0], rrecv.at[0, used],
            ))
            across = (zpp if x_first else xpp, two[1], two[2])
            twos.append(Spread(
                two[0], across, (a, b),
                lambda v, a, b: xb.at[a:b, quarter(v), :],
                lambda v, m: xf[m, quarter(v), :],
                l2, rsend.at[1, 0], rrecv.at[1, used, 0],
            ))
            used += 1
        rings1.append(ones)
        rings2.append(twos)

    def exchange(n):
        for a, b, x_first in parts[n]:
            p1, p2 = (x, z) if x_first else (z, x)
            rblk = block_of(p1, n)

            def one(f, up, side):
                m = f - first(n)
                stage = 2 * m + k
                cblk = block_of(turn, stage)
                wanted = (stage <= n) if side == 0 else (stage < n)
                rr, cc = (rblk, cblk) if side == 0 else (cblk, rblk)
                tx, tc = lax.div(rr, 12), lax.div(cc, 6)
                src = o.at[f]
                dst = u.at[mod(rr, 12), mod(cc, 6), quarter(p2), :]
                ty, tz = mod(tc, 4), 2 * up + lax.div(tc, 4)
                mine = (tx == x) & (ty == y) & (tz == z)

                @pl.when(wanted & jnp.logical_not(mine))
                def _():
                    rcopy(src, dst, fsem.at[0], fsem.at[1], dev(tx, ty, tz, k)).start()

                @pl.when(wanted & mine)
                def _():
                    pltpu.make_async_copy(src, dst, fsem.at[1]).start()
                    pltpu.make_async_copy(src, spare.at[f, 2 * side + up], fsem.at[0]).start()

            @pl.loop(a, b)
            def _(f):
                for side in (0, 1):
                    for up in (0, 1):
                        one(f, up, side)

    def begin(n):
        tiles(n)
        for r in rings1[n]:
            r.start()

    def pass1(n):
        for r in rings1[n]:
            r.pass_on()

    def reduce1(n):
        def put(m, v):
            xf[m] = v
            xb[m] = v.astype(BF16)

        for r, r2 in zip(rings1[n], rings2[n]):
            r.result(put)
            r2.start()

    def reduce2(n):
        def put(m, v):
            o[m] = v.astype(BF16)

        for r in rings2[n]:
            r.result(put)
        exchange(n)

    rounds = {}
    for n in range(STAGES):
        lags = (0, 1, 3, 4) if n < 7 else (0, 1, 2, 3)
        for place, (lag, what) in enumerate(zip(lags, (begin, pass1, reduce1, reduce2))):
            rounds.setdefault(n + 5 + lag, []).append((place, n, what))
    final = CHUNKS + 3
    for step in range(final):
        gather_step(step)
        for _, n, what in sorted(rounds.get(step, ()), key=lambda item: item[:2]):
            what(n)
    gather_step(final)
    for what, n in (
        (begin, 10), (pass1, 9), (reduce1, 8), (begin, 11), (reduce1, 9), (pass1, 10), (reduce2, 6), (reduce2, 7),
        (pass1, 11), (reduce2, 8), (reduce1, 10), (reduce2, 9), (reduce1, 11), (reduce2, 10), (reduce2, 11),
    ):
        what(n)

    def sent(n, ref):
        rcopy(ref, ref, csend.at[n], crecv.at[0, 0], sib).wait_send()

    sent(0, gsib)
    for n in (1, 2, 3, 4):
        sent(n, zrel.at[0])
    for n in (5, 6):
        sent(n, psend)
    sent(9, sline.at[0 : 4 * q])
    for n in (7, 8):
        sent(n, zrel.at[0])

    ups = sum((hi - lo + 1) // 2 for ps in parts for lo, hi, _ in ps)
    for half_, blocks in ((0, ups), (1, TOTAL - ups)):
        done = l1.at[0:3, 0:blocks]
        rcopy(done, done, rsend.at[0, half_], rrecv.at[0, 0, 0], sib).wait_send()
    rcopy(l2, l2, rsend.at[1, 0], rrecv.at[0, 0, 0], sib).wait_send()

    sized = (l1.at[0, 0:39], l1.at[0, 0:33])
    for core in (0, 1):

        @pl.when(k == core)
        def _():
            rcopy(sized[core], sized[core], fsem.at[0], fsem.at[1], sib).wait_recv()
            rcopy(sized[core], sized[core], fsem.at[0], fsem.at[1], sib).wait_send()

    @pl.loop(0, 12)
    def _(i):
        for j in range(6):
            direct = mod(i + 6 * lax.div(x, 2), 12) >= 6 * mod(col + zl, 2) + j
            from_me = jnp.where(direct, j % 2, mod(i, 2)) == k

            @pl.when(from_me)
            def _():
                rcopy(u.at[i, j], out.at[i, j], dsem.at[0], dsem.at[1], sib).start()
                pltpu.make_async_copy(u.at[i, j], out.at[i, j], lsem.at[0]).start()

    for core in (0, 1):

        @pl.when(k == core)
        def _():
            rcopy(sized[1 - core], sized[1 - core], dsem.at[0], dsem.at[1], sib).wait_recv()
            rcopy(sized[core], sized[core], dsem.at[0], dsem.at[1], sib).wait_send()
            pltpu.make_async_copy(sized[core], sized[core], lsem.at[0]).wait()


def gather_blocks(grad):
    _, n, d = grad.shape
    q, bs = n // 4, BLOCK
    b4 = bs // 4
    subs = STAGES + STAGES - BETA_FROM
    vm = pltpu.VMEM
    dma = pltpu.SemaphoreType.DMA
    return pl.pallas_call(
        kernel,
        out_shape=jax.ShapeDtypeStruct((12, 6, bs, bs), BF16),
        in_specs=[pl.BlockSpec(memory_space=pl.ANY)],
        out_specs=pl.BlockSpec(memory_space=pl.ANY),
        scratch_shapes=[
            vm((2, q, d), BF16), vm((2, q, d), BF16), vm((q, d), BF16),
            vm((2, q // 2, d), BF16), vm((2, q // 2, d), BF16),
            vm((8 * q, d), BF16), vm((8 * q, d // 8), BF16), vm((TOTAL, 4, bs, bs), BF16),
            vm((4, TOTAL, bs, bs), BF16), vm((3, TOTAL, b4, bs), BF16),
            vm((TOTAL, bs, bs), F32), vm((TOTAL, bs, bs), BF16),
            vm((TOTAL, b4, bs), BF16), vm((12, 6, bs, bs), BF16), vm((TOTAL, 4, b4, bs), BF16),
            dma((CHUNKS,)), dma((10,)), dma((10, CHUNKS)), dma((2, 2)), dma((2, subs, 3)), dma((2,)), dma((2,)),
        ],
        compiler_params=pltpu.CompilerParams(collective_id=0, has_side_effects=True, vmem_limit_bytes=56 * 1024 * 1024),
    )(grad.reshape(2, 2, q, d))


def finish(blocks, statistic, gram, following, ub, st, gr, fo, insem, outsem):
    n = ub.shape[-1]
    col = lax.axis_index("col")
    col0 = 6 * mod(col + lax.div(col, 4), 2)
    row0 = 6 * lax.div(lax.axis_index("row"), 2)

    def band(i):
        return pl.ds(pl.multiple_of(i * n, n), n)

    def reads(i):
        return (
            pltpu.make_async_copy(blocks.at[i], ub.at[i], insem.at[0, i]),
            pltpu.make_async_copy(statistic.at[band(i), :], st.at[band(i), :], insem.at[1, i]),
        )

    @pl.loop(0, 12)
    def _(i):
        for cp in reads(i):
            cp.start()

    @pl.loop(0, 12)
    def _(i):
        for cp in reads(i):
            cp.wait()
        rows = (band(i), slice(None))
        for j in range(6):
            at = (band(i), slice(j * n, (j + 1) * n))
            block = ub[i, j].astype(F32)
            value = jnp.where(mod(i + row0, 12) >= col0 + j, block, block.T)
            gr[at] = value
            fo[at] = 0.95 * st[at] + 0.05 * value
        pltpu.make_async_copy(gr.at[rows], gram.at[rows], outsem.at[0]).start()
        pltpu.make_async_copy(fo.at[rows], following.at[rows], outsem.at[1]).start()

    pltpu.make_async_copy(gr, gram, outsem.at[0]).wait()
    pltpu.make_async_copy(fo, following, outsem.at[1]).wait()


def shards(grad, statistic):
    blocks = gather_blocks(grad)
    shape = jax.ShapeDtypeStruct(statistic.shape, F32)
    whole = pltpu.VMEM(statistic.shape, F32)
    dma = pltpu.SemaphoreType.DMA
    return pl.pallas_call(
        finish,
        out_shape=(shape, shape),
        in_specs=[pl.BlockSpec(memory_space=pl.ANY)] * 2,
        out_specs=(pl.BlockSpec(memory_space=pl.ANY),) * 2,
        scratch_shapes=[pltpu.VMEM(blocks.shape, BF16), whole, whole, whole, dma((2, 12)), dma((2,))],
        compiler_params=pltpu.CompilerParams(vmem_limit_bytes=60 * 1024 * 1024),
    )(blocks, statistic)


def solution(mesh):
    return jax.shard_map(
        shards,
        mesh=mesh,
        in_specs=(P("rep", ("row", "col"), None), P("row", "col")),
        out_specs=(P("row", "col"), P("row", "col")),
        check_vma=False,
    )
```

```python
import functools

import jax
import jax.numpy as jnp
from jax import lax
from jax.experimental import pallas as pl
from jax.experimental.pallas import tpu as pltpu
from jax.sharding import PartitionSpec as P

MESH = pl.DeviceIdType.MESH
BF16 = jnp.bfloat16
F32 = jnp.float32
BLOCK = 128
STAGES = 12
WIDTHS = (4,) * 12
STARTS = tuple(sum(WIDTHS[:i]) for i in range(len(WIDTHS)))
CHUNKS = len(WIDTHS)
BETA_FROM = 8


def count(n):
    return n // 2 + 1


def first(n):
    return sum(count(i) for i in range(n))


TOTAL = first(STAGES)


def halved(v):
    return v // 2 if isinstance(v, int) else lax.div(v, 2)


def block_of(i, stage):
    upper = (halved(stage) + halved(i)) % 2 if isinstance(i, int) else mod(halved(stage) + halved(i), 2)
    odd = stage % 2 if isinstance(stage, int) else mod(stage, 2)
    return STAGES * i + 6 * upper + 2 * halved(halved(stage)) + odd


def stage_of(i, upper, place):
    return 4 * halved(place) + 2 * mod(upper + halved(i), 2) + (place % 2 if isinstance(place, int) else mod(place, 2))


def mod(a, n):
    return lax.rem(a, n)


def rcopy(src, dst, send, recv, device):
    return pltpu.make_async_remote_copy(
        src_ref=src, dst_ref=dst, send_sem=send, recv_sem=recv, device_id=device, device_id_type=MESH
    )


class Ring:
    def __init__(self, i, up, down, span, src, add, bufs, pair, sends, recvs):
        lo, hi = span
        mid = lo + (hi - lo + 1) // 2
        far, near, got, total = bufs
        at = lambda j: mod(i + j, 4)
        self.i, self.add, self.bufs, self.halves = i, add, bufs, []
        self.span, self.last, self.pair, self.up = span, recvs.at[2], pair, up
        for s, (a, b, long, short, j) in enumerate(((lo, mid, up, down, 3), (mid, hi, down, up, 1))):
            if a == b:
                continue
            cut = lambda ref: ref.at[a:b]
            self.halves.append((
                a, b, at(4 - j),
                rcopy(src(at(2), a, b), cut(far), sends.at[s], recvs.at[s], long),
                rcopy(src(at(j), a, b), cut(near), sends.at[s], recvs.at[2], short),
                rcopy(cut(total), cut(got), sends.at[s], recvs.at[2], long),
            ))

    def start(self):
        for h in self.halves:
            h[3].start()
        for h in self.halves:
            h[4].start()

    def pass_on(self):
        far, _, _, total = self.bufs
        for a, b, to, one, _, on in self.halves:
            one.wait_recv()

            @pl.loop(a, b)
            def _(m):
                total[m] = (far[m].astype(F32) + self.add(to, m)).astype(BF16)

            on.start()

    def result(self, put):
        _, near, got, _ = self.bufs
        both = self.pair.at[:, self.span[0] : self.span[1]]
        rcopy(both, both, self.last, self.last, self.up).wait_recv()
        for a, b, *_ in self.halves:

            @pl.loop(a, b)
            def _(m):
                put(m, self.add(self.i, m) + (near[m].astype(F32) + got[m].astype(F32)))


class Spread:
    def __init__(self, i, others, span, src, add, buf, send, recv):
        a, b = span
        self.i, self.add, self.buf, self.span = i, add, buf, span
        self.copies = [
            rcopy(src(mod(i + j, 4), a, b), buf.at[j - 1, a:b], send, recv, other) for j, other in zip((2, 1, 3), others)
        ]
        landed = buf.at[:, a:b]
        self.landed = rcopy(landed, landed, send, recv, others[0])

    def start(self):
        for c in self.copies:
            c.start()

    def result(self, put):
        self.landed.wait_recv()

        @pl.loop(*self.span)
        def _(m):
            theirs = (self.buf[0, m].astype(F32) + self.buf[1, m].astype(F32)) + self.buf[2, m].astype(F32)
            put(m, self.add(self.i, m) + theirs)


def kernel(
    g, out, gown, gsib, psend, zrel, zrec, sline, own, t, l1, l2, xf, xb, o, u, spare,
    lsem, csend, crecv, rsend, rrecv, fsem, dsem,
):
    rep, x, col = lax.axis_index("rep"), lax.axis_index("row"), lax.axis_index("col")
    zh, k = lax.div(rep, 2), mod(rep, 2)
    zl, y = lax.div(col, 4), mod(col, 4)
    z = 2 * zh + zl
    q, d = psend.shape
    half = q // 2
    bs = BLOCK
    b4 = bs // 4

    def dev(x, y, z, k):
        return {"rep": lax.div(z, 2) * 2 + k, "row": x, "col": mod(z, 2) * 4 + y}

    sib = dev(x, y, z, 1 - k)
    zp, zm = dev(x, y, mod(z + 1, 4), k), dev(x, y, mod(z + 3, 4), k)
    yp, ym = dev(x, mod(y + 1, 4), z, k), dev(x, mod(y + 3, 4), z, k)
    xp, xm = dev(mod(x + 1, 4), y, z, k), dev(mod(x + 3, 4), y, z, k)

    xpp, zpp = dev(mod(x + 2, 4), y, z, k), dev(x, y, mod(z + 2, 4), k)

    def cols(c):
        return slice(STARTS[c] * bs, (STARTS[c] + WIDTHS[c]) * bs)

    def rows(i):
        return pl.ds(pl.multiple_of(i * q, q), q)

    def strided(c):
        return [(pl.ds(block_of(i, c) * bs, bs), pl.ds((4 * c + i) * bs, bs)) for i in range(4)]

    def load(c):
        for there, here in strided(c):
            pltpu.make_async_copy(g.at[:, k, :, there], gown.at[:, :, here], lsem.at[c]).start()

    def swap(c):
        for there, here in strided(c):
            rcopy(g.at[:, 1 - k, :, there], gsib.at[:, :, here], csend.at[0], crecv.at[0, c], sib).start()

    def loaded(c):
        whole = gown.at[:, :, cols(c)]
        pltpu.make_async_copy(whole, whole, lsem.at[c]).wait()
        whole = gsib.at[:, :, cols(c)]
        rcopy(whole, whole, csend.at[0], crecv.at[0, c], sib).wait_recv()

    def z1(c):
        return (
            rcopy(psend.at[0:half, cols(c)], zrel.at[0, :, cols(c)], csend.at[1], crecv.at[1, c], zp),
            rcopy(psend.at[half:q, cols(c)], zrel.at[1, :, cols(c)], csend.at[2], crecv.at[2, c], zm),
        )

    def z2(c):
        return (
            rcopy(zrel.at[0, :, cols(c)], zrec.at[0, :, cols(c)], csend.at[3], crecv.at[3, c], zp),
            rcopy(zrel.at[1, :, cols(c)], zrec.at[1, :, cols(c)], csend.at[4], crecv.at[4, c], zm),
        )

    def block(j, c, part=None):
        base = (2 * mod(y + j, 4) + k) * q
        if part is None:
            return sline.at[pl.ds(pl.multiple_of(base, q), q), cols(c)]
        return sline.at[pl.ds(pl.multiple_of(base + part * half, half), half), cols(c)]

    def y1(c):
        own = block(0, c)
        return (
            rcopy(own, own, csend.at[5], crecv.at[5, c], yp),
            rcopy(own, own, csend.at[6], crecv.at[6, c], ym),
        )

    def y1_landed(c):
        down, upper = block(3, c), block(1, c)
        return (
            rcopy(down, down, csend.at[5], crecv.at[5, c], yp),
            rcopy(upper, upper, csend.at[6], crecv.at[6, c], ym),
        )

    def y2(c):
        down, upper = block(3, c, 0), block(1, c, 1)
        return (
            rcopy(down, down, csend.at[7], crecv.at[7, c], yp),
            rcopy(upper, upper, csend.at[8], crecv.at[8, c], ym),
        )

    def y2_landed(c):
        lo, hi = block(2, c, 0), block(2, c, 1)
        return (
            rcopy(lo, lo, csend.at[7], crecv.at[7, c], yp),
            rcopy(hi, hi, csend.at[8], crecv.at[8, c], ym),
        )

    def share(j, c):
        blk = block(j, c)
        return rcopy(blk, blk, csend.at[9], crecv.at[9, c], sib)

    def shares_landed(c):
        four = sline.at[0 : 4 * q, cols(c)]
        rcopy(four, four, csend.at[9], crecv.at[9, c], sib).wait_recv()

    barrier = pltpu.get_barrier_semaphore()
    around = (sib, xp, xm, yp, ym, zp, zm)
    for other in around:
        pl.semaphore_signal(barrier, inc=1, device_id=other, device_id_type=MESH)
    for c in range(CHUNKS):
        load(c)
    own[...] = jnp.zeros_like(own)
    pl.semaphore_wait(barrier, len(around))
    for c in range(CHUNKS):
        swap(c)

    def gather_step(step):
        c = step
        if c < CHUNKS:
            loaded(c)
            away = 1 - zh
            psend[:, cols(c)] = (gown[away, :, cols(c)].astype(F32) + gsib[away, :, cols(c)].astype(F32)).astype(BF16)
            for cp in z1(c):
                cp.start()
        c = step - 1
        if 0 <= c < CHUNKS:
            for cp, fwd in zip(z1(c), z2(c)):
                cp.wait_recv()
                fwd.start()
        c = step - 2
        if 0 <= c < CHUNKS:
            for cp in z2(c):
                cp.wait_recv()
            own = gown[zh, :, cols(c)].astype(F32) + gsib[zh, :, cols(c)].astype(F32)
            far = jnp.concatenate([zrec[0, :, cols(c)], zrec[1, :, cols(c)]], axis=0).astype(F32)
            sline[rows(2 * y + k), cols(c)] = (own + far).astype(BF16)
            for cp in y1(c):
                cp.start()
            share(0, c).start()
        c = step - 3
        if 0 <= c < CHUNKS:
            for cp, fwd, j in zip(y1_landed(c), y2(c), (3, 1)):
                cp.wait_recv()
                fwd.start()
                share(j, c).start()
        c = step - 4
        if 0 <= c < CHUNKS:
            for cp in y2_landed(c):
                cp.wait_recv()
            share(2, c).start()

    turn = 2 * mod(y, 2) + lax.div(y, 2)

    def quarter_of(m):
        return mod(turn + 2 * m + 2 * k, 4)


    def tiles(n):
        for c in range(CHUNKS):
            if STARTS[c] // 4 == n:
                shares_landed(c)
        last = n // 2

        @pl.when(k == n % 2)
        def _():
            mine = pl.ds(pl.multiple_of((4 * n + quarter_of(last)) * bs, bs), bs)
            own[:, last * bs : (last + 1) * bs] = sline[:, mine]

        lhs = sline[:, 4 * n * bs : 4 * (n + 1) * bs]
        acc = lax.dot_general(
            lhs, own[:, : count(n) * bs], (((0,), (0,)), ((), ())), preferred_element_type=F32
        )
        for m in range(count(n)):
            for p in range(4):
                t[first(n) + m, p] = acc[p * bs : (p + 1) * bs, m * bs : (m + 1) * bs].astype(BF16)

    def quarter(v):
        return pl.ds(pl.multiple_of(v * b4, b4), b4)

    parts = []
    for n in range(STAGES):
        a, b = first(n), first(n + 1)
        h = b if n < BETA_FROM else a + (b - a + 1) // 2
        parts.append([(a, h, True)] + ([(h, b, False)] if h < b else []))
    rings1, rings2, used = [], [], 0
    for n in range(STAGES):
        ones, twos = [], []
        for a, b, x_first in parts[n]:
            along = ((x, xp, xm), (z, zp, zm))
            one, two = along if x_first else along[::-1]
            ones.append(Ring(
                *one, (a, b),
                lambda p, a, b: t.at[a:b, p],
                lambda p, m: t[m, p].astype(F32),
                [l1.at[i] for i in range(4)],
                l1.at[0:2],
                rsend.at[0], rrecv.at[0, used],
            ))
            across = (zpp if x_first else xpp, two[1], two[2])
            twos.append(Spread(
                two[0], across, (a, b),
                lambda v, a, b: xb.at[a:b, quarter(v), :],
                lambda v, m: xf[m, quarter(v), :],
                l2, rsend.at[1, 0], rrecv.at[1, used, 0],
            ))
            used += 1
        rings1.append(ones)
        rings2.append(twos)

    def exchange(n):
        for a, b, x_first in parts[n]:
            p1, p2 = (x, z) if x_first else (z, x)
            rblk = block_of(p1, n)

            def one(f, up, side):
                m = f - first(n)
                stage = 2 * m + k
                cblk = block_of(quarter_of(m), stage)
                wanted = (stage <= n) if side == 0 else (stage < n)
                rr, cc = (rblk, cblk) if side == 0 else (cblk, rblk)
                tx, tc = lax.div(rr, 12), lax.div(cc, 6)
                src = o.at[f]
                dst = u.at[mod(rr, 12), mod(cc, 6), quarter(p2), :]
                ty, tz = mod(tc, 4), 2 * up + lax.div(tc, 4)
                mine = (tx == x) & (ty == y) & (tz == z)

                @pl.when(wanted & jnp.logical_not(mine))
                def _():
                    rcopy(src, dst, fsem.at[0], fsem.at[1], dev(tx, ty, tz, k)).start()

                @pl.when(wanted & mine)
                def _():
                    pltpu.make_async_copy(src, dst, fsem.at[1]).start()
                    pltpu.make_async_copy(src, spare.at[f, 2 * side + up], fsem.at[0]).start()

            @pl.loop(a, b)
            def _(f):
                for side in (0, 1):
                    for up in (0, 1):
                        one(f, up, side)

    def begin(n):
        tiles(n)
        for r in rings1[n]:
            r.start()

    def pass1(n):
        for r in rings1[n]:
            r.pass_on()

    def reduce1(n):
        def put(m, v):
            xf[m] = v
            xb[m] = v.astype(BF16)

        for r, r2 in zip(rings1[n], rings2[n]):
            r.result(put)
            r2.start()

    def reduce2(n):
        def put(m, v):
            o[m] = v.astype(BF16)

        for r in rings2[n]:
            r.result(put)
        exchange(n)

    rounds = {}
    for n in range(STAGES):
        lags = (0, 1, 3, 4) if n < 7 else (0, 1, 2, 3)
        for place, (lag, what) in enumerate(zip(lags, (begin, pass1, reduce1, reduce2))):
            rounds.setdefault(n + 5 + lag, []).append((place, n, what))
    final = CHUNKS + 3
    for step in range(final):
        gather_step(step)
        for _, n, what in sorted(rounds.get(step, ()), key=lambda item: item[:2]):
            what(n)
    gather_step(final)
    for what, n in (
        (begin, 10), (pass1, 9), (reduce1, 8), (begin, 11), (reduce1, 9), (pass1, 10), (reduce2, 6), (reduce2, 7),
        (pass1, 11), (reduce2, 8), (reduce1, 10), (reduce2, 9), (reduce1, 11), (reduce2, 10), (reduce2, 11),
    ):
        what(n)

    def sent(n, ref):
        rcopy(ref, ref, csend.at[n], crecv.at[0, 0], sib).wait_send()

    sent(0, gsib)
    for n in (1, 2, 3, 4):
        sent(n, zrel.at[0])
    for n in (5, 6):
        sent(n, psend)
    sent(9, sline.at[0 : 4 * q])
    for n in (7, 8):
        sent(n, zrel.at[0])

    ups = sum((hi - lo + 1) // 2 for ps in parts for lo, hi, _ in ps)
    for half_, blocks in ((0, ups), (1, TOTAL - ups)):
        done = l1.at[0:3, 0:blocks]
        rcopy(done, done, rsend.at[0, half_], rrecv.at[0, 0, 0], sib).wait_send()
    rcopy(l2, l2, rsend.at[1, 0], rrecv.at[0, 0, 0], sib).wait_send()

    sized = (l1.at[0, 0:39], l1.at[0, 0:33])
    for core in (0, 1):

        @pl.when(k == core)
        def _():
            rcopy(sized[core], sized[core], fsem.at[0], fsem.at[1], sib).wait_recv()
            rcopy(sized[core], sized[core], fsem.at[0], fsem.at[1], sib).wait_send()

    @pl.loop(0, 12)
    def _(i):
        for j in range(6):
            direct = stage_of(x, lax.div(i, 6), mod(i, 6)) >= stage_of(halved(col), mod(col, 2), j)
            from_me = jnp.where(direct, j % 2, mod(i, 2)) == k

            @pl.when(from_me)
            def _():
                rcopy(u.at[i, j], out.at[i, j], dsem.at[0], dsem.at[1], sib).start()
                pltpu.make_async_copy(u.at[i, j], out.at[i, j], lsem.at[0]).start()

    for core in (0, 1):

        @pl.when(k == core)
        def _():
            rcopy(sized[1 - core], sized[1 - core], dsem.at[0], dsem.at[1], sib).wait_recv()
            rcopy(sized[core], sized[core], dsem.at[0], dsem.at[1], sib).wait_send()
            pltpu.make_async_copy(sized[core], sized[core], lsem.at[0]).wait()


def gather_blocks(grad):
    _, n, d = grad.shape
    q, bs = n // 4, BLOCK
    b4 = bs // 4
    subs = STAGES + STAGES - BETA_FROM
    vm = pltpu.VMEM
    dma = pltpu.SemaphoreType.DMA
    return pl.pallas_call(
        kernel,
        out_shape=jax.ShapeDtypeStruct((12, 6, bs, bs), BF16),
        in_specs=[pl.BlockSpec(memory_space=pl.ANY)],
        out_specs=pl.BlockSpec(memory_space=pl.ANY),
        scratch_shapes=[
            vm((2, q, d), BF16), vm((2, q, d), BF16), vm((q, d), BF16),
            vm((2, q // 2, d), BF16), vm((2, q // 2, d), BF16),
            vm((8 * q, d), BF16), vm((8 * q, d // 8), BF16), vm((TOTAL, 4, bs, bs), BF16),
            vm((4, TOTAL, bs, bs), BF16), vm((3, TOTAL, b4, bs), BF16),
            vm((TOTAL, bs, bs), F32), vm((TOTAL, bs, bs), BF16),
            vm((TOTAL, b4, bs), BF16), vm((12, 6, bs, bs), BF16), vm((TOTAL, 4, b4, bs), BF16),
            dma((CHUNKS,)), dma((10,)), dma((10, CHUNKS)), dma((2, 2)), dma((2, subs, 3)), dma((2,)), dma((2,)),
        ],
        compiler_params=pltpu.CompilerParams(collective_id=0, has_side_effects=True, vmem_limit_bytes=56 * 1024 * 1024),
    )(grad.reshape(2, 2, q, d))


def finish(blocks, statistic, gram, following, ub, st, gr, fo, insem, outsem):
    n = ub.shape[-1]
    col = lax.axis_index("col")
    row = lax.axis_index("row")

    def band(i):
        return pl.ds(pl.multiple_of(i * n, n), n)

    def reads(i):
        return (
            pltpu.make_async_copy(blocks.at[i], ub.at[i], insem.at[0, i]),
            pltpu.make_async_copy(statistic.at[band(i), :], st.at[band(i), :], insem.at[1, i]),
        )

    @pl.loop(0, 12)
    def _(i):
        for cp in reads(i):
            cp.start()

    @pl.loop(0, 12)
    def _(i):
        for cp in reads(i):
            cp.wait()
        rows = (band(i), slice(None))
        for j in range(6):
            at = (band(i), slice(j * n, (j + 1) * n))
            block = ub[i, j].astype(F32)
            direct = stage_of(row, lax.div(i, 6), mod(i, 6)) >= stage_of(halved(col), mod(col, 2), j)
            value = jnp.where(direct, block, block.T)
            gr[at] = value
            fo[at] = 0.95 * st[at] + 0.05 * value
        pltpu.make_async_copy(gr.at[rows], gram.at[rows], outsem.at[0]).start()
        pltpu.make_async_copy(fo.at[rows], following.at[rows], outsem.at[1]).start()

    pltpu.make_async_copy(gr, gram, outsem.at[0]).wait()
    pltpu.make_async_copy(fo, following, outsem.at[1]).wait()


def shards(grad, statistic):
    blocks = gather_blocks(grad)
    shape = jax.ShapeDtypeStruct(statistic.shape, F32)
    whole = pltpu.VMEM(statistic.shape, F32)
    dma = pltpu.SemaphoreType.DMA
    return pl.pallas_call(
        finish,
        out_shape=(shape, shape),
        in_specs=[pl.BlockSpec(memory_space=pl.ANY)] * 2,
        out_specs=(pl.BlockSpec(memory_space=pl.ANY),) * 2,
        scratch_shapes=[pltpu.VMEM(blocks.shape, BF16), whole, whole, whole, dma((2, 12)), dma((2,))],
        compiler_params=pltpu.CompilerParams(vmem_limit_bytes=60 * 1024 * 1024),
    )(blocks, statistic)


def solution(mesh):
    return jax.shard_map(
        shards,
        mesh=mesh,
        in_specs=(P("rep", ("row", "col"), None), P("row", "col")),
        out_specs=(P("row", "col"), P("row", "col")),
        check_vma=False,
    )
```

```python
import functools

import jax
import jax.numpy as jnp
from jax import lax
from jax.experimental import pallas as pl
from jax.experimental.pallas import tpu as pltpu
from jax.sharding import PartitionSpec as P

MESH = pl.DeviceIdType.MESH
BF16 = jnp.bfloat16
F32 = jnp.float32
BLOCK = 128
STAGES = 12
WIDTHS = (4,) * 12
STARTS = tuple(sum(WIDTHS[:i]) for i in range(len(WIDTHS)))
CHUNKS = len(WIDTHS)
BETA_FROM = 8


def count(n):
    return n // 2 + 1


def first(n):
    return sum(count(i) for i in range(n))


TOTAL = first(STAGES)


def halved(v):
    return v // 2 if isinstance(v, int) else lax.div(v, 2)


def block_of(i, stage):
    upper = (halved(stage) + halved(i)) % 2 if isinstance(i, int) else mod(halved(stage) + halved(i), 2)
    odd = stage % 2 if isinstance(stage, int) else mod(stage, 2)
    return STAGES * i + 6 * upper + 2 * halved(halved(stage)) + odd


def stage_of(i, upper, place):
    return 4 * halved(place) + 2 * mod(upper + halved(i), 2) + (place % 2 if isinstance(place, int) else mod(place, 2))


def mod(a, n):
    return lax.rem(a, n)


def rcopy(src, dst, send, recv, device):
    return pltpu.make_async_remote_copy(
        src_ref=src, dst_ref=dst, send_sem=send, recv_sem=recv, device_id=device, device_id_type=MESH
    )


class Ring:
    def __init__(self, i, up, down, span, src, add, bufs, pair, sends, recvs):
        lo, hi = span
        mid = lo + (hi - lo + 1) // 2
        far, near, got, total = bufs
        at = lambda j: mod(i + j, 4)
        self.i, self.add, self.bufs, self.halves = i, add, bufs, []
        self.span, self.last, self.pair, self.up = span, recvs.at[2], pair, up
        for s, (a, b, long, short, j) in enumerate(((lo, mid, up, down, 3), (mid, hi, down, up, 1))):
            if a == b:
                continue
            cut = lambda ref: ref.at[a:b]
            self.halves.append((
                a, b, at(4 - j),
                rcopy(src(at(2), a, b), cut(far), sends.at[s], recvs.at[s], long),
                rcopy(src(at(j), a, b), cut(near), sends.at[s], recvs.at[2], short),
                rcopy(cut(total), cut(got), sends.at[s], recvs.at[2], long),
            ))

    def start(self):
        for h in self.halves:
            h[3].start()
        for h in self.halves:
            h[4].start()

    def pass_on(self):
        far, _, _, total = self.bufs
        for a, b, to, one, _, on in self.halves:
            one.wait_recv()

            @pl.loop(a, b)
            def _(m):
                total[m] = (far[m].astype(F32) + self.add(to, m)).astype(BF16)

            on.start()

    def result(self, put):
        _, near, got, _ = self.bufs
        both = self.pair.at[:, self.span[0] : self.span[1]]
        rcopy(both, both, self.last, self.last, self.up).wait_recv()
        for a, b, *_ in self.halves:

            @pl.loop(a, b)
            def _(m):
                put(m, self.add(self.i, m) + (near[m].astype(F32) + got[m].astype(F32)))


class Spread:
    def __init__(self, i, others, span, src, add, buf, send, recv):
        a, b = span
        self.i, self.add, self.buf, self.span = i, add, buf, span
        self.copies = [
            rcopy(src(mod(i + j, 4), a, b), buf.at[j - 1, a:b], send, recv, other) for j, other in zip((2, 1, 3), others)
        ]
        landed = buf.at[:, a:b]
        self.landed = rcopy(landed, landed, send, recv, others[0])

    def start(self):
        for c in self.copies:
            c.start()

    def result(self, put):
        self.landed.wait_recv()

        @pl.loop(*self.span)
        def _(m):
            theirs = (self.buf[0, m].astype(F32) + self.buf[1, m].astype(F32)) + self.buf[2, m].astype(F32)
            put(m, self.add(self.i, m) + theirs)


def kernel(
    g, out, gown, gsib, psend, zrel, zrec, sline, own, t, l1, l2, xf, xb, o, u, spare,
    lsem, csend, crecv, rsend, rrecv, fsem, dsem,
):
    rep, x, col = lax.axis_index("rep"), lax.axis_index("row"), lax.axis_index("col")
    zh, k = lax.div(rep, 2), mod(rep, 2)
    zl, y = lax.div(col, 4), mod(col, 4)
    z = 2 * zh + zl
    q, d = psend.shape
    half = q // 2
    bs = BLOCK
    b4 = bs // 4

    def dev(x, y, z, k):
        return {"rep": lax.div(z, 2) * 2 + k, "row": x, "col": mod(z, 2) * 4 + y}

    sib = dev(x, y, z, 1 - k)
    zp, zm = dev(x, y, mod(z + 1, 4), k), dev(x, y, mod(z + 3, 4), k)
    yp, ym = dev(x, mod(y + 1, 4), z, k), dev(x, mod(y + 3, 4), z, k)
    xp, xm = dev(mod(x + 1, 4), y, z, k), dev(mod(x + 3, 4), y, z, k)

    xpp, zpp = dev(mod(x + 2, 4), y, z, k), dev(x, y, mod(z + 2, 4), k)

    def cols(c):
        return slice(STARTS[c] * bs, (STARTS[c] + WIDTHS[c]) * bs)

    def rows(i):
        return pl.ds(pl.multiple_of(i * q, q), q)

    def strided(c):
        return [(pl.ds(block_of(i, c) * bs, bs), pl.ds((4 * c + i) * bs, bs)) for i in range(4)]

    def load(c):
        for there, here in strided(c):
            pltpu.make_async_copy(g.at[:, k, :, there], gown.at[:, :, here], lsem.at[c]).start()

    def swap(c):
        for there, here in strided(c):
            rcopy(g.at[:, 1 - k, :, there], gsib.at[:, :, here], csend.at[0], crecv.at[0, c], sib).start()

    def loaded(c):
        whole = gown.at[:, :, cols(c)]
        pltpu.make_async_copy(whole, whole, lsem.at[c]).wait()
        whole = gsib.at[:, :, cols(c)]
        rcopy(whole, whole, csend.at[0], crecv.at[0, c], sib).wait_recv()

    def z1(c):
        return (
            rcopy(psend.at[0:half, cols(c)], zrel.at[0, :, cols(c)], csend.at[1], crecv.at[1, c], zp),
            rcopy(psend.at[half:q, cols(c)], zrel.at[1, :, cols(c)], csend.at[2], crecv.at[2, c], zm),
        )

    def z2(c):
        return (
            rcopy(zrel.at[0, :, cols(c)], zrec.at[0, :, cols(c)], csend.at[3], crecv.at[3, c], zp),
            rcopy(zrel.at[1, :, cols(c)], zrec.at[1, :, cols(c)], csend.at[4], crecv.at[4, c], zm),
        )

    def block(j, c, part=None):
        base = (2 * mod(y + j, 4) + k) * q
        if part is None:
            return sline.at[pl.ds(pl.multiple_of(base, q), q), cols(c)]
        return sline.at[pl.ds(pl.multiple_of(base + part * half, half), half), cols(c)]

    def y1(c):
        own = block(0, c)
        return (
            rcopy(own, own, csend.at[5], crecv.at[5, c], yp),
            rcopy(own, own, csend.at[6], crecv.at[6, c], ym),
        )

    def y1_landed(c):
        down, upper = block(3, c), block(1, c)
        return (
            rcopy(down, down, csend.at[5], crecv.at[5, c], yp),
            rcopy(upper, upper, csend.at[6], crecv.at[6, c], ym),
        )

    def y2(c):
        down, upper = block(3, c, 0), block(1, c, 1)
        return (
            rcopy(down, down, csend.at[7], crecv.at[7, c], yp),
            rcopy(upper, upper, csend.at[8], crecv.at[8, c], ym),
        )

    def y2_landed(c):
        lo, hi = block(2, c, 0), block(2, c, 1)
        return (
            rcopy(lo, lo, csend.at[7], crecv.at[7, c], yp),
            rcopy(hi, hi, csend.at[8], crecv.at[8, c], ym),
        )

    def share(j, c):
        blk = block(j, c)
        return rcopy(blk, blk, csend.at[9], crecv.at[9, c], sib)

    def shares_landed(c):
        four = sline.at[0 : 4 * q, cols(c)]
        rcopy(four, four, csend.at[9], crecv.at[9, c], sib).wait_recv()

    barrier = pltpu.get_barrier_semaphore()
    around = (sib, xp, xm, yp, ym, zp, zm)
    for other in around:
        pl.semaphore_signal(barrier, inc=1, device_id=other, device_id_type=MESH)
    for c in range(CHUNKS):
        load(c)
    own[...] = jnp.zeros_like(own)
    pl.semaphore_wait(barrier, len(around))
    for c in range(CHUNKS):
        swap(c)

    def gather_step(step):
        c = step
        if c < CHUNKS:
            loaded(c)
            away = 1 - zh
            psend[:, cols(c)] = (gown[away, :, cols(c)].astype(F32) + gsib[away, :, cols(c)].astype(F32)).astype(BF16)
            for cp in z1(c):
                cp.start()
        c = step - 1
        if 0 <= c < CHUNKS:
            for cp, fwd in zip(z1(c), z2(c)):
                cp.wait_recv()
                fwd.start()
        c = step - 2
        if 0 <= c < CHUNKS:
            for cp in z2(c):
                cp.wait_recv()
            own = gown[zh, :, cols(c)].astype(F32) + gsib[zh, :, cols(c)].astype(F32)
            far = jnp.concatenate([zrec[0, :, cols(c)], zrec[1, :, cols(c)]], axis=0).astype(F32)
            sline[rows(2 * y + k), cols(c)] = (own + far).astype(BF16)
            for cp in y1(c):
                cp.start()
            share(0, c).start()
        c = step - 3
        if 0 <= c < CHUNKS:
            for cp, fwd, j in zip(y1_landed(c), y2(c), (3, 1)):
                cp.wait_recv()
                fwd.start()
                share(j, c).start()
        c = step - 4
        if 0 <= c < CHUNKS:
            for cp in y2_landed(c):
                cp.wait_recv()
            share(2, c).start()

    turn = 2 * mod(y, 2) + lax.div(y, 2)

    def quarter_of(m):
        return mod(turn + 2 * m + 2 * k, 4)


    def tiles(n):
        for c in range(CHUNKS):
            if STARTS[c] // 4 == n:
                shares_landed(c)
        last = n // 2

        @pl.when(k == n % 2)
        def _():
            mine = pl.ds(pl.multiple_of((4 * n + quarter_of(last)) * bs, bs), bs)
            own[:, last * bs : (last + 1) * bs] = sline[:, mine]

        lhs = sline[:, 4 * n * bs : 4 * (n + 1) * bs]
        acc = lax.dot_general(
            lhs, own[:, : count(n) * bs], (((0,), (0,)), ((), ())), preferred_element_type=F32
        )
        for m in range(count(n)):
            for p in range(4):
                t[first(n) + m, p] = acc[p * bs : (p + 1) * bs, m * bs : (m + 1) * bs].astype(BF16)

    def quarter(v):
        return pl.ds(pl.multiple_of(v * b4, b4), b4)

    parts = []
    for n in range(STAGES):
        a, b = first(n), first(n + 1)
        h = b if n < BETA_FROM else a + (b - a + 1) // 2
        parts.append([(a, h, True)] + ([(h, b, False)] if h < b else []))
    rings1, rings2, used = [], [], 0
    for n in range(STAGES):
        ones, twos = [], []
        for a, b, x_first in parts[n]:
            along = ((x, xp, xm), (z, zp, zm))
            one, two = along if x_first else along[::-1]
            ones.append(Ring(
                *one, (a, b),
                lambda p, a, b: t.at[a:b, p],
                lambda p, m: t[m, p].astype(F32),
                [l1.at[i] for i in range(4)],
                l1.at[0:2],
                rsend.at[0], rrecv.at[0, used],
            ))
            across = (zpp if x_first else xpp, two[1], two[2])
            twos.append(Spread(
                two[0], across, (a, b),
                lambda v, a, b: xb.at[a:b, quarter(v), :],
                lambda v, m: xf[m, quarter(v), :],
                l2, rsend.at[1, 0], rrecv.at[1, used, 0],
            ))
            used += 1
        rings1.append(ones)
        rings2.append(twos)

    def exchange(n):
        for a, b, x_first in parts[n]:
            p1, p2 = (x, z) if x_first else (z, x)
            rblk = block_of(p1, n)

            def one(f, up, side):
                m = f - first(n)
                stage = 2 * m + k
                cblk = block_of(quarter_of(m), stage)
                wanted = (stage <= n) if side == 0 else (stage < n)
                rr, cc = (rblk, cblk) if side == 0 else (cblk, rblk)
                tx, tc = lax.div(rr, 12), lax.div(cc, 6)
                src = o.at[f]
                dst = u.at[mod(rr, 12), mod(cc, 6), quarter(p2), :]
                ty, tz = mod(tc, 4), 2 * up + lax.div(tc, 4)
                mine = (tx == x) & (ty == y) & (tz == z)

                @pl.when(wanted & jnp.logical_not(mine))
                def _():
                    rcopy(src, dst, fsem.at[0], fsem.at[1], dev(tx, ty, tz, k)).start()

                @pl.when(wanted & mine)
                def _():
                    pltpu.make_async_copy(src, dst, fsem.at[1]).start()
                    pltpu.make_async_copy(src, spare.at[f, 2 * side + up], fsem.at[0]).start()

            @pl.loop(a, b)
            def _(f):
                for side in (0, 1):
                    for up in (0, 1):
                        one(f, up, side)

    def begin(n):
        tiles(n)
        for r in rings1[n]:
            r.start()

    def pass1(n):
        for r in rings1[n]:
            r.pass_on()

    def reduce1(n):
        def put(m, v):
            xf[m] = v
            xb[m] = v.astype(BF16)

        for r, r2 in zip(rings1[n], rings2[n]):
            r.result(put)
            r2.start()

    def reduce2(n):
        def put(m, v):
            o[m] = v.astype(BF16)

        for r in rings2[n]:
            r.result(put)
        exchange(n)

    rounds = {}
    for n in range(STAGES):
        lags = (0, 1, 3, 4) if n < 6 else (0, 1, 2, 3)
        for place, (lag, what) in enumerate(zip(lags, (begin, pass1, reduce1, reduce2))):
            rounds.setdefault(n + 5 + lag, []).append((place, n, what))
    final = CHUNKS + 3
    for step in range(final):
        gather_step(step)
        for _, n, what in sorted(rounds.get(step, ()), key=lambda item: item[:2]):
            what(n)
    gather_step(final)
    for what, n in (
        (begin, 10), (pass1, 9), (reduce1, 8), (begin, 11), (reduce2, 7), (pass1, 10), (reduce1, 9), (pass1, 11),
        (reduce2, 8), (reduce1, 10), (reduce2, 9), (reduce1, 11), (reduce2, 10), (reduce2, 11),
    ):
        what(n)

    def sent(n, ref):
        rcopy(ref, ref, csend.at[n], crecv.at[0, 0], sib).wait_send()

    sent(0, gsib)
    for n in (1, 2, 3, 4):
        sent(n, zrel.at[0])
    for n in (5, 6):
        sent(n, psend)
    sent(9, sline.at[0 : 4 * q])
    for n in (7, 8):
        sent(n, zrel.at[0])

    ups = sum((hi - lo + 1) // 2 for ps in parts for lo, hi, _ in ps)
    for half_, blocks in ((0, ups), (1, TOTAL - ups)):
        done = l1.at[0:3, 0:blocks]
        rcopy(done, done, rsend.at[0, half_], rrecv.at[0, 0, 0], sib).wait_send()
    rcopy(l2, l2, rsend.at[1, 0], rrecv.at[0, 0, 0], sib).wait_send()

    sized = (l1.at[0, 0:39], l1.at[0, 0:33])
    for core in (0, 1):

        @pl.when(k == core)
        def _():
            rcopy(sized[core], sized[core], fsem.at[0], fsem.at[1], sib).wait_recv()
            rcopy(sized[core], sized[core], fsem.at[0], fsem.at[1], sib).wait_send()

    @pl.loop(0, 12)
    def _(i):
        for j in range(6):
            direct = stage_of(x, lax.div(i, 6), mod(i, 6)) >= stage_of(halved(col), mod(col, 2), j)
            from_me = jnp.where(direct, j % 2, mod(i, 2)) == k

            @pl.when(from_me)
            def _():
                rcopy(u.at[i, j], out.at[i, j], dsem.at[0], dsem.at[1], sib).start()
                pltpu.make_async_copy(u.at[i, j], out.at[i, j], lsem.at[0]).start()

    for core in (0, 1):

        @pl.when(k == core)
        def _():
            rcopy(sized[1 - core], sized[1 - core], dsem.at[0], dsem.at[1], sib).wait_recv()
            rcopy(sized[core], sized[core], dsem.at[0], dsem.at[1], sib).wait_send()
            pltpu.make_async_copy(sized[core], sized[core], lsem.at[0]).wait()


def gather_blocks(grad):
    _, n, d = grad.shape
    q, bs = n // 4, BLOCK
    b4 = bs // 4
    subs = STAGES + STAGES - BETA_FROM
    vm = pltpu.VMEM
    dma = pltpu.SemaphoreType.DMA
    return pl.pallas_call(
        kernel,
        out_shape=jax.ShapeDtypeStruct((12, 6, bs, bs), BF16),
        in_specs=[pl.BlockSpec(memory_space=pl.ANY)],
        out_specs=pl.BlockSpec(memory_space=pl.ANY),
        scratch_shapes=[
            vm((2, q, d), BF16), vm((2, q, d), BF16), vm((q, d), BF16),
            vm((2, q // 2, d), BF16), vm((2, q // 2, d), BF16),
            vm((8 * q, d), BF16), vm((8 * q, d // 8), BF16), vm((TOTAL, 4, bs, bs), BF16),
            vm((4, TOTAL, bs, bs), BF16), vm((3, TOTAL, b4, bs), BF16),
            vm((TOTAL, bs, bs), F32), vm((TOTAL, bs, bs), BF16),
            vm((TOTAL, b4, bs), BF16), vm((12, 6, bs, bs), BF16), vm((TOTAL, 4, b4, bs), BF16),
            dma((CHUNKS,)), dma((10,)), dma((10, CHUNKS)), dma((2, 2)), dma((2, subs, 3)), dma((2,)), dma((2,)),
        ],
        compiler_params=pltpu.CompilerParams(collective_id=0, has_side_effects=True, vmem_limit_bytes=56 * 1024 * 1024),
    )(grad.reshape(2, 2, q, d))


def finish(blocks, statistic, gram, following, ub, st, gr, fo, insem, outsem):
    n = ub.shape[-1]
    col = lax.axis_index("col")
    row = lax.axis_index("row")

    def band(i):
        return pl.ds(pl.multiple_of(i * n, n), n)

    def reads(i):
        return (
            pltpu.make_async_copy(blocks.at[i], ub.at[i], insem.at[0, i]),
            pltpu.make_async_copy(statistic.at[band(i), :], st.at[band(i), :], insem.at[1, i]),
        )

    @pl.loop(0, 12)
    def _(i):
        for cp in reads(i):
            cp.start()

    @pl.loop(0, 12)
    def _(i):
        for cp in reads(i):
            cp.wait()
        rows = (band(i), slice(None))
        for j in range(6):
            at = (band(i), slice(j * n, (j + 1) * n))
            block = ub[i, j].astype(F32)
            direct = stage_of(row, lax.div(i, 6), mod(i, 6)) >= stage_of(halved(col), mod(col, 2), j)
            value = jnp.where(direct, block, block.T)
            gr[at] = value
            fo[at] = 0.95 * st[at] + 0.05 * value
        pltpu.make_async_copy(gr.at[rows], gram.at[rows], outsem.at[0]).start()
        pltpu.make_async_copy(fo.at[rows], following.at[rows], outsem.at[1]).start()

    pltpu.make_async_copy(gr, gram, outsem.at[0]).wait()
    pltpu.make_async_copy(fo, following, outsem.at[1]).wait()


def shards(grad, statistic):
    blocks = gather_blocks(grad)
    shape = jax.ShapeDtypeStruct(statistic.shape, F32)
    whole = pltpu.VMEM(statistic.shape, F32)
    dma = pltpu.SemaphoreType.DMA
    return pl.pallas_call(
        finish,
        out_shape=(shape, shape),
        in_specs=[pl.BlockSpec(memory_space=pl.ANY)] * 2,
        out_specs=(pl.BlockSpec(memory_space=pl.ANY),) * 2,
        scratch_shapes=[pltpu.VMEM(blocks.shape, BF16), whole, whole, whole, dma((2, 12)), dma((2,))],
        compiler_params=pltpu.CompilerParams(vmem_limit_bytes=60 * 1024 * 1024),
    )(blocks, statistic)


def solution(mesh):
    return jax.shard_map(
        shards,
        mesh=mesh,
        in_specs=(P("rep", ("row", "col"), None), P("row", "col")),
        out_specs=(P("row", "col"), P("row", "col")),
        check_vma=False,
    )
```

```python
import functools

import jax
import jax.numpy as jnp
from jax import lax
from jax.experimental import pallas as pl
from jax.experimental.pallas import tpu as pltpu
from jax.sharding import PartitionSpec as P

MESH = pl.DeviceIdType.MESH
BF16 = jnp.bfloat16
F32 = jnp.float32
BLOCK = 128
STAGES = 12
WIDTHS = (4,) * 12
STARTS = tuple(sum(WIDTHS[:i]) for i in range(len(WIDTHS)))
CHUNKS = len(WIDTHS)
BETA_FROM = 8
LATE = 10


def count(n):
    return n // 2 + 1


def first(n):
    return sum(count(i) for i in range(n))


TOTAL = first(STAGES)


def halved(v):
    return v // 2 if isinstance(v, int) else lax.div(v, 2)


def block_of(i, stage):
    upper = (halved(stage) + halved(i)) % 2 if isinstance(i, int) else mod(halved(stage) + halved(i), 2)
    odd = stage % 2 if isinstance(stage, int) else mod(stage, 2)
    return STAGES * i + 6 * upper + 2 * halved(halved(stage)) + odd


def stage_of(i, upper, place):
    return 4 * halved(place) + 2 * mod(upper + halved(i), 2) + (place % 2 if isinstance(place, int) else mod(place, 2))


def landing(core, upper, late):
    total = 0
    for r in range(STAGES):
        for c in range(STAGES):
            if (c // 2) % 2 == upper and min(r, c) % 2 == core and (max(r, c) >= LATE) == late:
                total += 1
    return total


def mod(a, n):
    return lax.rem(a, n)


def rcopy(src, dst, send, recv, device):
    return pltpu.make_async_remote_copy(
        src_ref=src, dst_ref=dst, send_sem=send, recv_sem=recv, device_id=device, device_id_type=MESH
    )


class Ring:
    def __init__(self, i, up, down, span, src, add, bufs, pair, sends, recvs):
        lo, hi = span
        mid = lo + (hi - lo + 1) // 2
        far, near, got, total = bufs
        at = lambda j: mod(i + j, 4)
        self.i, self.add, self.bufs, self.halves = i, add, bufs, []
        self.span, self.last, self.pair, self.up = span, recvs.at[2], pair, up
        for s, (a, b, long, short, j) in enumerate(((lo, mid, up, down, 3), (mid, hi, down, up, 1))):
            if a == b:
                continue
            cut = lambda ref: ref.at[a:b]
            self.halves.append((
                a, b, at(4 - j),
                rcopy(src(at(2), a, b), cut(far), sends.at[s], recvs.at[s], long),
                rcopy(src(at(j), a, b), cut(near), sends.at[s], recvs.at[2], short),
                rcopy(cut(total), cut(got), sends.at[s], recvs.at[2], long),
            ))

    def start(self):
        for h in self.halves:
            h[3].start()
        for h in self.halves:
            h[4].start()

    def pass_on(self):
        far, _, _, total = self.bufs
        for a, b, to, one, _, on in self.halves:
            one.wait_recv()

            @pl.loop(a, b)
            def _(m):
                total[m] = (far[m].astype(F32) + self.add(to, m)).astype(BF16)

            on.start()

    def result(self, put):
        _, near, got, _ = self.bufs
        both = self.pair.at[:, self.span[0] : self.span[1]]
        rcopy(both, both, self.last, self.last, self.up).wait_recv()
        for a, b, *_ in self.halves:

            @pl.loop(a, b)
            def _(m):
                put(m, self.add(self.i, m) + (near[m].astype(F32) + got[m].astype(F32)))


class Spread:
    def __init__(self, i, others, span, src, add, buf, send, recv):
        a, b = span
        self.i, self.add, self.buf, self.span = i, add, buf, span
        self.copies = [
            rcopy(src(mod(i + j, 4), a, b), buf.at[j - 1, a:b], send, recv, other) for j, other in zip((2, 1, 3), others)
        ]
        landed = buf.at[:, a:b]
        self.landed = rcopy(landed, landed, send, recv, others[0])

    def start(self):
        for c in self.copies:
            c.start()

    def result(self, put):
        self.landed.wait_recv()

        @pl.loop(*self.span)
        def _(m):
            theirs = (self.buf[0, m].astype(F32) + self.buf[1, m].astype(F32)) + self.buf[2, m].astype(F32)
            put(m, self.add(self.i, m) + theirs)


def kernel(
    g, out, gown, gsib, psend, zrel, zrec, sline, own, t, l1, l2, xf, xb, o, u, spare,
    lsem, csend, crecv, rsend, rrecv, fsem, dsem,
):
    rep, x, col = lax.axis_index("rep"), lax.axis_index("row"), lax.axis_index("col")
    zh, k = lax.div(rep, 2), mod(rep, 2)
    zl, y = lax.div(col, 4), mod(col, 4)
    z = 2 * zh + zl
    q, d = psend.shape
    half = q // 2
    bs = BLOCK
    b4 = bs // 4

    def dev(x, y, z, k):
        return {"rep": lax.div(z, 2) * 2 + k, "row": x, "col": mod(z, 2) * 4 + y}

    sib = dev(x, y, z, 1 - k)
    zp, zm = dev(x, y, mod(z + 1, 4), k), dev(x, y, mod(z + 3, 4), k)
    yp, ym = dev(x, mod(y + 1, 4), z, k), dev(x, mod(y + 3, 4), z, k)
    xp, xm = dev(mod(x + 1, 4), y, z, k), dev(mod(x + 3, 4), y, z, k)

    xpp, zpp = dev(mod(x + 2, 4), y, z, k), dev(x, y, mod(z + 2, 4), k)

    def cols(c):
        return slice(STARTS[c] * bs, (STARTS[c] + WIDTHS[c]) * bs)

    def rows(i):
        return pl.ds(pl.multiple_of(i * q, q), q)

    def strided(c):
        return [(pl.ds(block_of(i, c) * bs, bs), pl.ds((4 * c + i) * bs, bs)) for i in range(4)]

    def load(c):
        for there, here in strided(c):
            pltpu.make_async_copy(g.at[:, k, :, there], gown.at[:, :, here], lsem.at[c]).start()

    def swap(c):
        for there, here in strided(c):
            rcopy(g.at[:, 1 - k, :, there], gsib.at[:, :, here], csend.at[0], crecv.at[0, c], sib).start()

    def loaded(c):
        whole = gown.at[:, :, cols(c)]
        pltpu.make_async_copy(whole, whole, lsem.at[c]).wait()
        whole = gsib.at[:, :, cols(c)]
        rcopy(whole, whole, csend.at[0], crecv.at[0, c], sib).wait_recv()

    def z1(c):
        return (
            rcopy(psend.at[0:half, cols(c)], zrel.at[0, :, cols(c)], csend.at[1], crecv.at[1, c], zp),
            rcopy(psend.at[half:q, cols(c)], zrel.at[1, :, cols(c)], csend.at[2], crecv.at[2, c], zm),
        )

    def z2(c):
        return (
            rcopy(zrel.at[0, :, cols(c)], zrec.at[0, :, cols(c)], csend.at[3], crecv.at[3, c], zp),
            rcopy(zrel.at[1, :, cols(c)], zrec.at[1, :, cols(c)], csend.at[4], crecv.at[4, c], zm),
        )

    def block(j, c, part=None):
        base = (2 * mod(y + j, 4) + k) * q
        if part is None:
            return sline.at[pl.ds(pl.multiple_of(base, q), q), cols(c)]
        return sline.at[pl.ds(pl.multiple_of(base + part * half, half), half), cols(c)]

    def y1(c):
        own = block(0, c)
        return (
            rcopy(own, own, csend.at[5], crecv.at[5, c], yp),
            rcopy(own, own, csend.at[6], crecv.at[6, c], ym),
        )

    def y1_landed(c):
        down, upper = block(3, c), block(1, c)
        return (
            rcopy(down, down, csend.at[5], crecv.at[5, c], yp),
            rcopy(upper, upper, csend.at[6], crecv.at[6, c], ym),
        )

    def y2(c):
        down, upper = block(3, c, 0), block(1, c, 1)
        return (
            rcopy(down, down, csend.at[7], crecv.at[7, c], yp),
            rcopy(upper, upper, csend.at[8], crecv.at[8, c], ym),
        )

    def y2_landed(c):
        lo, hi = block(2, c, 0), block(2, c, 1)
        return (
            rcopy(lo, lo, csend.at[7], crecv.at[7, c], yp),
            rcopy(hi, hi, csend.at[8], crecv.at[8, c], ym),
        )

    def share(j, c):
        blk = block(j, c)
        return rcopy(blk, blk, csend.at[9], crecv.at[9, c], sib)

    def shares_landed(c):
        four = sline.at[0 : 4 * q, cols(c)]
        rcopy(four, four, csend.at[9], crecv.at[9, c], sib).wait_recv()

    barrier = pltpu.get_barrier_semaphore()
    around = (sib, xp, xm, yp, ym, zp, zm)
    for other in around:
        pl.semaphore_signal(barrier, inc=1, device_id=other, device_id_type=MESH)
    for c in range(CHUNKS):
        load(c)
    own[...] = jnp.zeros_like(own)
    pl.semaphore_wait(barrier, len(around))
    for c in range(CHUNKS):
        swap(c)

    def gather_step(step):
        c = step
        if c < CHUNKS:
            loaded(c)
            away = 1 - zh
            psend[:, cols(c)] = (gown[away, :, cols(c)].astype(F32) + gsib[away, :, cols(c)].astype(F32)).astype(BF16)
            for cp in z1(c):
                cp.start()
        c = step - 1
        if 0 <= c < CHUNKS:
            for cp, fwd in zip(z1(c), z2(c)):
                cp.wait_recv()
                fwd.start()
        c = step - 2
        if 0 <= c < CHUNKS:
            for cp in z2(c):
                cp.wait_recv()
            own = gown[zh, :, cols(c)].astype(F32) + gsib[zh, :, cols(c)].astype(F32)
            far = jnp.concatenate([zrec[0, :, cols(c)], zrec[1, :, cols(c)]], axis=0).astype(F32)
            sline[rows(2 * y + k), cols(c)] = (own + far).astype(BF16)
            for cp in y1(c):
                cp.start()
            share(0, c).start()
        c = step - 3
        if 0 <= c < CHUNKS:
            for cp, fwd, j in zip(y1_landed(c), y2(c), (3, 1)):
                cp.wait_recv()
                fwd.start()
                share(j, c).start()
        c = step - 4
        if 0 <= c < CHUNKS:
            for cp in y2_landed(c):
                cp.wait_recv()
            share(2, c).start()

    turn = 2 * mod(y, 2) + lax.div(y, 2)

    def quarter_of(m):
        return mod(turn + 2 * m + 2 * k, 4)


    def tiles(n):
        for c in range(CHUNKS):
            if STARTS[c] // 4 == n:
                shares_landed(c)
        last = n // 2

        @pl.when(k == n % 2)
        def _():
            mine = pl.ds(pl.multiple_of((4 * n + quarter_of(last)) * bs, bs), bs)
            own[:, last * bs : (last + 1) * bs] = sline[:, mine]

        lhs = sline[:, 4 * n * bs : 4 * (n + 1) * bs]
        acc = lax.dot_general(
            lhs, own[:, : count(n) * bs], (((0,), (0,)), ((), ())), preferred_element_type=F32
        )
        for m in range(count(n)):
            for p in range(4):
                t[first(n) + m, p] = acc[p * bs : (p + 1) * bs, m * bs : (m + 1) * bs].astype(BF16)

    def quarter(v):
        return pl.ds(pl.multiple_of(v * b4, b4), b4)

    parts = []
    for n in range(STAGES):
        a, b = first(n), first(n + 1)
        h = b if n < BETA_FROM else a + (b - a + 1) // 2
        parts.append([(a, h, True)] + ([(h, b, False)] if h < b else []))
    rings1, rings2, used = [], [], 0
    for n in range(STAGES):
        ones, twos = [], []
        for a, b, x_first in parts[n]:
            along = ((x, xp, xm), (z, zp, zm))
            one, two = along if x_first else along[::-1]
            ones.append(Ring(
                *one, (a, b),
                lambda p, a, b: t.at[a:b, p],
                lambda p, m: t[m, p].astype(F32),
                [l1.at[i] for i in range(4)],
                l1.at[0:2],
                rsend.at[0], rrecv.at[0, used],
            ))
            across = (zpp if x_first else xpp, two[1], two[2])
            twos.append(Spread(
                two[0], across, (a, b),
                lambda v, a, b: xb.at[a:b, quarter(v), :],
                lambda v, m: xf[m, quarter(v), :],
                l2, rsend.at[1, 0], rrecv.at[1, used, 0],
            ))
            used += 1
        rings1.append(ones)
        rings2.append(twos)

    def exchange(n):
        landed = fsem.at[2 if n >= LATE else 1]
        for a, b, x_first in parts[n]:
            p1, p2 = (x, z) if x_first else (z, x)
            rblk = block_of(p1, n)

            def one(f, up, side):
                m = f - first(n)
                stage = 2 * m + k
                cblk = block_of(quarter_of(m), stage)
                wanted = (stage <= n) if side == 0 else (stage < n)
                rr, cc = (rblk, cblk) if side == 0 else (cblk, rblk)
                tx, tc = lax.div(rr, 12), lax.div(cc, 6)
                src = o.at[f]
                dst = u.at[mod(rr, 12), mod(cc, 6), quarter(p2), :]
                ty, tz = mod(tc, 4), 2 * up + lax.div(tc, 4)
                mine = (tx == x) & (ty == y) & (tz == z)

                @pl.when(wanted & jnp.logical_not(mine))
                def _():
                    rcopy(src, dst, fsem.at[0], landed, dev(tx, ty, tz, k)).start()

                @pl.when(wanted & mine)
                def _():
                    pltpu.make_async_copy(src, dst, landed).start()
                    pltpu.make_async_copy(src, spare.at[f, 2 * side + up], fsem.at[0]).start()

            @pl.loop(a, b)
            def _(f):
                for side in (0, 1):
                    for up in (0, 1):
                        one(f, up, side)

    def begin(n):
        tiles(n)
        for r in rings1[n]:
            r.start()

    def pass1(n):
        for r in rings1[n]:
            r.pass_on()

    def reduce1(n):
        def put(m, v):
            xf[m] = v
            xb[m] = v.astype(BF16)

        for r, r2 in zip(rings1[n], rings2[n]):
            r.result(put)
            r2.start()

    def reduce2(n):
        def put(m, v):
            o[m] = v.astype(BF16)

        for r in rings2[n]:
            r.result(put)
        exchange(n)

    rounds = {}
    for n in range(STAGES):
        lags = (0, 1, 3, 4) if n < 6 else (0, 1, 2, 3)
        for place, (lag, what) in enumerate(zip(lags, (begin, pass1, reduce1, reduce2))):
            rounds.setdefault(n + 5 + lag, []).append((place, n, what))
    final = CHUNKS + 3
    for step in range(final):
        gather_step(step)
        for _, n, what in sorted(rounds.get(step, ()), key=lambda item: item[:2]):
            what(n)
    gather_step(final)
    for what, n in (
        (begin, 10), (pass1, 9), (reduce1, 8), (begin, 11), (reduce2, 7), (pass1, 10), (reduce1, 9), (pass1, 11),
        (reduce2, 8), (reduce1, 10), (reduce2, 9), (reduce1, 11), (reduce2, 10), (reduce2, 11),
    ):
        what(n)

    def sent(n, ref):
        rcopy(ref, ref, csend.at[n], crecv.at[0, 0], sib).wait_send()

    sent(0, gsib)
    for n in (1, 2, 3, 4):
        sent(n, zrel.at[0])
    for n in (5, 6):
        sent(n, psend)
    sent(9, sline.at[0 : 4 * q])
    for n in (7, 8):
        sent(n, zrel.at[0])

    ups = sum((hi - lo + 1) // 2 for ps in parts for lo, hi, _ in ps)
    for half_, blocks in ((0, ups), (1, TOTAL - ups)):
        done = l1.at[0:3, 0:blocks]
        rcopy(done, done, rsend.at[0, half_], rrecv.at[0, 0, 0], sib).wait_send()
    rcopy(l2, l2, rsend.at[1, 0], rrecv.at[0, 0, 0], sib).wait_send()

    upper = mod(col + zl, 2)

    def arrived(late):
        for core in (0, 1):
            for part in (0, 1):

                @pl.when((k == core) & (upper == part))
                def _():
                    ref = l1.at[0, 0 : landing(core, part, late)]
                    rcopy(ref, ref, fsem.at[0], fsem.at[2 if late else 1], sib).wait_recv()

    def swap_blocks(late):
        @pl.loop(0, 12)
        def _(i):
            for j in range(6):
                r = stage_of(x, lax.div(i, 6), mod(i, 6))
                c = stage_of(halved(col), mod(col, 2), j)
                from_me = jnp.where(r >= c, j % 2, mod(i, 2)) == k
                now = (r >= LATE) | (c >= LATE)

                @pl.when(from_me & (now if late else jnp.logical_not(now)))
                def _():
                    rcopy(u.at[i, j], out.at[i, j], dsem.at[0], dsem.at[1], sib).start()
                    pltpu.make_async_copy(u.at[i, j], out.at[i, j], lsem.at[0]).start()

    for late in (False, True):
        arrived(late)
        swap_blocks(late)
    sized = (l1.at[0, 0:39], l1.at[0, 0:33])
    for core in (0, 1):

        @pl.when(k == core)
        def _():
            rcopy(sized[core], sized[core], fsem.at[0], fsem.at[1], sib).wait_send()

    for core in (0, 1):

        @pl.when(k == core)
        def _():
            rcopy(sized[1 - core], sized[1 - core], dsem.at[0], dsem.at[1], sib).wait_recv()
            rcopy(sized[core], sized[core], dsem.at[0], dsem.at[1], sib).wait_send()
            pltpu.make_async_copy(sized[core], sized[core], lsem.at[0]).wait()


def gather_blocks(grad):
    _, n, d = grad.shape
    q, bs = n // 4, BLOCK
    b4 = bs // 4
    subs = STAGES + STAGES - BETA_FROM
    vm = pltpu.VMEM
    dma = pltpu.SemaphoreType.DMA
    return pl.pallas_call(
        kernel,
        out_shape=jax.ShapeDtypeStruct((12, 6, bs, bs), BF16),
        in_specs=[pl.BlockSpec(memory_space=pl.ANY)],
        out_specs=pl.BlockSpec(memory_space=pl.ANY),
        scratch_shapes=[
            vm((2, q, d), BF16), vm((2, q, d), BF16), vm((q, d), BF16),
            vm((2, q // 2, d), BF16), vm((2, q // 2, d), BF16),
            vm((8 * q, d), BF16), vm((8 * q, d // 8), BF16), vm((TOTAL, 4, bs, bs), BF16),
            vm((4, TOTAL, bs, bs), BF16), vm((3, TOTAL, b4, bs), BF16),
            vm((TOTAL, bs, bs), F32), vm((TOTAL, bs, bs), BF16),
            vm((TOTAL, b4, bs), BF16), vm((12, 6, bs, bs), BF16), vm((TOTAL, 4, b4, bs), BF16),
            dma((CHUNKS,)), dma((10,)), dma((10, CHUNKS)), dma((2, 2)), dma((2, subs, 3)), dma((3,)), dma((2,)),
        ],
        compiler_params=pltpu.CompilerParams(collective_id=0, has_side_effects=True, vmem_limit_bytes=56 * 1024 * 1024),
    )(grad.reshape(2, 2, q, d))


def finish(blocks, statistic, gram, following, ub, st, gr, fo, insem, outsem):
    n = ub.shape[-1]
    col = lax.axis_index("col")
    row = lax.axis_index("row")

    def band(i):
        return pl.ds(pl.multiple_of(i * n, n), n)

    def reads(i):
        return (
            pltpu.make_async_copy(blocks.at[i], ub.at[i], insem.at[0, i]),
            pltpu.make_async_copy(statistic.at[band(i), :], st.at[band(i), :], insem.at[1, i]),
        )

    @pl.loop(0, 12)
    def _(i):
        for cp in reads(i):
            cp.start()

    @pl.loop(0, 12)
    def _(i):
        for cp in reads(i):
            cp.wait()
        rows = (band(i), slice(None))
        for j in range(6):
            at = (band(i), slice(j * n, (j + 1) * n))
            block = ub[i, j].astype(F32)
            direct = stage_of(row, lax.div(i, 6), mod(i, 6)) >= stage_of(halved(col), mod(col, 2), j)
            value = jnp.where(direct, block, block.T)
            gr[at] = value
            fo[at] = 0.95 * st[at] + 0.05 * value
        pltpu.make_async_copy(gr.at[rows], gram.at[rows], outsem.at[0]).start()
        pltpu.make_async_copy(fo.at[rows], following.at[rows], outsem.at[1]).start()

    pltpu.make_async_copy(gr, gram, outsem.at[0]).wait()
    pltpu.make_async_copy(fo, following, outsem.at[1]).wait()


def shards(grad, statistic):
    blocks = gather_blocks(grad)
    shape = jax.ShapeDtypeStruct(statistic.shape, F32)
    whole = pltpu.VMEM(statistic.shape, F32)
    dma = pltpu.SemaphoreType.DMA
    return pl.pallas_call(
        finish,
        out_shape=(shape, shape),
        in_specs=[pl.BlockSpec(memory_space=pl.ANY)] * 2,
        out_specs=(pl.BlockSpec(memory_space=pl.ANY),) * 2,
        scratch_shapes=[pltpu.VMEM(blocks.shape, BF16), whole, whole, whole, dma((2, 12)), dma((2,))],
        compiler_params=pltpu.CompilerParams(vmem_limit_bytes=60 * 1024 * 1024),
    )(blocks, statistic)


def solution(mesh):
    return jax.shard_map(
        shards,
        mesh=mesh,
        in_specs=(P("rep", ("row", "col"), None), P("row", "col")),
        out_specs=(P("row", "col"), P("row", "col")),
        check_vma=False,
    )
```
